8 devices in a mesh: part: 1 (over z), model: 2 (over y), data: 4 (over x, core).
Axes of the slice: x: 2, y: 2, z: 1, core: 2. Of those that a mesh axis runs over, the one named last changes fastest.
Arguments:
- hidden: bfloat16 [256, 1, 2560], P(('part', 'data'))
- positions: int32 [256], P(('part', 'data'))
- k_local: bfloat16 [256, 64, 4, 256], P(('part', 'data'), None, 'model')
- v_local: bfloat16 [256, 64, 4, 256], P(('part', 'data'), None, 'model')
- k_global: bfloat16 [256, 512, 4, 256], P(('part', 'data'), None, 'model')
- v_global: bfloat16 [256, 512, 4, 256], P(('part', 'data'), None, 'model')
- w_q: bfloat16 [2, 2560, 8, 256], P(None, 'data', 'model')
- w_k: bfloat16 [2, 2560, 4, 256], P(None, 'data', 'model')
- w_v: bfloat16 [2, 2560, 4, 256], P(None, 'data', 'model')
- w_o: bfloat16 [2, 8, 256, 2560], P(None, 'model', None, 'data')
- w_gate: bfloat16 [2, 2560, 10240], P(None, 'data', 'model')
- w_up: bfloat16 [2, 2560, 10240], P(None, 'data', 'model')
- w_down: bfloat16 [2, 10240, 2560], P(None, 'model', 'data')
- norm_gains: bfloat16 [2, 4, 2560], replicated
Outputs:
- output 1: bfloat16 [256, 1, 2560], P(('part', 'data'))
- output 2: bfloat16 [256, 64, 4, 256], P(('part', 'data'), None, 'model')
- output 3: bfloat16 [256, 64, 4, 256], P(('part', 'data'), None, 'model')
- output 4: bfloat16 [256, 512, 4, 256], P(('part', 'data'), None, 'model')
- output 5: bfloat16 [256, 512, 4, 256], P(('part', 'data'), None, 'model')
All inputs are finite; a program needn't handle non-finite values.
Results may differ from the reference program's by a relative error of at most 0.02.
Values are sent between devices in bfloat16 or wider.
A program may use at most 1 GiB of HBM per device.

```python
import jax
import jax.numpy as jnp
from jax import lax

MODEL_DIM = 2560
NUM_HEADS = 8
NUM_KV = 4
HEAD_DIM = 256
FF_DIM = 10240
WINDOW = 64
CTX_LEN = 512
BATCH = 256

HEAD_GROUP = NUM_HEADS // NUM_KV
SOFT_CAP = 50.0
NORM_EPS = 1e-6
ROPE_BASE = 10000.0
QK_SCALE = 6.0


def setup_inputs(seed: int = 0, part: int = 0) -> dict:
    base_key = jax.random.key(seed)
    weight_keys = jax.random.split(base_key, 8)
    part_keys = jax.random.split(jax.random.fold_in(base_key, part), 6)

    def normal_bf16(rng_key, arr_shape, factor):
        return (factor * jax.random.normal(rng_key, arr_shape, jnp.float32)).astype(jnp.bfloat16)

    raw_pos = jax.random.randint(part_keys[0], (BATCH,), 0, CTX_LEN)
    row_ids = jnp.arange(BATCH)
    positions = jnp.where(row_ids == 0, CTX_LEN - 1, jnp.where(row_ids == BATCH // 2, raw_pos % WINDOW, raw_pos)).astype(jnp.int32)
    kv_local = (BATCH, WINDOW, NUM_KV, HEAD_DIM)
    kv_global = (BATCH, CTX_LEN, NUM_KV, HEAD_DIM)
    in_scale = MODEL_DIM ** -0.5
    return {
        "hidden": normal_bf16(part_keys[1], (BATCH, 1, MODEL_DIM), 1.0),
        "positions": positions,
        "k_local": normal_bf16(part_keys[2], kv_local, QK_SCALE),
        "v_local": normal_bf16(part_keys[3], kv_local, 1.0),
        "k_global": normal_bf16(part_keys[4], kv_global, QK_SCALE),
        "v_global": normal_bf16(part_keys[5], kv_global, 1.0),
        "w_q": normal_bf16(weight_keys[0], (2, MODEL_DIM, NUM_HEADS, HEAD_DIM), QK_SCALE * in_scale),
        "w_k": normal_bf16(weight_keys[1], (2, MODEL_DIM, NUM_KV, HEAD_DIM), QK_SCALE * in_scale),
        "w_v": normal_bf16(weight_keys[2], (2, MODEL_DIM, NUM_KV, HEAD_DIM), in_scale),
        "w_o": normal_bf16(weight_keys[3], (2, NUM_HEADS, HEAD_DIM, MODEL_DIM), (NUM_HEADS * HEAD_DIM) ** -0.5),
        "w_gate": normal_bf16(weight_keys[4], (2, MODEL_DIM, FF_DIM), in_scale),
        "w_up": normal_bf16(weight_keys[5], (2, MODEL_DIM, FF_DIM), in_scale),
        "w_down": normal_bf16(weight_keys[6], (2, FF_DIM, MODEL_DIM), FF_DIM ** -0.5),
        "norm_gains": normal_bf16(weight_keys[7], (2, 4, MODEL_DIM), 0.5),
    }


def rms_norm(hidden, gain):
    mean_sq = jnp.mean(jnp.square(hidden), axis=-1, keepdims=True)
    return hidden * lax.rsqrt(mean_sq + NORM_EPS) * (1.0 + gain.astype(jnp.float32))


def rotary(hidden, cos_t, sin_t):
    half_dim = hidden.shape[-1] // 2
    first_half = hidden[..., :half_dim]
    second_half = hidden[..., half_dim:]
    return jnp.concatenate([first_half * cos_t - second_half * sin_t, second_half * cos_t + first_half * sin_t], axis=-1)


def rope_tables(positions):
    inv_freq = ROPE_BASE ** (-jnp.arange(0, HEAD_DIM, 2).astype(jnp.float32) / HEAD_DIM)
    angles = positions.astype(jnp.float32)[:, None] * inv_freq[None, :]
    return jnp.cos(angles)[:, None, :], jnp.sin(angles)[:, None, :]


def attend_row(operands):
    q_row, k_row, v_row, valid_row = operands
    q_grp = q_row.reshape(NUM_KV, HEAD_GROUP, HEAD_DIM).astype(jnp.float32)
    scores = jnp.einsum("kgd,tkd->kgt", q_grp, k_row.astype(jnp.float32))
    scores = SOFT_CAP * jnp.tanh(scores / SOFT_CAP)
    scores = jnp.where(valid_row[None, None, :], scores, -1e30)
    attn_prob = jax.nn.softmax(scores, axis=-1).astype(jnp.bfloat16)
    head_out = jnp.einsum("kgt,tkd->kgd", attn_prob.astype(jnp.float32), v_row.astype(jnp.float32))
    return head_out.astype(jnp.bfloat16).reshape(NUM_HEADS, HEAD_DIM)


def decoder_layer(hidden, positions, k_cache, v_cache, weights, layer, is_local):
    w_q, w_k, w_v, w_o, w_gate, w_up, w_down, norm_gains = weights
    layer_gains = norm_gains[layer]
    residual = hidden[:, 0, :].astype(jnp.float32)
    normed = rms_norm(residual, layer_gains[0]).astype(jnp.bfloat16)
    q_proj = jnp.dot(normed, w_q[layer].reshape(MODEL_DIM, NUM_HEADS * HEAD_DIM), preferred_element_type=jnp.float32).reshape(BATCH, NUM_HEADS, HEAD_DIM)
    k_proj = jnp.dot(normed, w_k[layer].reshape(MODEL_DIM, NUM_KV * HEAD_DIM), preferred_element_type=jnp.float32).reshape(BATCH, NUM_KV, HEAD_DIM)
    v_proj = jnp.dot(normed, w_v[layer].reshape(MODEL_DIM, NUM_KV * HEAD_DIM), preferred_element_type=jnp.float32).reshape(BATCH, NUM_KV, HEAD_DIM)
    cos_t, sin_t = rope_tables(positions)
    q_new = (rotary(q_proj, cos_t, sin_t) * HEAD_DIM ** -0.5).astype(jnp.bfloat16)
    k_new = rotary(k_proj, cos_t, sin_t).astype(jnp.bfloat16)
    v_new = v_proj.astype(jnp.bfloat16)
    cache_len = k_cache.shape[1]
    slot_ids = jnp.arange(cache_len)
    if is_local:
        slot_now = positions % cache_len
        valid_mask = ((positions[:, None] - slot_ids[None, :]) % cache_len) <= positions[:, None]
    else:
        slot_now = positions
        valid_mask = slot_ids[None, :] <= positions[:, None]
    slot_hit = (slot_ids[None, :] == slot_now[:, None])[:, :, None, None]
    k_cache = jnp.where(slot_hit, k_new[:, None], k_cache)
    v_cache = jnp.where(slot_hit, v_new[:, None], v_cache)
    head_out = lax.map(attend_row, (q_new, k_cache, v_cache, valid_mask))
    attn_sum = jnp.dot(head_out.reshape(BATCH, NUM_HEADS * HEAD_DIM), w_o[layer].reshape(NUM_HEADS * HEAD_DIM, MODEL_DIM), preferred_element_type=jnp.float32)
    mid_hidden = (residual + rms_norm(attn_sum, layer_gains[1])).astype(jnp.bfloat16)
    mid_f = mid_hidden.astype(jnp.float32)
    normed_ff = rms_norm(mid_f, layer_gains[2]).astype(jnp.bfloat16)
    gate_proj = jnp.dot(normed_ff, w_gate[layer], preferred_element_type=jnp.float32)
    up_proj = jnp.dot(normed_ff, w_up[layer], preferred_element_type=jnp.float32)
    gated_act = (jax.nn.gelu(gate_proj, approximate=True) * up_proj).astype(jnp.bfloat16)
    down_sum = jnp.dot(gated_act, w_down[layer], preferred_element_type=jnp.float32)
    layer_out = (mid_f + rms_norm(down_sum, layer_gains[3])).astype(jnp.bfloat16)
    return layer_out[:, None, :], k_cache, v_cache


def reference(hidden, positions, k_local, v_local, k_global, v_global, w_q, w_k, w_v, w_o, w_gate, w_up, w_down, norm_gains):
    weights = (w_q, w_k, w_v, w_o, w_gate, w_up, w_down, norm_gains)
    mid_hidden, k_local, v_local = decoder_layer(hidden, positions, k_local, v_local, weights, 0, True)
    final, k_global, v_global = decoder_layer(mid_hidden, positions, k_global, v_global, weights, 1, False)
    return (final, k_local, v_local, k_global, v_global)
```

```python
import jax
import jax.numpy as jnp
from jax import lax
from jax.sharding import PartitionSpec as P

SOFT_CAP = 50.0
NORM_EPS = 1e-6
ROPE_BASE = 10000.0

ROW_SPEC = P(("part", "data"), None, None)
POS_SPEC = P(("part", "data"))
CACHE_SPEC = P(("part", "data"), None, "model", None)
PROJ_IN_SPEC = P(None, "data", "model", None)
PROJ_OUT_SPEC = P(None, "model", None, "data")
FF_IN_SPEC = P(None, "data", "model")
FF_OUT_SPEC = P(None, "model", "data")
GAIN_SPEC = P(None, None, None)


def rotary(hidden, cos_t, sin_t):
    half_dim = hidden.shape[-1] // 2
    first_half = hidden[..., :half_dim]
    second_half = hidden[..., half_dim:]
    return jnp.concatenate([first_half * cos_t - second_half * sin_t, second_half * cos_t + first_half * sin_t], axis=-1)


def rope_tables(positions, head_dim):
    inv_freq = ROPE_BASE ** (-jnp.arange(0, head_dim, 2).astype(jnp.float32) / head_dim)
    angles = positions.astype(jnp.float32)[:, None] * inv_freq[None, :]
    return jnp.cos(angles)[:, None, :], jnp.sin(angles)[:, None, :]


def attend(q_new, k_new, v_new, positions, k_cache, v_cache, is_local):
    n_rows, cache_len, kv_loc, head_dim = k_cache.shape
    group_size = q_new.shape[1] // kv_loc
    slot_ids = jnp.arange(cache_len)
    if is_local:
        slot_now = positions % cache_len
        valid_mask = ((positions[:, None] - slot_ids[None, :]) % cache_len) <= positions[:, None]
    else:
        slot_now = positions
        valid_mask = slot_ids[None, :] <= positions[:, None]
    slot_hit = (slot_ids[None, :] == slot_now[:, None])[:, :, None, None]
    k_cache = jnp.where(slot_hit, k_new[:, None], k_cache)
    v_cache = jnp.where(slot_hit, v_new[:, None], v_cache)
    q_grp = q_new.reshape(n_rows, kv_loc, group_size, head_dim)
    scores = jnp.einsum("bkgd,btkd->bkgt", q_grp, k_cache, preferred_element_type=jnp.float32)
    scores = SOFT_CAP * jnp.tanh(scores / SOFT_CAP)
    scores = jnp.where(valid_mask[:, None, None, :], scores, -1e30)
    attn_prob = jax.nn.softmax(scores, axis=-1).astype(jnp.bfloat16)
    head_out = jnp.einsum("bkgt,btkd->bkgd", attn_prob, v_cache, preferred_element_type=jnp.float32)
    return head_out.astype(jnp.bfloat16).reshape(n_rows, kv_loc * group_size, head_dim), k_cache, v_cache


def width_norm(hidden, gain, width):
    sum_sq = lax.psum(jnp.sum(jnp.square(hidden), axis=-1, keepdims=True), "data")
    return hidden * lax.rsqrt(sum_sq / width + NORM_EPS) * (1.0 + gain.astype(jnp.float32))


def layer_block(hidden, positions, k_cache, v_cache, weights, layer, is_local):
    w_q, w_k, w_v, w_o, w_gate, w_up, w_down, norm_gains = weights
    share = hidden.shape[1]
    n_data = lax.axis_size("data")
    width = share * n_data
    gains = lax.dynamic_slice_in_dim(norm_gains[layer], lax.axis_index("data") * share, share, axis=1)
    n_q, head_dim = w_q.shape[2:]
    n_kv = w_k.shape[2]
    residual = hidden.astype(jnp.float32)
    normed = width_norm(residual, gains[0], width).astype(jnp.bfloat16)
    w_in = jnp.concatenate([w_q[layer].reshape(share, -1), w_k[layer].reshape(share, -1), w_v[layer].reshape(share, -1)], axis=1)
    qkv = jnp.dot(normed, w_in, preferred_element_type=jnp.float32)
    qkv = lax.psum_scatter(qkv, "data", scatter_dimension=0, tiled=True)
    n_rows = qkv.shape[0]
    q_proj = qkv[:, :n_q * head_dim].reshape(n_rows, n_q, head_dim)
    k_proj = qkv[:, n_q * head_dim:(n_q + n_kv) * head_dim].reshape(n_rows, n_kv, head_dim)
    v_proj = qkv[:, (n_q + n_kv) * head_dim:].reshape(n_rows, n_kv, head_dim)
    cos_t, sin_t = rope_tables(positions, head_dim)
    q_new = (rotary(q_proj, cos_t, sin_t) * head_dim ** -0.5).astype(jnp.bfloat16)
    k_new = rotary(k_proj, cos_t, sin_t).astype(jnp.bfloat16)
    head_out, k_cache, v_cache = attend(q_new, k_new, v_proj.astype(jnp.bfloat16), positions, k_cache, v_cache, is_local)
    heads_all = lax.all_gather(head_out.reshape(n_rows, -1), "data", axis=0, tiled=True)
    attn_sum = lax.psum(jnp.dot(heads_all, w_o[layer].reshape(-1, share), preferred_element_type=jnp.float32), "model")
    mid_hidden = (residual + width_norm(attn_sum, gains[1], width)).astype(jnp.bfloat16)
    mid_f = mid_hidden.astype(jnp.float32)
    normed_ff = width_norm(mid_f, gains[2], width).astype(jnp.bfloat16)
    gate_proj = jnp.dot(normed_ff, w_gate[layer], preferred_element_type=jnp.float32)
    gate_proj = lax.psum_scatter(gate_proj, "data", scatter_dimension=0, tiled=True)
    up_proj = jnp.dot(normed_ff, w_up[layer], preferred_element_type=jnp.float32)
    up_proj = lax.psum_scatter(up_proj, "data", scatter_dimension=0, tiled=True)
    gated_act = (jax.nn.gelu(gate_proj, approximate=True) * up_proj).astype(jnp.bfloat16)
    acts_all = lax.all_gather(gated_act, "data", axis=0, tiled=True)
    down_sum = lax.psum(jnp.dot(acts_all, w_down[layer], preferred_element_type=jnp.float32), "model")
    return (mid_f + width_norm(down_sum, gains[3], width)).astype(jnp.bfloat16), k_cache, v_cache


def solution(mesh):
    def device_step(hidden, positions, k_local, v_local, k_global, v_global, w_q, w_k, w_v, w_o, w_gate, w_up, w_down, norm_gains):
        weights = (w_q, w_k, w_v, w_o, w_gate, w_up, w_down, norm_gains)
        hidden_cols = lax.all_to_all(hidden[:, 0, :], "data", 1, 0, tiled=True)
        hidden_cols, k_local, v_local = layer_block(hidden_cols, positions, k_local, v_local, weights, 0, True)
        hidden_cols, k_global, v_global = layer_block(hidden_cols, positions, k_global, v_global, weights, 1, False)
        final = lax.all_to_all(hidden_cols, "data", 0, 1, tiled=True)[:, None, :]
        return final, k_local, v_local, k_global, v_global

    in_specs = (ROW_SPEC, POS_SPEC, CACHE_SPEC, CACHE_SPEC, CACHE_SPEC, CACHE_SPEC, PROJ_IN_SPEC, PROJ_IN_SPEC, PROJ_IN_SPEC, PROJ_OUT_SPEC, FF_IN_SPEC, FF_IN_SPEC, FF_OUT_SPEC, GAIN_SPEC)
    out_specs = (ROW_SPEC, CACHE_SPEC, CACHE_SPEC, CACHE_SPEC, CACHE_SPEC)
    return jax.shard_map(device_step, mesh=mesh, in_specs=in_specs, out_specs=out_specs, check_vma=False)
```

```python
import functools

import jax
import jax.numpy as jnp
from jax import lax
from jax.experimental import pallas as pl
from jax.experimental.pallas import tpu as pltpu
from jax.sharding import PartitionSpec as P

SOFT_CAP = 50.0
NORM_EPS = 1e-6
ROPE_BASE = 10000.0

ROW_SPEC = P(("part", "data"), None, None)
POS_SPEC = P(("part", "data"))
CACHE_SPEC = P(("part", "data"), None, "model", None)
PROJ_IN_SPEC = P(None, "data", "model", None)
PROJ_OUT_SPEC = P(None, "model", None, "data")
FF_IN_SPEC = P(None, "data", "model")
FF_OUT_SPEC = P(None, "model", "data")
GAIN_SPEC = P(None, None, None)


def rotary(hidden, cos_t, sin_t):
    half_dim = hidden.shape[-1] // 2
    first_half = hidden[..., :half_dim]
    second_half = hidden[..., half_dim:]
    return jnp.concatenate([first_half * cos_t - second_half * sin_t, second_half * cos_t + first_half * sin_t], axis=-1)


def rope_tables(positions, head_dim):
    inv_freq = ROPE_BASE ** (-jnp.arange(0, head_dim, 2).astype(jnp.float32) / head_dim)
    angles = positions.astype(jnp.float32)[:, None] * inv_freq[None, :]
    return jnp.cos(angles)[:, None, :], jnp.sin(angles)[:, None, :]


LANES = 128
STEP_ROWS = 4


def attend_kernel(cache_len, n_rows, depth, pos_ref, q_ref, kn_ref, vn_ref, k_hbm, v_hbm, head_ref, ko_hbm, vo_hbm, kbuf, vbuf, rd_sem, wr_sem):
    n_steps = n_rows // STEP_ROWS
    n_cols = cache_len * 4

    def reads(step):
        slot = lax.rem(step, depth)
        rows = pl.ds(step * STEP_ROWS, STEP_ROWS)
        return (pltpu.make_async_copy(k_hbm.at[rows], kbuf.at[slot], rd_sem.at[0, slot]),
                pltpu.make_async_copy(v_hbm.at[rows], vbuf.at[slot], rd_sem.at[1, slot]))

    def writes(step):
        slot = lax.rem(step, depth)
        rows = pl.ds(step * STEP_ROWS, STEP_ROWS)
        return (pltpu.make_async_copy(kbuf.at[slot], ko_hbm.at[rows], wr_sem.at[0, slot]),
                pltpu.make_async_copy(vbuf.at[slot], vo_hbm.at[rows], wr_sem.at[1, slot]))

    ahead = depth - 2
    for step in range(ahead):
        for copy in reads(step):
            copy.start()

    row_id = lax.broadcasted_iota(jnp.int32, (8, n_cols), 0)
    col_id = lax.broadcasted_iota(jnp.int32, (8, n_cols), 1)
    half_row, kv_row = row_id // 4, (row_id // 2) % 2
    half_col, kv_col, slot_col = (col_id // 2) % 2, col_id % 2, col_id // 4
    same_half, same_kv = half_row == half_col, kv_row == kv_col
    sub_id = lax.broadcasted_iota(jnp.int32, (16, LANES), 0) // 4

    @pl.loop(0, n_steps)
    def _(step):
        slot = lax.rem(step, depth)

        @pl.when(step + ahead < n_steps)
        def _():
            @pl.when(step >= 2)
            def _():
                for copy in writes(step - 2):
                    copy.wait()
            for copy in reads(step + ahead):
                copy.start()

        for copy in reads(step):
            copy.wait()
        for i in range(STEP_ROWS):
            row = step * STEP_ROWS + i
            pos = pos_ref[row]
            now = lax.rem(pos, cache_len)
            window = pl.ds(pl.multiple_of(now // 4 * 16, 16), 16)
            hit = sub_id == lax.rem(now, 4)
            kbuf[slot, i, window, :] = jnp.where(hit, kn_ref[row], kbuf[slot, i, window, :])
            vbuf[slot, i, window, :] = jnp.where(hit, vn_ref[row], vbuf[slot, i, window, :])
        for i in range(STEP_ROWS):
            row = step * STEP_ROWS + i
            pos = pos_ref[row]
            part = lax.dot_general(q_ref[row], kbuf[slot, i], (((1,), (1,)), ((), ())), preferred_element_type=jnp.float32)
            part = jnp.where(same_half & same_kv, part, 0.0)
            part = part + pltpu.roll(part, 4, 0)
            other = jnp.where(half_col == 0, pltpu.roll(part, n_cols - 2, 1), pltpu.roll(part, 2, 1))
            scores = SOFT_CAP * jnp.tanh((part + other) / SOFT_CAP)
            scores = jnp.where(same_kv & (slot_col <= pos), scores, -1e30)
            weights = jnp.exp(scores - jnp.max(scores, axis=1, keepdims=True))
            total = jnp.sum(jnp.where(same_half, weights, 0.0), axis=1, keepdims=True)
            prob = jnp.where(same_half, weights / total, 0.0).astype(jnp.bfloat16)
            out = jnp.dot(prob, vbuf[slot, i], preferred_element_type=jnp.float32)
            head_ref[row] = out.astype(jnp.bfloat16)
        for copy in writes(step):
            copy.start()

    for step in range(max(n_steps - depth, 0), n_steps):
        for copy in writes(step):
            copy.wait()


def attend(q_new, k_new, v_new, positions, k_cache, v_cache):
    n_rows, cache_len, kv_loc, head_dim = k_cache.shape
    halves = head_dim // LANES
    group_size = q_new.shape[1] // kv_loc
    depth = 6

    def flat(cache):
        return cache.reshape(n_rows, cache_len, kv_loc, halves, LANES).transpose(0, 1, 3, 2, 4).reshape(n_rows, cache_len * halves * kv_loc, LANES)

    def unflat(cache):
        return cache.reshape(n_rows, cache_len, halves, kv_loc, LANES).transpose(0, 1, 3, 2, 4).reshape(n_rows, cache_len, kv_loc, head_dim)

    def fresh(new):
        return jnp.tile(new.reshape(n_rows, kv_loc, halves, LANES).transpose(0, 2, 1, 3).reshape(n_rows, halves * kv_loc, LANES), (1, 4, 1))

    q_rows = q_new.reshape(n_rows, kv_loc, group_size, halves, LANES).transpose(0, 3, 1, 2, 4).reshape(n_rows, -1, LANES)
    vmem, hbm = pl.BlockSpec(memory_space=pltpu.VMEM), pl.BlockSpec(memory_space=pl.ANY)
    k_flat, v_flat = flat(k_cache), flat(v_cache)
    block = (depth, STEP_ROWS) + k_flat.shape[1:]
    n_bytes = 4 * k_flat.size * 2
    heads, k_out, v_out = pl.pallas_call(
        functools.partial(attend_kernel, cache_len, n_rows, depth),
        out_shape=(jax.ShapeDtypeStruct(q_rows.shape, jnp.bfloat16), jax.ShapeDtypeStruct(k_flat.shape, jnp.bfloat16), jax.ShapeDtypeStruct(v_flat.shape, jnp.bfloat16)),
        in_specs=[pl.BlockSpec(memory_space=pltpu.SMEM), vmem, vmem, vmem, hbm, hbm],
        out_specs=(vmem, hbm, hbm),
        scratch_shapes=[pltpu.VMEM(block, jnp.bfloat16), pltpu.VMEM(block, jnp.bfloat16), pltpu.SemaphoreType.DMA((2, depth)), pltpu.SemaphoreType.DMA((2, depth))],
        compiler_params=pltpu.CompilerParams(vmem_limit_bytes=60 * 2**20),
        cost_estimate=pl.CostEstimate(flops=n_rows * 8 * cache_len * 4 * LANES * 4, bytes_accessed=n_bytes, transcendentals=0),
        name=f"attend_{cache_len}",
    )(positions, q_rows, fresh(k_new), fresh(v_new), k_flat, v_flat)
    head_out = heads.reshape(n_rows, halves, kv_loc * group_size, LANES).transpose(0, 2, 1, 3).reshape(n_rows, kv_loc * group_size, head_dim)
    return head_out, unflat(k_out), unflat(v_out)


def width_norm(hidden, gain, width):
    sum_sq = lax.psum(jnp.sum(jnp.square(hidden), axis=-1, keepdims=True), "data")
    return hidden * lax.rsqrt(sum_sq / width + NORM_EPS) * (1.0 + gain.astype(jnp.float32))


def layer_block(hidden, positions, k_cache, v_cache, weights, layer):
    w_q, w_k, w_v, w_o, w_gate, w_up, w_down, norm_gains = weights
    share = hidden.shape[1]
    n_data = lax.axis_size("data")
    width = share * n_data
    gains = lax.dynamic_slice_in_dim(norm_gains[layer], lax.axis_index("data") * share, share, axis=1)
    n_q, head_dim = w_q.shape[2:]
    n_kv = w_k.shape[2]
    residual = hidden.astype(jnp.float32)
    normed = width_norm(residual, gains[0], width).astype(jnp.bfloat16)
    w_in = jnp.concatenate([w_q[layer].reshape(share, -1), w_k[layer].reshape(share, -1), w_v[layer].reshape(share, -1)], axis=1)
    qkv = jnp.dot(normed, w_in, preferred_element_type=jnp.float32)
    qkv = lax.psum_scatter(qkv, "data", scatter_dimension=0, tiled=True)
    n_rows = qkv.shape[0]
    q_proj = qkv[:, :n_q * head_dim].reshape(n_rows, n_q, head_dim)
    k_proj = qkv[:, n_q * head_dim:(n_q + n_kv) * head_dim].reshape(n_rows, n_kv, head_dim)
    v_proj = qkv[:, (n_q + n_kv) * head_dim:].reshape(n_rows, n_kv, head_dim)
    cos_t, sin_t = rope_tables(positions, head_dim)
    q_new = (rotary(q_proj, cos_t, sin_t) * head_dim ** -0.5).astype(jnp.bfloat16)
    k_new = rotary(k_proj, cos_t, sin_t).astype(jnp.bfloat16)
    head_out, k_cache, v_cache = attend(q_new, k_new, v_proj.astype(jnp.bfloat16), positions, k_cache, v_cache)
    heads_all = lax.all_gather(head_out.reshape(n_rows, -1), "data", axis=0, tiled=True)
    attn_sum = lax.psum(jnp.dot(heads_all, w_o[layer].reshape(-1, share), preferred_element_type=jnp.float32), "model")
    mid_hidden = (residual + width_norm(attn_sum, gains[1], width)).astype(jnp.bfloat16)
    mid_f = mid_hidden.astype(jnp.float32)
    normed_ff = width_norm(mid_f, gains[2], width).astype(jnp.bfloat16)
    gate_proj = jnp.dot(normed_ff, w_gate[layer], preferred_element_type=jnp.float32)
    gate_proj = lax.psum_scatter(gate_proj, "data", scatter_dimension=0, tiled=True)
    up_proj = jnp.dot(normed_ff, w_up[layer], preferred_element_type=jnp.float32)
    up_proj = lax.psum_scatter(up_proj, "data", scatter_dimension=0, tiled=True)
    gated_act = (jax.nn.gelu(gate_proj, approximate=True) * up_proj).astype(jnp.bfloat16)
    acts_all = lax.all_gather(gated_act, "data", axis=0, tiled=True)
    down_sum = lax.psum(jnp.dot(acts_all, w_down[layer], preferred_element_type=jnp.float32), "model")
    return (mid_f + width_norm(down_sum, gains[3], width)).astype(jnp.bfloat16), k_cache, v_cache


def solution(mesh):
    def device_step(hidden, positions, k_local, v_local, k_global, v_global, w_q, w_k, w_v, w_o, w_gate, w_up, w_down, norm_gains):
        weights = (w_q, w_k, w_v, w_o, w_gate, w_up, w_down, norm_gains)
        hidden_cols = lax.all_to_all(hidden[:, 0, :], "data", 1, 0, tiled=True)
        hidden_cols, k_local, v_local = layer_block(hidden_cols, positions, k_local, v_local, weights, 0)
        hidden_cols, k_global, v_global = layer_block(hidden_cols, positions, k_global, v_global, weights, 1)
        final = lax.all_to_all(hidden_cols, "data", 0, 1, tiled=True)[:, None, :]
        return final, k_local, v_local, k_global, v_global

    in_specs = (ROW_SPEC, POS_SPEC, CACHE_SPEC, CACHE_SPEC, CACHE_SPEC, CACHE_SPEC, PROJ_IN_SPEC, PROJ_IN_SPEC, PROJ_IN_SPEC, PROJ_OUT_SPEC, FF_IN_SPEC, FF_IN_SPEC, FF_OUT_SPEC, GAIN_SPEC)
    out_specs = (ROW_SPEC, CACHE_SPEC, CACHE_SPEC, CACHE_SPEC, CACHE_SPEC)
    return jax.shard_map(device_step, mesh=mesh, in_specs=in_specs, out_specs=out_specs, check_vma=False)
```

```python
import functools

import jax
import jax.numpy as jnp
from jax import lax
from jax.experimental import pallas as pl
from jax.experimental.pallas import tpu as pltpu
from jax.sharding import PartitionSpec as P

SOFT_CAP = 50.0
NORM_EPS = 1e-6
ROPE_BASE = 10000.0

ROW_SPEC = P(("part", "data"), None, None)
POS_SPEC = P(("part", "data"))
CACHE_SPEC = P(("part", "data"), None, "model", None)
PROJ_IN_SPEC = P(None, "data", "model", None)
PROJ_OUT_SPEC = P(None, "model", None, "data")
FF_IN_SPEC = P(None, "data", "model")
FF_OUT_SPEC = P(None, "model", "data")
GAIN_SPEC = P(None, None, None)


def rotary(hidden, cos_t, sin_t):
    half_dim = hidden.shape[-1] // 2
    first_half = hidden[..., :half_dim]
    second_half = hidden[..., half_dim:]
    return jnp.concatenate([first_half * cos_t - second_half * sin_t, second_half * cos_t + first_half * sin_t], axis=-1)


def rope_tables(positions, head_dim):
    inv_freq = ROPE_BASE ** (-jnp.arange(0, head_dim, 2).astype(jnp.float32) / head_dim)
    angles = positions.astype(jnp.float32)[:, None] * inv_freq[None, :]
    return jnp.cos(angles)[:, None, :], jnp.sin(angles)[:, None, :]


LANES = 128
STEP_ROWS = 4


def attend_kernel(cache_len, n_rows, depth, pos_ref, q_ref, kn_ref, vn_ref, k_hbm, v_hbm, head_ref, ko_hbm, vo_hbm, kbuf, vbuf, rd_sem, wr_sem):
    n_steps = n_rows // STEP_ROWS
    n_cols = cache_len * 4

    def reads(step):
        slot = lax.rem(step, depth)
        rows = pl.ds(step * STEP_ROWS, STEP_ROWS)
        return (pltpu.make_async_copy(k_hbm.at[rows], kbuf.at[slot], rd_sem.at[0, slot]),
                pltpu.make_async_copy(v_hbm.at[rows], vbuf.at[slot], rd_sem.at[1, slot]))

    def writes(step):
        slot = lax.rem(step, depth)
        rows = pl.ds(step * STEP_ROWS, STEP_ROWS)
        return (pltpu.make_async_copy(kbuf.at[slot], ko_hbm.at[rows], wr_sem.at[0, slot]),
                pltpu.make_async_copy(vbuf.at[slot], vo_hbm.at[rows], wr_sem.at[1, slot]))

    ahead = depth - 2
    for step in range(ahead):
        for copy in reads(step):
            copy.start()

    row_id = lax.broadcasted_iota(jnp.int32, (8, n_cols), 0)
    col_id = lax.broadcasted_iota(jnp.int32, (8, n_cols), 1)
    half_row, kv_row = row_id // 4, (row_id // 2) % 2
    half_col, kv_col, slot_col = (col_id // 2) % 2, col_id % 2, col_id // 4
    same_half, same_kv = half_row == half_col, kv_row == kv_col
    sub_id = lax.broadcasted_iota(jnp.int32, (16, LANES), 0) // 4

    @pl.loop(0, n_steps)
    def _(step):
        slot = lax.rem(step, depth)

        @pl.when(step + ahead < n_steps)
        def _():
            @pl.when(step >= 2)
            def _():
                for copy in writes(step - 2):
                    copy.wait()
            for copy in reads(step + ahead):
                copy.start()

        for copy in reads(step):
            copy.wait()
        for i in range(STEP_ROWS):
            row = step * STEP_ROWS + i
            pos = pos_ref[row]
            now = lax.rem(pos, cache_len)
            window = pl.ds(pl.multiple_of(now // 4 * 16, 16), 16)
            hit = sub_id == lax.rem(now, 4)
            kbuf[slot, i, window, :] = jnp.where(hit, kn_ref[row], kbuf[slot, i, window, :])
            vbuf[slot, i, window, :] = jnp.where(hit, vn_ref[row], vbuf[slot, i, window, :])
        for i in range(STEP_ROWS):
            row = step * STEP_ROWS + i
            pos = pos_ref[row]
            part = lax.dot_general(q_ref[row], kbuf[slot, i], (((1,), (1,)), ((), ())), preferred_element_type=jnp.float32)
            part = jnp.where(same_half & same_kv, part, 0.0)
            part = part + pltpu.roll(part, 4, 0)
            other = jnp.where(half_col == 0, pltpu.roll(part, n_cols - 2, 1), pltpu.roll(part, 2, 1))
            scores = SOFT_CAP * jnp.tanh((part + other) / SOFT_CAP)
            scores = jnp.where(same_kv & (slot_col <= pos), scores, -1e30)
            weights = jnp.exp(scores - jnp.max(scores, axis=1, keepdims=True))
            total = jnp.sum(jnp.where(same_half, weights, 0.0), axis=1, keepdims=True)
            prob = jnp.where(same_half, weights / total, 0.0).astype(jnp.bfloat16)
            out = jnp.dot(prob, vbuf[slot, i], preferred_element_type=jnp.float32)
            head_ref[row] = out.astype(jnp.bfloat16)
        for copy in writes(step):
            copy.start()

    for step in range(max(n_steps - depth, 0), n_steps):
        for copy in writes(step):
            copy.wait()


def attend(q_new, k_new, v_new, positions, k_cache, v_cache):
    n_rows, cache_len, kv_loc, head_dim = k_cache.shape
    halves = head_dim // LANES
    group_size = q_new.shape[1] // kv_loc
    depth = 6

    def flat(cache):
        return cache.reshape(n_rows, cache_len, kv_loc, halves, LANES).transpose(0, 1, 3, 2, 4).reshape(n_rows, cache_len * halves * kv_loc, LANES)

    def unflat(cache):
        return cache.reshape(n_rows, cache_len, halves, kv_loc, LANES).transpose(0, 1, 3, 2, 4).reshape(n_rows, cache_len, kv_loc, head_dim)

    def fresh(new):
        return jnp.tile(new.reshape(n_rows, kv_loc, halves, LANES).transpose(0, 2, 1, 3).reshape(n_rows, halves * kv_loc, LANES), (1, 4, 1))

    q_rows = q_new.reshape(n_rows, kv_loc, group_size, halves, LANES).transpose(0, 3, 1, 2, 4).reshape(n_rows, -1, LANES)
    vmem, hbm = pl.BlockSpec(memory_space=pltpu.VMEM), pl.BlockSpec(memory_space=pl.ANY)
    k_flat, v_flat = flat(k_cache), flat(v_cache)
    block = (depth, STEP_ROWS) + k_flat.shape[1:]
    n_bytes = 4 * k_flat.size * 2
    heads, k_out, v_out = pl.pallas_call(
        functools.partial(attend_kernel, cache_len, n_rows, depth),
        out_shape=(jax.ShapeDtypeStruct(q_rows.shape, jnp.bfloat16), jax.ShapeDtypeStruct(k_flat.shape, jnp.bfloat16), jax.ShapeDtypeStruct(v_flat.shape, jnp.bfloat16)),
        in_specs=[pl.BlockSpec(memory_space=pltpu.SMEM), vmem, vmem, vmem, hbm, hbm],
        out_specs=(vmem, hbm, hbm),
        scratch_shapes=[pltpu.VMEM(block, jnp.bfloat16), pltpu.VMEM(block, jnp.bfloat16), pltpu.SemaphoreType.DMA((2, depth)), pltpu.SemaphoreType.DMA((2, depth))],
        compiler_params=pltpu.CompilerParams(vmem_limit_bytes=60 * 2**20),
        cost_estimate=pl.CostEstimate(flops=n_rows * 8 * cache_len * 4 * LANES * 4, bytes_accessed=n_bytes, transcendentals=0),
        name=f"attend_{cache_len}",
    )(positions, q_rows, fresh(k_new), fresh(v_new), k_flat, v_flat)
    head_out = heads.reshape(n_rows, halves, kv_loc * group_size, LANES).transpose(0, 2, 1, 3).reshape(n_rows, kv_loc * group_size, head_dim)
    return head_out, unflat(k_out), unflat(v_out)


FF_CHUNK = 512
QKV_CHUNK = 512
MESH = pl.DeviceIdType.MESH


def comm_kernel(cfg, *refs):
    it = iter(refs)
    post, layer, rows, share, width = cfg["post"], cfg["layer"], cfg["rows"], cfg["share"], cfg["width"]
    qkv, first, n_ff = cfg["qkv"], cfg["first"], cfg["n_ff"]
    x_ref = next(it)
    g_ref = next(it)
    if post:
        res_ref, wo_hbm, wg_hbm, wu_hbm, wd_hbm = (next(it) for _ in range(5))
    if qkv:
        wi_hbm = next(it)
        hid_ref, qkv_ref = next(it), next(it)
    else:
        out_ref = next(it)
    tcol, st_src, st_rcv, hp, st_ss, st_rs, misc_ss, misc_rs, ld_sem = (next(it) for _ in range(9))
    if post:
        hall, apart, arecv, mpart, mrecv, wo, wg, wu, wd, sib_out, sib_in, mine, x_in, u_all = (next(it) for _ in range(14))
        y_ss, y_rs, ff_ss, ff_rs = (next(it) for _ in range(4))
    if qkv:
        wi, q_out, q_in, q_mine, q_x, q_ss, q_rs = (next(it) for _ in range(7))

    model, me = lax.axis_index("model"), lax.axis_index("data")
    x_pos, core = me // 2, lax.rem(me, 2)
    sib, part, diag = x_pos * 2 + 1 - core, (1 - x_pos) * 2 + core, (1 - x_pos) * 2 + 1 - core
    DIAG, SIB, PART, OWN = (pl.ds(i * rows, rows) for i in range(4))
    sends = []

    def remote(src, dst, send_sem, recv_sem, data=None):
        where = {"data": data} if data is not None else {"model": 1 - model}
        return pltpu.make_async_remote_copy(src_ref=src, dst_ref=dst, send_sem=send_sem, recv_sem=recv_sem, device_id=where, device_id_type=MESH)

    def send(*args):
        copy = remote(*args)
        copy.start()
        sends.append(copy)
        return copy

    loads = []

    def load(src, dst, sem):
        copy = pltpu.make_async_copy(src, dst, sem)
        copy.start()
        return copy

    if post:
        wo_load = load(wo_hbm.at[layer], wo, ld_sem.at[0])
        wg_load = load(wg_hbm.at[layer], wg, ld_sem.at[1])
        wu_load = load(wu_hbm.at[layer], wu, ld_sem.at[2])
        wd_load = load(wd_hbm.at[layer], wd, ld_sem.at[3])
    if qkv:
        wi_load = load(wi_hbm, wi, ld_sem.at[4])

    barrier = pltpu.get_barrier_semaphore()
    for dev in (sib, part, diag):
        pl.semaphore_signal(barrier, inc=1, device_id={"data": dev}, device_id_type=MESH)
    pl.semaphore_signal(barrier, inc=1, device_id={"model": 1 - model}, device_id_type=MESH)
    pl.semaphore_wait(barrier, 4)

    def square_sums(block, value):
        total = None
        for k in range(share // LANES):
            piece = value[:, k * LANES:(k + 1) * LANES]
            total = piece * piece if total is None else total + piece * piece
        tcol[block, :] = total

    def scales(idx):
        own = jnp.sum(jnp.transpose(tcol[...]).reshape(LANES // 8, 8, 4 * rows), axis=0)
        st_src[idx] = own
        copies = [send(st_src.at[idx], st_rcv.at[idx, k], st_ss.at[idx, k], st_rs.at[idx, k], dev) for k, dev in enumerate((sib, part, diag))]
        for copy in copies:
            copy.wait_recv()

        def swap(value):
            return jnp.concatenate([value[:, LANES:], value[:, :LANES]], axis=1)

        def flip(value):
            return jnp.concatenate([pltpu.roll(value[:, :LANES], LANES // 2, 1), pltpu.roll(value[:, LANES:], LANES // 2, 1)], axis=1)

        total = own + swap(st_rcv[idx, 0]) + flip(st_rcv[idx, 1]) + swap(flip(st_rcv[idx, 2]))
        total = jnp.sum(total, axis=0, keepdims=True)
        inverse = lax.rsqrt(total / width + NORM_EPS)
        tcol[...] = jnp.transpose(jnp.broadcast_to(inverse, (LANES, 4 * rows)))

    def scaled(block, value, gain):
        return value * jnp.concatenate([tcol[block, :]] * (share // LANES), axis=1) * g_ref[gain:gain + 1, :]

    blocks = (OWN, SIB, PART, DIAG)
    if first:
        for k, (dev, there) in enumerate(((sib, SIB), (part, PART), (diag, DIAG))):
            cols = pl.ds(pl.multiple_of(dev * share, LANES), share)
            send(x_ref.at[:, cols], hid_ref.at[there, :], misc_ss.at[k], misc_rs.at[k], dev)
        hid_ref[OWN, :] = x_ref[:, pl.ds(pl.multiple_of(me * share, LANES), share)]
        square_sums(OWN, hid_ref[OWN, :].astype(jnp.float32))
        for copy, block in zip(list(sends), (SIB, PART, DIAG)):
            copy.wait_recv()
            square_sums(block, hid_ref[block, :].astype(jnp.float32))
    if post:
        to_part = send(x_ref, hall.at[PART, :], misc_ss.at[0], misc_rs.at[0], part)
        to_sib = send(x_ref, hall.at[SIB, :], misc_ss.at[1], misc_rs.at[1], sib)
        wo_load.wait()
        y_copies = []
        for k, block in enumerate(blocks):
            if k == 1:
                to_sib.wait_recv()
            if k == 2:
                to_part.wait_recv()
                forward = send(hall.at[PART, :], hall.at[DIAG, :], misc_ss.at[2], misc_rs.at[2], sib)
            if k == 3:
                forward.wait_recv()
            heads = x_ref[...] if k == 0 else hall[block, :]
            apart[block, :] = jnp.dot(heads, wo[...], preferred_element_type=jnp.float32)
            y_copies.append(send(apart.at[block, :], arecv.at[block, :], y_ss.at[k], y_rs.at[k]))
        for copy, block in zip(y_copies, blocks):
            copy.wait_recv()
            total = apart[block, :] + arecv[block, :]
            arecv[block, :] = total
            square_sums(block, total)
        scales(0)
        for block in blocks:
            mid = (res_ref[block, :].astype(jnp.float32) + scaled(block, arecv[block, :], 0)).astype(jnp.bfloat16).astype(jnp.float32)
            arecv[block, :] = mid
            mpart[block, :] = jnp.zeros((rows, share), jnp.float32)
        for block in blocks:
            square_sums(block, arecv[block, :])
        scales(1)
        for block in blocks:
            hp[block, :] = scaled(block, arecv[block, :], 1).astype(jnp.bfloat16)
        wg_load.wait()
        wu_load.wait()

        def to_sibling(c):
            return remote(sib_out.at[c], sib_in.at[c], ff_ss.at[0, c], ff_rs.at[0, c], sib)

        def to_partner(c):
            return remote(mine.at[c, pl.ds(0, rows)], x_in.at[c], ff_ss.at[1, c], ff_rs.at[1, c], part)

        def act_partner(c):
            return remote(u_all.at[c, OWN], u_all.at[c, PART], ff_ss.at[2, c], ff_rs.at[2, c], part)

        def act_sibling(c):
            return remote(u_all.at[c, OWN], u_all.at[c, SIB], ff_ss.at[3, c], ff_rs.at[3, c], sib)

        def act_forward(c):
            return remote(u_all.at[c, PART], u_all.at[c, DIAG], ff_ss.at[4, c], ff_rs.at[4, c], sib)

        def add_sibling(c):
            to_sibling(c).wait_recv()
            mine[c] = mine[c] + sib_in[c]
            to_partner(c).start()

        @pl.loop(0, n_ff)
        def _(c):
            cols = pl.ds(pl.multiple_of(c * FF_CHUNK, FF_CHUNK), FF_CHUNK)
            for k, weight in enumerate((wg, wu)):
                sums = jnp.dot(hp[...], weight[:, cols], preferred_element_type=jnp.float32)
                sib_out[c, :, pl.ds(k * FF_CHUNK, FF_CHUNK)] = sums[:2 * rows]
                mine[c, :, pl.ds(k * FF_CHUNK, FF_CHUNK)] = sums[2 * rows:]
            to_sibling(c).start()

            @pl.when(c >= 1)
            def _():
                add_sibling(c - 1)

        add_sibling(n_ff - 1)

        @pl.loop(0, n_ff)
        def _(c):
            to_partner(c).wait_recv()
            both = mine[c, pl.ds(rows, rows), :] + x_in[c]
            u_all[c, OWN, :] = (jax.nn.gelu(both[:, :FF_CHUNK], approximate=True) * both[:, FF_CHUNK:]).astype(jnp.bfloat16)
            act_partner(c).start()
            act_sibling(c).start()

        wd_load.wait()

        def down(c):
            act_sibling(c).wait_recv()
            act_forward(c).wait_recv()
            deep = pl.ds(pl.multiple_of(c * FF_CHUNK, FF_CHUNK), FF_CHUNK)
            mpart[...] += jnp.dot(u_all[c], wd[deep, :], preferred_element_type=jnp.float32)

        @pl.loop(0, n_ff)
        def _(c):
            act_partner(c).wait_recv()
            act_forward(c).start()

            @pl.when(c >= 1)
            def _():
                down(c - 1)

        down(n_ff - 1)
        y_copies = [send(mpart.at[block, :], mrecv.at[block, :], y_ss.at[4 + k], y_rs.at[4 + k]) for k, block in enumerate(blocks)]
        for copy, block in zip(y_copies, blocks):
            copy.wait_recv()
            total = mpart[block, :] + mrecv[block, :]
            mrecv[block, :] = total
            square_sums(block, total)
        scales(2)
        for block in blocks:
            value = (arecv[block, :] + scaled(block, mrecv[block, :], 2)).astype(jnp.bfloat16)
            if qkv:
                hid_ref[block, :] = value
            else:
                hp[block, :] = value
        if qkv:
            for block in blocks:
                square_sums(block, hid_ref[block, :].astype(jnp.float32))

        @pl.loop(0, n_ff)
        def _(c):
            for copy in (to_sibling(c), to_partner(c), act_partner(c), act_sibling(c), act_forward(c)):
                copy.wait_send()
    if qkv:
        scales(3)
        for block in blocks:
            hp[block, :] = scaled(block, hid_ref[block, :].astype(jnp.float32), 3).astype(jnp.bfloat16)
        wi_load.wait()
        n_q = wi.shape[1] // QKV_CHUNK

        def q_partner(c):
            return remote(q_mine.at[c, pl.ds(0, rows)], q_x.at[c], q_ss.at[1, c], q_rs.at[1, c], part)

        for c in range(n_q):
            sums = jnp.dot(hp[...], wi[:, c * QKV_CHUNK:(c + 1) * QKV_CHUNK], preferred_element_type=jnp.float32)
            q_out[c] = sums[:2 * rows]
            q_mine[c] = sums[2 * rows:]
            copy = send(q_out.at[c], q_in.at[c], q_ss.at[0, c], q_rs.at[0, c], sib)
            if c >= 1:
                before.wait_recv()
                q_mine[c - 1] = q_mine[c - 1] + q_in[c - 1]
                q_partner(c - 1).start()
            before = copy
        before.wait_recv()
        q_mine[n_q - 1] = q_mine[n_q - 1] + q_in[n_q - 1]
        q_partner(n_q - 1).start()
        for c in range(n_q):
            q_partner(c).wait_recv()
            qkv_ref[:, c * QKV_CHUNK:(c + 1) * QKV_CHUNK] = q_mine[c, pl.ds(rows, rows), :] + q_x[c]
        for c in range(n_q):
            q_partner(c).wait_send()
    else:
        here = pl.ds(pl.multiple_of(me * share, LANES), share)
        out_copies = [send(hp.at[block, :], out_ref.at[:, here], misc_ss.at[3 + k], misc_rs.at[3 + k], dev)
                      for k, (dev, block) in enumerate(((sib, SIB), (part, PART), (diag, DIAG)))]
        out_ref[:, here] = hp[OWN, :]
        for dev, copy in zip((sib, part, diag), out_copies):
            copy.wait_recv()
    for copy in sends:
        copy.wait_send()


def comm(x, gains, qkv_weight=None, post=None, layer=0, collective_id=0):
    rows = x.shape[0]
    share = gains.shape[1]
    n_rows = rows * 4
    f32, bf16, vmem, hbm = jnp.float32, jnp.bfloat16, pl.BlockSpec(memory_space=pltpu.VMEM), pl.BlockSpec(memory_space=pl.ANY)
    dma = pltpu.SemaphoreType.DMA
    args, specs = [x, gains], [vmem, vmem]
    scratch = [pltpu.VMEM((n_rows, LANES), f32), pltpu.VMEM((4, 8, n_rows), f32), pltpu.VMEM((4, 3, 8, n_rows), f32), pltpu.VMEM((n_rows, share), bf16),
               dma((4, 3)), dma((4, 3)), dma((6,)), dma((6,)), dma((5,))]
    n_ff = 0
    if post is not None:
        residual, w_o, w_gate, w_up, w_down = post
        args += list(post)
        specs += [vmem, hbm, hbm, hbm, hbm]
        ff = w_gate.shape[2]
        n_ff = ff // FF_CHUNK
        scratch += [pltpu.VMEM((n_rows, w_o.shape[1]), bf16)] + [pltpu.VMEM((n_rows, share), f32)] * 4
        scratch += [pltpu.VMEM(w_o.shape[1:], bf16), pltpu.VMEM((share, ff), bf16), pltpu.VMEM((share, ff), bf16), pltpu.VMEM((ff, share), bf16)]
        scratch += [pltpu.VMEM((n_ff, 2 * rows, 2 * FF_CHUNK), f32)] * 3 + [pltpu.VMEM((n_ff, rows, 2 * FF_CHUNK), f32), pltpu.VMEM((n_ff, n_rows, FF_CHUNK), bf16)]
        scratch += [dma((8,)), dma((8,)), dma((5, n_ff)), dma((5, n_ff))]
    if qkv_weight is not None:
        args.append(qkv_weight)
        specs.append(hbm)
        n_q = qkv_weight.shape[1] // QKV_CHUNK
        scratch += [pltpu.VMEM(qkv_weight.shape, bf16)] + [pltpu.VMEM((n_q, 2 * rows, QKV_CHUNK), f32)] * 3 + [pltpu.VMEM((n_q, rows, QKV_CHUNK), f32), dma((2, n_q)), dma((2, n_q))]
        out_shape = (jax.ShapeDtypeStruct((n_rows, share), bf16), jax.ShapeDtypeStruct((rows, qkv_weight.shape[1]), f32))
        out_specs = (vmem, vmem)
    else:
        out_shape = jax.ShapeDtypeStruct((rows, 4 * share), bf16)
        out_specs = vmem
    cfg = {"post": post is not None, "qkv": qkv_weight is not None, "first": post is None, "layer": layer, "rows": rows, "share": share, "width": 4 * share, "n_ff": n_ff}
    return pl.pallas_call(
        functools.partial(comm_kernel, cfg),
        out_shape=out_shape, in_specs=specs, out_specs=out_specs, scratch_shapes=scratch,
        compiler_params=pltpu.CompilerParams(collective_id=collective_id, has_side_effects=True, vmem_limit_bytes=(62 if post is not None else 20) * 2**20),
        name=f"comm_{collective_id}",
    )(*args)


def attention(qkv, positions, k_cache, v_cache, n_q):
    n_rows = qkv.shape[0]
    n_kv, head_dim = k_cache.shape[2:]
    q_proj = qkv[:, :n_q * head_dim].reshape(n_rows, n_q, head_dim)
    k_proj = qkv[:, n_q * head_dim:(n_q + n_kv) * head_dim].reshape(n_rows, n_kv, head_dim)
    v_proj = qkv[:, (n_q + n_kv) * head_dim:].reshape(n_rows, n_kv, head_dim)
    cos_t, sin_t = rope_tables(positions, head_dim)
    q_new = (rotary(q_proj, cos_t, sin_t) * head_dim ** -0.5).astype(jnp.bfloat16)
    k_new = rotary(k_proj, cos_t, sin_t).astype(jnp.bfloat16)
    head_out, k_cache, v_cache = attend(q_new, k_new, v_proj.astype(jnp.bfloat16), positions, k_cache, v_cache)
    return head_out.reshape(n_rows, -1), k_cache, v_cache


def solution(mesh):
    def device_step(hidden, positions, k_local, v_local, k_global, v_global, w_q, w_k, w_v, w_o, w_gate, w_up, w_down, norm_gains):
        share = w_q.shape[1]
        n_q = w_q.shape[2]
        gains = 1.0 + lax.dynamic_slice_in_dim(norm_gains, lax.axis_index("data") * share, share, axis=2).astype(jnp.float32)
        in_weights = [jnp.concatenate([w[layer].reshape(share, -1) for w in (w_q, w_k, w_v)], axis=1) for layer in range(2)]
        out_weights = w_o.reshape(2, -1, share)
        first_gains = jnp.concatenate([gains[0, 1:], gains[0, :1]], axis=0)
        mid_gains = jnp.concatenate([gains[0, 1:], gains[1, :1]], axis=0)
        last_gains = jnp.concatenate([gains[1, 1:], gains[1, :1]], axis=0)
        residual, qkv = comm(hidden[:, 0, :], first_gains, in_weights[0], collective_id=0)
        heads, k_local, v_local = attention(qkv, positions, k_local, v_local, n_q)
        residual, qkv = comm(heads, mid_gains, in_weights[1], (residual, out_weights, w_gate, w_up, w_down), layer=0, collective_id=1)
        heads, k_global, v_global = attention(qkv, positions, k_global, v_global, n_q)
        final = comm(heads, last_gains, None, (residual, out_weights, w_gate, w_up, w_down), layer=1, collective_id=2)[:, None, :]
        return final, k_local, v_local, k_global, v_global

    in_specs = (ROW_SPEC, POS_SPEC, CACHE_SPEC, CACHE_SPEC, CACHE_SPEC, CACHE_SPEC, PROJ_IN_SPEC, PROJ_IN_SPEC, PROJ_IN_SPEC, PROJ_OUT_SPEC, FF_IN_SPEC, FF_IN_SPEC, FF_OUT_SPEC, GAIN_SPEC)
    out_specs = (ROW_SPEC, CACHE_SPEC, CACHE_SPEC, CACHE_SPEC, CACHE_SPEC)
    return jax.shard_map(device_step, mesh=mesh, in_specs=in_specs, out_specs=out_specs, check_vma=False)
```

```python
import functools

import jax
import jax.numpy as jnp
from jax import lax
from jax.experimental import pallas as pl
from jax.experimental.pallas import tpu as pltpu
from jax.sharding import PartitionSpec as P

SOFT_CAP = 50.0
NORM_EPS = 1e-6
ROPE_BASE = 10000.0

ROW_SPEC = P(("part", "data"), None, None)
POS_SPEC = P(("part", "data"))
CACHE_SPEC = P(("part", "data"), None, "model", None)
PROJ_IN_SPEC = P(None, "data", "model", None)
PROJ_OUT_SPEC = P(None, "model", None, "data")
FF_IN_SPEC = P(None, "data", "model")
FF_OUT_SPEC = P(None, "model", "data")
GAIN_SPEC = P(None, None, None)


def rope_tables(positions, head_dim):
    inv_freq = ROPE_BASE ** (-jnp.arange(0, head_dim, 2).astype(jnp.float32) / head_dim)
    angles = positions.astype(jnp.float32)[:, None] * inv_freq[None, :]
    return jnp.cos(angles), jnp.sin(angles)


LANES = 128


def attend_kernel(cache_len, n_rows, group, depth, pos_ref, qkv_ref, cos_ref, sin_ref, k_hbm, v_hbm, head_ref, ko_hbm, vo_hbm, kbuf, vbuf, q8, kn, vn, outs, sbuf, pbuf, rd_sem, wr_sem):
    n_steps = n_rows // group
    n_cols = cache_len * 4

    def reads(step):
        slot = lax.rem(step, depth)
        rows = pl.ds(step * group, group)
        return (pltpu.make_async_copy(k_hbm.at[rows], kbuf.at[slot], rd_sem.at[0, slot]),
                pltpu.make_async_copy(v_hbm.at[rows], vbuf.at[slot], rd_sem.at[1, slot]))

    def writes(step):
        slot = lax.rem(step, depth)
        rows = pl.ds(step * group, group)
        return (pltpu.make_async_copy(kbuf.at[slot], ko_hbm.at[rows], wr_sem.at[0, slot]),
                pltpu.make_async_copy(vbuf.at[slot], vo_hbm.at[rows], wr_sem.at[1, slot]))

    ahead = max(depth - 2, 1) if depth < n_steps else n_steps
    for step in range(ahead):
        for copy in reads(step):
            copy.start()

    cos_t, sin_t = cos_ref[...], sin_ref[...]
    scale = (2 * LANES) ** -0.5
    for h in range(4):
        first, second = qkv_ref[:, h * 256:h * 256 + LANES], qkv_ref[:, h * 256 + LANES:h * 256 + 256]
        q8[:, h, :] = (first * cos_t - second * sin_t) * scale
        q8[:, 4 + h, :] = (second * cos_t + first * sin_t) * scale
    for h in range(2):
        base = 1024 + h * 256
        first, second = qkv_ref[:, base:base + LANES], qkv_ref[:, base + LANES:base + 256]
        halves = (first * cos_t - second * sin_t, second * cos_t + first * sin_t)
        for half in range(2):
            value = qkv_ref[:, base + 512 + half * LANES:base + 512 + (half + 1) * LANES]
            for i in range(4):
                kn[:, i * 4 + half * 2 + h, :] = halves[half]
                vn[:, i * 4 + half * 2 + h, :] = value

    row_id = lax.broadcasted_iota(jnp.int32, (8, n_cols), 0)
    col_id = lax.broadcasted_iota(jnp.int32, (8, n_cols), 1)
    half_col = (col_id // 2) % 2
    same_half = row_id // 4 == half_col
    same_kv = (row_id // 2) % 2 == col_id % 2
    slot_col = col_id // 4
    sub_id = lax.broadcasted_iota(jnp.int32, (16, LANES), 0) // 4

    @pl.loop(0, n_steps)
    def _(step):
        slot = lax.rem(step, depth)
        if ahead < n_steps:
            @pl.when(step + ahead < n_steps)
            def _():
                @pl.when(step >= depth - ahead)
                def _():
                    for copy in writes(step - (depth - ahead)):
                        copy.wait()
                for copy in reads(step + ahead):
                    copy.start()

        for copy in reads(step):
            copy.wait()
        for i in range(group):
            row = step * group + i
            now = lax.rem(pos_ref[row], cache_len)
            window = pl.ds(pl.multiple_of(now // 4 * 16, 16), 16)
            hit = sub_id == lax.rem(now, 4)
            kbuf[slot, i, window, :] = jnp.where(hit, kn[row].astype(jnp.bfloat16), kbuf[slot, i, window, :])
            vbuf[slot, i, window, :] = jnp.where(hit, vn[row].astype(jnp.bfloat16), vbuf[slot, i, window, :])
        for i in range(group):
            part = lax.dot_general(q8[step * group + i].astype(jnp.bfloat16), kbuf[slot, i], (((1,), (1,)), ((), ())), preferred_element_type=jnp.float32)
            sbuf[i] = jnp.where(same_half & same_kv, part, 0.0)
        for i in range(group):
            part = sbuf[i]
            part = part + pltpu.roll(part, 4, 0)
            other = jnp.where(half_col == 0, pltpu.roll(part, n_cols - 2, 1), pltpu.roll(part, 2, 1))
            scores = SOFT_CAP * jnp.tanh((part + other) / SOFT_CAP)
            scores = jnp.where(same_kv & (slot_col <= pos_ref[step * group + i]), scores, -1e30)
            weights = jnp.exp(scores - jnp.max(scores, axis=1, keepdims=True))
            total = jnp.sum(jnp.where(same_half, weights, 0.0), axis=1, keepdims=True)
            pbuf[i] = jnp.where(same_half, weights / total, 0.0).astype(jnp.bfloat16)
        for i in range(group):
            outs[step * group + i] = jnp.dot(pbuf[i], vbuf[slot, i], preferred_element_type=jnp.float32)
        for copy in writes(step):
            copy.start()

    for h in range(4):
        for half in range(2):
            head_ref[:, h * 256 + half * LANES:h * 256 + (half + 1) * LANES] = outs[:, half * 4 + h, :].astype(jnp.bfloat16)
    for step in range(max(n_steps - depth, 0) if ahead < n_steps else 0, n_steps):
        for copy in writes(step):
            copy.wait()


def attend(qkv, tables, positions, k_cache, v_cache):
    n_rows, cache_len, kv_loc, head_dim = k_cache.shape
    halves = head_dim // LANES
    group = 16 if cache_len <= 64 else 4
    depth = 4 if cache_len <= 64 else 6
    f32, bf16 = jnp.float32, jnp.bfloat16

    def flat(cache):
        return cache.reshape(n_rows, cache_len, kv_loc, halves, LANES).transpose(0, 1, 3, 2, 4).reshape(n_rows, cache_len * halves * kv_loc, LANES)

    def unflat(cache):
        return cache.reshape(n_rows, cache_len, halves, kv_loc, LANES).transpose(0, 1, 3, 2, 4).reshape(n_rows, cache_len, kv_loc, head_dim)

    vmem, hbm = pl.BlockSpec(memory_space=pltpu.VMEM), pl.BlockSpec(memory_space=pl.ANY)
    k_flat, v_flat = flat(k_cache), flat(v_cache)
    n_cols = k_flat.shape[1]
    block = (depth, group, n_cols, LANES)
    dma = pltpu.SemaphoreType.DMA
    heads, k_out, v_out = pl.pallas_call(
        functools.partial(attend_kernel, cache_len, n_rows, group, depth),
        out_shape=(jax.ShapeDtypeStruct((n_rows, 4 * head_dim), bf16), jax.ShapeDtypeStruct(k_flat.shape, bf16), jax.ShapeDtypeStruct(v_flat.shape, bf16)),
        in_specs=[pl.BlockSpec(memory_space=pltpu.SMEM), vmem, vmem, vmem, hbm, hbm],
        out_specs=(vmem, hbm, hbm),
        scratch_shapes=[pltpu.VMEM(block, bf16), pltpu.VMEM(block, bf16), pltpu.VMEM((n_rows, 8, LANES), f32), pltpu.VMEM((n_rows, 16, LANES), f32),
                        pltpu.VMEM((n_rows, 16, LANES), f32), pltpu.VMEM((n_rows, 8, LANES), f32), pltpu.VMEM((group, 8, n_cols), f32), pltpu.VMEM((group, 8, n_cols), bf16),
                        dma((2, depth)), dma((2, depth))],
        compiler_params=pltpu.CompilerParams(vmem_limit_bytes=(32 if cache_len <= 64 else 48) * 2**20),
        cost_estimate=pl.CostEstimate(flops=n_rows * 8 * n_cols * LANES * 4, bytes_accessed=4 * k_flat.size * 2, transcendentals=0),
        name=f"attend_{cache_len}",
    )(positions, qkv, *tables, k_flat, v_flat)
    return heads, unflat(k_out), unflat(v_out)


FF_CHUNK = 512
QKV_CHUNK = 512
MESH = pl.DeviceIdType.MESH


def comm_kernel(cfg, *refs):
    it = iter(refs)
    post, layer, rows, share, width = cfg["post"], cfg["layer"], cfg["rows"], cfg["share"], cfg["width"]
    qkv, first, n_ff = cfg["qkv"], cfg["first"], cfg["n_ff"]
    x_ref = next(it)
    g_ref = next(it)
    if post:
        res_ref, wo_hbm, wg_hbm, wu_hbm, wd_hbm = (next(it) for _ in range(5))
    if qkv:
        wq_hbm, wk_hbm, wv_hbm = (next(it) for _ in range(3))
        hid_ref, qkv_ref = next(it), next(it)
    else:
        out_ref = next(it)
    tcol, st_src, st_rcv, hp, st_ss, st_rs, misc_ss, misc_rs, ld_sem = (next(it) for _ in range(9))
    if post:
        hall, apart, arecv, mpart, mrecv, wo, wg, wu, wd, sib_out, sib_in, mine, x_in, u_all = (next(it) for _ in range(14))
        y_ss, y_rs, ff_ss, ff_rs = (next(it) for _ in range(4))
    if qkv:
        wi, wq, wk, wv, q_out, q_in, q_mine, q_x, q_ss, q_rs = (next(it) for _ in range(10))

    model, me = lax.axis_index("model"), lax.axis_index("data")
    x_pos, core = me // 2, lax.rem(me, 2)
    sib, part, diag = x_pos * 2 + 1 - core, (1 - x_pos) * 2 + core, (1 - x_pos) * 2 + 1 - core
    DIAG, SIB, PART, OWN = (pl.ds(i * rows, rows) for i in range(4))
    sends = []

    def remote(src, dst, send_sem, recv_sem, data=None):
        where = {"data": data} if data is not None else {"model": 1 - model}
        return pltpu.make_async_remote_copy(src_ref=src, dst_ref=dst, send_sem=send_sem, recv_sem=recv_sem, device_id=where, device_id_type=MESH)

    def send(*args):
        copy = remote(*args)
        copy.start()
        sends.append(copy)
        return copy

    loads = []

    def load(src, dst, sem):
        copy = pltpu.make_async_copy(src, dst, sem)
        copy.start()
        return copy

    if post:
        wo_load = load(wo_hbm.at[layer], wo, ld_sem.at[0])
        wg_load = load(wg_hbm.at[layer], wg, ld_sem.at[1])
        wu_load = load(wu_hbm.at[layer], wu, ld_sem.at[2])
        wd_load = load(wd_hbm.at[layer], wd, ld_sem.at[3])
    if qkv:
        in_loads = [load(src.at[layer + 1], dst, ld_sem.at[4 + k]) for k, (src, dst) in enumerate(((wq_hbm, wq), (wk_hbm, wk), (wv_hbm, wv)))]

    def relay_weights():
        col = 0
        for copy, weight in zip(in_loads, (wq, wk, wv)):
            copy.wait()
            n_heads, head_dim = weight.shape[1:]
            for h in range(n_heads):
                wi[:, col:col + head_dim] = weight[:, h, :]
                col += head_dim

    barrier = pltpu.get_barrier_semaphore()
    for dev in (sib, part, diag):
        pl.semaphore_signal(barrier, inc=1, device_id={"data": dev}, device_id_type=MESH)
    pl.semaphore_signal(barrier, inc=1, device_id={"model": 1 - model}, device_id_type=MESH)
    pl.semaphore_wait(barrier, 4)

    def square_sums(block, value):
        total = None
        for k in range(share // LANES):
            piece = value[:, k * LANES:(k + 1) * LANES]
            total = piece * piece if total is None else total + piece * piece
        tcol[block, :] = total

    def scales(idx):
        own = jnp.sum(jnp.transpose(tcol[...]).reshape(LANES // 8, 8, 4 * rows), axis=0)
        st_src[idx] = own
        copies = [send(st_src.at[idx], st_rcv.at[idx, k], st_ss.at[idx, k], st_rs.at[idx, k], dev) for k, dev in enumerate((sib, part, diag))]
        for copy in copies:
            copy.wait_recv()

        def swap(value):
            return jnp.concatenate([value[:, LANES:], value[:, :LANES]], axis=1)

        def flip(value):
            return jnp.concatenate([pltpu.roll(value[:, :LANES], LANES // 2, 1), pltpu.roll(value[:, LANES:], LANES // 2, 1)], axis=1)

        total = own + swap(st_rcv[idx, 0]) + flip(st_rcv[idx, 1]) + swap(flip(st_rcv[idx, 2]))
        total = jnp.sum(total, axis=0, keepdims=True)
        inverse = lax.rsqrt(total / width + NORM_EPS)
        tcol[...] = jnp.transpose(jnp.broadcast_to(inverse, (LANES, 4 * rows)))

    def gain_row(k):
        at, which = (layer + 1, 0) if k == 3 else (layer, k + 1)
        return 1.0 + g_ref[at, which:which + 1, pl.ds(pl.multiple_of(me * share, LANES), share)].astype(jnp.float32)

    def scaled(block, value, gain):
        return value * jnp.concatenate([tcol[block, :]] * (share // LANES), axis=1) * gain_row(gain)

    blocks = (OWN, SIB, PART, DIAG)
    if first:
        for k, (dev, there) in enumerate(((sib, SIB), (part, PART), (diag, DIAG))):
            cols = pl.ds(pl.multiple_of(dev * share, LANES), share)
            send(x_ref.at[:, cols], hid_ref.at[there, :], misc_ss.at[k], misc_rs.at[k], dev)
        relay_weights()
        hid_ref[OWN, :] = x_ref[:, pl.ds(pl.multiple_of(me * share, LANES), share)]
        square_sums(OWN, hid_ref[OWN, :].astype(jnp.float32))
        for copy, block in zip(list(sends), (SIB, PART, DIAG)):
            copy.wait_recv()
            square_sums(block, hid_ref[block, :].astype(jnp.float32))
    if post:
        to_part = send(x_ref, hall.at[PART, :], misc_ss.at[0], misc_rs.at[0], part)
        to_sib = send(x_ref, hall.at[SIB, :], misc_ss.at[1], misc_rs.at[1], sib)
        wo_load.wait()
        y_copies = []
        for k, block in enumerate(blocks):
            if k == 1:
                to_sib.wait_recv()
            if k == 2:
                to_part.wait_recv()
                forward = send(hall.at[PART, :], hall.at[DIAG, :], misc_ss.at[2], misc_rs.at[2], sib)
            if k == 3:
                forward.wait_recv()
            heads = x_ref[...] if k == 0 else hall[block, :]
            apart[block, :] = jnp.dot(heads, wo[...], preferred_element_type=jnp.float32)
            y_copies.append(send(apart.at[block, :], arecv.at[block, :], y_ss.at[k], y_rs.at[k]))
        for copy, block in zip(y_copies, blocks):
            copy.wait_recv()
            total = apart[block, :] + arecv[block, :]
            arecv[block, :] = total
            square_sums(block, total)
        scales(0)
        for block in blocks:
            mid = (res_ref[block, :].astype(jnp.float32) + scaled(block, arecv[block, :], 0)).astype(jnp.bfloat16).astype(jnp.float32)
            arecv[block, :] = mid
            mpart[block, :] = jnp.zeros((rows, share), jnp.float32)
        for block in blocks:
            square_sums(block, arecv[block, :])
        scales(1)
        for block in blocks:
            hp[block, :] = scaled(block, arecv[block, :], 1).astype(jnp.bfloat16)
        wg_load.wait()
        wu_load.wait()

        def to_sibling(c):
            return remote(sib_out.at[c], sib_in.at[c], ff_ss.at[0, c], ff_rs.at[0, c], sib)

        def to_partner(c):
            return remote(mine.at[c, pl.ds(0, rows)], x_in.at[c], ff_ss.at[1, c], ff_rs.at[1, c], part)

        def act_partner(c):
            return remote(u_all.at[c, OWN], u_all.at[c, PART], ff_ss.at[2, c], ff_rs.at[2, c], part)

        def act_sibling(c):
            return remote(u_all.at[c, OWN], u_all.at[c, SIB], ff_ss.at[3, c], ff_rs.at[3, c], sib)

        def act_forward(c):
            return remote(u_all.at[c, PART], u_all.at[c, DIAG], ff_ss.at[4, c], ff_rs.at[4, c], sib)

        def add_sibling(c):
            to_sibling(c).wait_recv()
            mine[c] = mine[c] + sib_in[c]
            to_partner(c).start()

        @pl.loop(0, n_ff)
        def _(c):
            cols = pl.ds(pl.multiple_of(c * FF_CHUNK, FF_CHUNK), FF_CHUNK)
            for k, weight in enumerate((wg, wu)):
                sums = jnp.dot(hp[...], weight[:, cols], preferred_element_type=jnp.float32)
                sib_out[c, :, pl.ds(k * FF_CHUNK, FF_CHUNK)] = sums[:2 * rows]
                mine[c, :, pl.ds(k * FF_CHUNK, FF_CHUNK)] = sums[2 * rows:]
            to_sibling(c).start()

            @pl.when(c >= 1)
            def _():
                add_sibling(c - 1)

        add_sibling(n_ff - 1)

        @pl.loop(0, n_ff)
        def _(c):
            to_partner(c).wait_recv()
            both = mine[c, pl.ds(rows, rows), :] + x_in[c]
            u_all[c, OWN, :] = (jax.nn.gelu(both[:, :FF_CHUNK], approximate=True) * both[:, FF_CHUNK:]).astype(jnp.bfloat16)
            act_partner(c).start()
            act_sibling(c).start()

        wd_load.wait()
        if qkv:
            relay_weights()

        def down(c):
            act_sibling(c).wait_recv()
            act_forward(c).wait_recv()
            deep = pl.ds(pl.multiple_of(c * FF_CHUNK, FF_CHUNK), FF_CHUNK)
            mpart[...] += jnp.dot(u_all[c], wd[deep, :], preferred_element_type=jnp.float32)

        @pl.loop(0, n_ff)
        def _(c):
            act_partner(c).wait_recv()
            act_forward(c).start()

            @pl.when(c >= 1)
            def _():
                down(c - 1)

        down(n_ff - 1)
        y_copies = [send(mpart.at[block, :], mrecv.at[block, :], y_ss.at[4 + k], y_rs.at[4 + k]) for k, block in enumerate(blocks)]
        for copy, block in zip(y_copies, blocks):
            copy.wait_recv()
            total = mpart[block, :] + mrecv[block, :]
            mrecv[block, :] = total
            square_sums(block, total)
        scales(2)
        for block in blocks:
            value = (arecv[block, :] + scaled(block, mrecv[block, :], 2)).astype(jnp.bfloat16)
            if qkv:
                hid_ref[block, :] = value
            else:
                hp[block, :] = value
        if qkv:
            for block in blocks:
                square_sums(block, hid_ref[block, :].astype(jnp.float32))

        @pl.loop(0, n_ff)
        def _(c):
            for copy in (to_sibling(c), to_partner(c), act_partner(c), act_sibling(c), act_forward(c)):
                copy.wait_send()
    if qkv:
        scales(3)
        for block in blocks:
            hp[block, :] = scaled(block, hid_ref[block, :].astype(jnp.float32), 3).astype(jnp.bfloat16)
        n_q = wi.shape[1] // QKV_CHUNK

        def q_partner(c):
            return remote(q_mine.at[c, pl.ds(0, rows)], q_x.at[c], q_ss.at[1, c], q_rs.at[1, c], part)

        for c in range(n_q):
            sums = jnp.dot(hp[...], wi[:, c * QKV_CHUNK:(c + 1) * QKV_CHUNK], preferred_element_type=jnp.float32)
            q_out[c] = sums[:2 * rows]
            q_mine[c] = sums[2 * rows:]
            copy = send(q_out.at[c], q_in.at[c], q_ss.at[0, c], q_rs.at[0, c], sib)
            if c >= 1:
                before.wait_recv()
                q_mine[c - 1] = q_mine[c - 1] + q_in[c - 1]
                q_partner(c - 1).start()
            before = copy
        before.wait_recv()
        q_mine[n_q - 1] = q_mine[n_q - 1] + q_in[n_q - 1]
        q_partner(n_q - 1).start()
        for c in range(n_q):
            q_partner(c).wait_recv()
            qkv_ref[:, c * QKV_CHUNK:(c + 1) * QKV_CHUNK] = q_mine[c, pl.ds(rows, rows), :] + q_x[c]
        for c in range(n_q):
            q_partner(c).wait_send()
    else:
        here = pl.ds(pl.multiple_of(me * share, LANES), share)
        out_copies = [send(hp.at[block, :], out_ref.at[:, here], misc_ss.at[3 + k], misc_rs.at[3 + k], dev)
                      for k, (dev, block) in enumerate(((sib, SIB), (part, PART), (diag, DIAG)))]
        out_ref[:, here] = hp[OWN, :]
        for dev, copy in zip((sib, part, diag), out_copies):
            copy.wait_recv()
    for copy in sends:
        copy.wait_send()


def comm(x, gains, in_weights=None, post=None, layer=0, collective_id=0):
    rows = x.shape[0]
    share = gains.shape[2] // 4
    n_rows = rows * 4
    f32, bf16, vmem, hbm = jnp.float32, jnp.bfloat16, pl.BlockSpec(memory_space=pltpu.VMEM), pl.BlockSpec(memory_space=pl.ANY)
    dma = pltpu.SemaphoreType.DMA
    args, specs = [x, gains], [vmem, vmem]
    scratch = [pltpu.VMEM((n_rows, LANES), f32), pltpu.VMEM((4, 8, n_rows), f32), pltpu.VMEM((4, 3, 8, n_rows), f32), pltpu.VMEM((n_rows, share), bf16),
               dma((4, 3)), dma((4, 3)), dma((6,)), dma((6,)), dma((7,))]
    n_ff = 0
    if post is not None:
        residual, w_o, w_gate, w_up, w_down = post
        args += list(post)
        specs += [vmem, hbm, hbm, hbm, hbm]
        ff = w_gate.shape[2]
        n_ff = ff // FF_CHUNK
        scratch += [pltpu.VMEM((n_rows, w_o.shape[1]), bf16)] + [pltpu.VMEM((n_rows, share), f32)] * 4
        scratch += [pltpu.VMEM(w_o.shape[1:], bf16), pltpu.VMEM((share, ff), bf16), pltpu.VMEM((share, ff), bf16), pltpu.VMEM((ff, share), bf16)]
        scratch += [pltpu.VMEM((n_ff, 2 * rows, 2 * FF_CHUNK), f32)] * 3 + [pltpu.VMEM((n_ff, rows, 2 * FF_CHUNK), f32), pltpu.VMEM((n_ff, n_rows, FF_CHUNK), bf16)]
        scratch += [dma((8,)), dma((8,)), dma((5, n_ff)), dma((5, n_ff))]
    if in_weights is not None:
        args += list(in_weights)
        specs += [hbm] * 3
        n_in = sum(w.shape[2] * w.shape[3] for w in in_weights)
        n_q = n_in // QKV_CHUNK
        scratch += [pltpu.VMEM((share, n_in), bf16)] + [pltpu.VMEM(w.shape[1:], bf16) for w in in_weights]
        scratch += [pltpu.VMEM((n_q, 2 * rows, QKV_CHUNK), f32)] * 3 + [pltpu.VMEM((n_q, rows, QKV_CHUNK), f32), dma((2, n_q)), dma((2, n_q))]
        out_shape = (jax.ShapeDtypeStruct((n_rows, share), bf16), jax.ShapeDtypeStruct((rows, n_in), f32))
        out_specs = (vmem, vmem)
    else:
        out_shape = jax.ShapeDtypeStruct((rows, 4 * share), bf16)
        out_specs = vmem
    cfg = {"post": post is not None, "qkv": in_weights is not None, "first": post is None, "layer": layer, "rows": rows, "share": share, "width": 4 * share, "n_ff": n_ff}
    return pl.pallas_call(
        functools.partial(comm_kernel, cfg),
        out_shape=out_shape, in_specs=specs, out_specs=out_specs, scratch_shapes=scratch,
        compiler_params=pltpu.CompilerParams(collective_id=collective_id, has_side_effects=True, vmem_limit_bytes=(62 if post is not None else 20) * 2**20),
        name=f"comm_{collective_id}",
    )(*args)


def solution(mesh):
    def device_step(hidden, positions, k_local, v_local, k_global, v_global, w_q, w_k, w_v, w_o, w_gate, w_up, w_down, norm_gains):
        share = w_q.shape[1]
        tables = rope_tables(positions, w_q.shape[3])
        in_weights = (w_q, w_k, w_v)
        post_weights = (w_o.reshape(2, -1, share), w_gate, w_up, w_down)
        residual, qkv = comm(hidden[:, 0, :], norm_gains, in_weights, layer=-1, collective_id=0)
        heads, k_local, v_local = attend(qkv, tables, positions, k_local, v_local)
        residual, qkv = comm(heads, norm_gains, in_weights, (residual,) + post_weights, layer=0, collective_id=1)
        heads, k_global, v_global = attend(qkv, tables, positions, k_global, v_global)
        final = comm(heads, norm_gains, None, (residual,) + post_weights, layer=1, collective_id=2)[:, None, :]
        return final, k_local, v_local, k_global, v_global

    in_specs = (ROW_SPEC, POS_SPEC, CACHE_SPEC, CACHE_SPEC, CACHE_SPEC, CACHE_SPEC, PROJ_IN_SPEC, PROJ_IN_SPEC, PROJ_IN_SPEC, PROJ_OUT_SPEC, FF_IN_SPEC, FF_IN_SPEC, FF_OUT_SPEC, GAIN_SPEC)
    out_specs = (ROW_SPEC, CACHE_SPEC, CACHE_SPEC, CACHE_SPEC, CACHE_SPEC)
    return jax.shard_map(device_step, mesh=mesh, in_specs=in_specs, out_specs=out_specs, check_vma=False)
```

```python
import functools

import jax
import jax.numpy as jnp
from jax import lax
from jax.experimental import pallas as pl
from jax.experimental.pallas import tpu as pltpu
from jax.sharding import PartitionSpec as P

SOFT_CAP = 50.0
NORM_EPS = 1e-6
ROPE_BASE = 10000.0

ROW_SPEC = P(("part", "data"), None, None)
POS_SPEC = P(("part", "data"))
CACHE_SPEC = P(("part", "data"), None, "model", None)
PROJ_IN_SPEC = P(None, "data", "model", None)
PROJ_OUT_SPEC = P(None, "model", None, "data")
FF_IN_SPEC = P(None, "data", "model")
FF_OUT_SPEC = P(None, "model", "data")
GAIN_SPEC = P(None, None, None)


def rope_tables(positions, head_dim):
    inv_freq = ROPE_BASE ** (-jnp.arange(0, head_dim, 2).astype(jnp.float32) / head_dim)
    angles = positions.astype(jnp.float32)[:, None] * inv_freq[None, :]
    return jnp.cos(angles), jnp.sin(angles)


LANES = 128


def attend_kernel(cache_len, n_rows, group, depth, pos_ref, qkv_ref, cos_ref, sin_ref, k_hbm, v_hbm, head_ref, ko_hbm, vo_hbm, kbuf, vbuf, q8, kn, vn, outs, sbuf, pbuf, rd_sem, wr_sem):
    n_steps = n_rows // group
    n_cols = cache_len * 4

    def reads(step):
        slot = lax.rem(step, depth)
        rows = pl.ds(step * group, group)
        return (pltpu.make_async_copy(k_hbm.at[rows], kbuf.at[slot], rd_sem.at[0, slot]),
                pltpu.make_async_copy(v_hbm.at[rows], vbuf.at[slot], rd_sem.at[1, slot]))

    def writes(step):
        slot = lax.rem(step, depth)
        rows = pl.ds(step * group, group)
        return (pltpu.make_async_copy(kbuf.at[slot], ko_hbm.at[rows], wr_sem.at[0, slot]),
                pltpu.make_async_copy(vbuf.at[slot], vo_hbm.at[rows], wr_sem.at[1, slot]))

    ahead = max(depth - 2, 1) if depth < n_steps else n_steps
    for step in range(ahead):
        for copy in reads(step):
            copy.start()

    cos_t, sin_t = cos_ref[...], sin_ref[...]
    scale = (2 * LANES) ** -0.5
    for h in range(4):
        first, second = qkv_ref[:, h * 256:h * 256 + LANES], qkv_ref[:, h * 256 + LANES:h * 256 + 256]
        q8[:, h, :] = (first * cos_t - second * sin_t) * scale
        q8[:, 4 + h, :] = (second * cos_t + first * sin_t) * scale
    for h in range(2):
        base = 1024 + h * 256
        first, second = qkv_ref[:, base:base + LANES], qkv_ref[:, base + LANES:base + 256]
        halves = (first * cos_t - second * sin_t, second * cos_t + first * sin_t)
        for half in range(2):
            value = qkv_ref[:, base + 512 + half * LANES:base + 512 + (half + 1) * LANES]
            for i in range(4):
                kn[:, i * 4 + half * 2 + h, :] = halves[half]
                vn[:, i * 4 + half * 2 + h, :] = value

    row_id = lax.broadcasted_iota(jnp.int32, (8, n_cols), 0)
    col_id = lax.broadcasted_iota(jnp.int32, (8, n_cols), 1)
    half_col = (col_id // 2) % 2
    same_half = row_id // 4 == half_col
    same_kv = (row_id // 2) % 2 == col_id % 2
    slot_col = col_id // 4
    sub_id = lax.broadcasted_iota(jnp.int32, (16, LANES), 0) // 4

    @pl.loop(0, n_steps)
    def _(step):
        slot = lax.rem(step, depth)
        if ahead < n_steps:
            @pl.when(step + ahead < n_steps)
            def _():
                @pl.when(step >= depth - ahead)
                def _():
                    for copy in writes(step - (depth - ahead)):
                        copy.wait()
                for copy in reads(step + ahead):
                    copy.start()

        for copy in reads(step):
            copy.wait()
        for i in range(group):
            row = step * group + i
            now = lax.rem(pos_ref[row], cache_len)
            window = pl.ds(pl.multiple_of(now // 4 * 16, 16), 16)
            hit = sub_id == lax.rem(now, 4)
            kbuf[slot, i, window, :] = jnp.where(hit, kn[row].astype(jnp.bfloat16), kbuf[slot, i, window, :])
            vbuf[slot, i, window, :] = jnp.where(hit, vn[row].astype(jnp.bfloat16), vbuf[slot, i, window, :])
        for i in range(group):
            part = lax.dot_general(q8[step * group + i].astype(jnp.bfloat16), kbuf[slot, i], (((1,), (1,)), ((), ())), preferred_element_type=jnp.float32)
            sbuf[i] = jnp.where(same_half & same_kv, part, 0.0)
        for i in range(group):
            part = sbuf[i]
            part = part + pltpu.roll(part, 4, 0)
            other = jnp.where(half_col == 0, pltpu.roll(part, n_cols - 2, 1), pltpu.roll(part, 2, 1))
            scores = SOFT_CAP * jnp.tanh((part + other) / SOFT_CAP)
            scores = jnp.where(same_kv & (slot_col <= pos_ref[step * group + i]), scores, -1e30)
            weights = jnp.exp(scores - jnp.max(scores, axis=1, keepdims=True))
            total = jnp.sum(jnp.where(same_half, weights, 0.0), axis=1, keepdims=True)
            pbuf[i] = jnp.where(same_half, weights / total, 0.0).astype(jnp.bfloat16)
        for i in range(group):
            outs[step * group + i] = jnp.dot(pbuf[i], vbuf[slot, i], preferred_element_type=jnp.float32)
        for copy in writes(step):
            copy.start()

    for h in range(4):
        for half in range(2):
            head_ref[:, h * 256 + half * LANES:h * 256 + (half + 1) * LANES] = outs[:, half * 4 + h, :].astype(jnp.bfloat16)
    for step in range(max(n_steps - depth, 0) if ahead < n_steps else 0, n_steps):
        for copy in writes(step):
            copy.wait()


def attend(qkv, tables, positions, k_cache, v_cache):
    n_rows, cache_len, kv_loc, head_dim = k_cache.shape
    halves = head_dim // LANES
    group = 16 if cache_len <= 64 else 4
    depth = 4 if cache_len <= 64 else 6
    f32, bf16 = jnp.float32, jnp.bfloat16

    def flat(cache):
        return cache.reshape(n_rows, cache_len, kv_loc, halves, LANES).transpose(0, 1, 3, 2, 4).reshape(n_rows, cache_len * halves * kv_loc, LANES)

    def unflat(cache):
        return cache.reshape(n_rows, cache_len, halves, kv_loc, LANES).transpose(0, 1, 3, 2, 4).reshape(n_rows, cache_len, kv_loc, head_dim)

    vmem, hbm = pl.BlockSpec(memory_space=pltpu.VMEM), pl.BlockSpec(memory_space=pl.ANY)
    k_flat, v_flat = flat(k_cache), flat(v_cache)
    n_cols = k_flat.shape[1]
    block = (depth, group, n_cols, LANES)
    dma = pltpu.SemaphoreType.DMA
    heads, k_out, v_out = pl.pallas_call(
        functools.partial(attend_kernel, cache_len, n_rows, group, depth),
        out_shape=(jax.ShapeDtypeStruct((n_rows, 4 * head_dim), bf16), jax.ShapeDtypeStruct(k_flat.shape, bf16), jax.ShapeDtypeStruct(v_flat.shape, bf16)),
        in_specs=[pl.BlockSpec(memory_space=pltpu.SMEM), vmem, vmem, vmem, hbm, hbm],
        out_specs=(vmem, hbm, hbm),
        scratch_shapes=[pltpu.VMEM(block, bf16), pltpu.VMEM(block, bf16), pltpu.VMEM((n_rows, 8, LANES), f32), pltpu.VMEM((n_rows, 16, LANES), f32),
                        pltpu.VMEM((n_rows, 16, LANES), f32), pltpu.VMEM((n_rows, 8, LANES), f32), pltpu.VMEM((group, 8, n_cols), f32), pltpu.VMEM((group, 8, n_cols), bf16),
                        dma((2, depth)), dma((2, depth))],
        compiler_params=pltpu.CompilerParams(vmem_limit_bytes=62 * 2**20),
        cost_estimate=pl.CostEstimate(flops=n_rows * 8 * n_cols * LANES * 4, bytes_accessed=4 * k_flat.size * 2, transcendentals=0),
        name=f"attend_{cache_len}",
    )(positions, qkv, *tables, k_flat, v_flat)
    return heads, unflat(k_out), unflat(v_out)


FF_CHUNK = 512
QKV_CHUNK = 512
MESH = pl.DeviceIdType.MESH


GROUPS = 2


def comm_kernel(cfg, *refs):
    it = iter(refs)
    post, layer, rows, share, width = cfg["post"], cfg["layer"], cfg["rows"], cfg["share"], cfg["width"]
    qkv, n_ff, n_q = cfg["qkv"], cfg["n_ff"], cfg["n_q"]
    x_ref = next(it)
    g_ref = next(it)
    if post:
        res_ref, wo_hbm, wg_hbm, wu_hbm, wd_hbm = (next(it) for _ in range(5))
    if qkv:
        wq_hbm, wk_hbm, wv_hbm = (next(it) for _ in range(3))
        hid_ref, qkv_ref = next(it), next(it)
    else:
        out_ref = next(it)
    tcol, st_src, st_rcv, hp, st_ss, st_rs, misc_ss, misc_rs, ld_sem = (next(it) for _ in range(9))
    if post:
        hall, apart, arecv, mpart, mrecv, wo, wg, wu, wd, sib_out, sib_in, mine, x_in, u_all = (next(it) for _ in range(14))
        y_ss, y_rs, ff_ss, ff_rs = (next(it) for _ in range(4))
    if qkv:
        wi, wq, wk, wv, q_out, q_in, q_mine, q_x, q_ss, q_rs = (next(it) for _ in range(10))

    model, me = lax.axis_index("model"), lax.axis_index("data")
    x_pos, core = me // 2, lax.rem(me, 2)
    sib, part, diag = x_pos * 2 + 1 - core, (1 - x_pos) * 2 + core, (1 - x_pos) * 2 + 1 - core
    n_group = 4 * rows
    DIAG, SIB, PART, OWN = (pl.ds(i * rows, rows) for i in range(4))
    blocks = (OWN, SIB, PART, DIAG)
    mine_rows = [pl.ds(h * rows, rows) for h in range(GROUPS)]
    sends = []

    def remote(src, dst, send_sem, recv_sem, data=None):
        where = {"data": data} if data is not None else {"model": 1 - model}
        return pltpu.make_async_remote_copy(src_ref=src, dst_ref=dst, send_sem=send_sem, recv_sem=recv_sem, device_id=where, device_id_type=MESH)

    def send(*args):
        copy = remote(*args)
        copy.start()
        sends.append(copy)
        return copy

    def load(src, dst, sem):
        copy = pltpu.make_async_copy(src, dst, sem)
        copy.start()
        return copy

    if post:
        wo_load = load(wo_hbm.at[layer], wo, ld_sem.at[0])
        wg_load = load(wg_hbm.at[layer], wg, ld_sem.at[1])
        wu_load = load(wu_hbm.at[layer], wu, ld_sem.at[2])
        wd_load = load(wd_hbm.at[layer], wd, ld_sem.at[3])
    if qkv:
        in_loads = [load(src.at[layer + 1], dst, ld_sem.at[4 + k]) for k, (src, dst) in enumerate(((wq_hbm, wq), (wk_hbm, wk), (wv_hbm, wv)))]

    def relay_weights():
        col = 0
        for copy, weight in zip(in_loads, (wq, wk, wv)):
            copy.wait()
            n_heads, head_dim = weight.shape[1:]
            for h in range(n_heads):
                wi[:, col:col + head_dim] = weight[:, h, :]
                col += head_dim

    barrier = pltpu.get_barrier_semaphore()
    for dev in (sib, part, diag):
        pl.semaphore_signal(barrier, inc=1, device_id={"data": dev}, device_id_type=MESH)
    pl.semaphore_signal(barrier, inc=1, device_id={"model": 1 - model}, device_id_type=MESH)
    pl.semaphore_wait(barrier, 4)

    def square_sums(h, block, value):
        total = None
        for k in range(share // LANES):
            piece = value[:, k * LANES:(k + 1) * LANES]
            total = piece * piece if total is None else total + piece * piece
        tcol[h, block, :] = total

    flip_low = lax.rem(lax.broadcasted_iota(jnp.int32, (8, n_group), 1) // rows, 2) == 0

    def start_scales(h, which):
        idx = which * GROUPS + h
        st_src[idx] = jnp.sum(jnp.transpose(tcol[h]).reshape(LANES // 8, 8, n_group), axis=0)
        return [send(st_src.at[idx], st_rcv.at[idx, k], st_ss.at[idx, k], st_rs.at[idx, k], dev) for k, dev in enumerate((sib, part, diag))]

    def end_scales(h, which, copies):
        idx = which * GROUPS + h
        for copy in copies:
            copy.wait_recv()

        def swap(value):
            return pltpu.roll(value, 2 * rows, 1)

        def flip(value):
            return jnp.where(flip_low, pltpu.roll(value, n_group - rows, 1), pltpu.roll(value, rows, 1))

        total = st_src[idx] + swap(st_rcv[idx, 0]) + flip(st_rcv[idx, 1]) + swap(flip(st_rcv[idx, 2]))
        total = jnp.sum(total, axis=0, keepdims=True)
        inverse = lax.rsqrt(total / width + NORM_EPS)
        tcol[h] = jnp.transpose(jnp.broadcast_to(inverse, (LANES, n_group)))

    def scales(h, which):
        end_scales(h, which, start_scales(h, which))

    def gain_row(k):
        at, which = (layer + 1, 0) if k == 3 else (layer, k + 1)
        return 1.0 + g_ref[at, which:which + 1, pl.ds(pl.multiple_of(me * share, LANES), share)].astype(jnp.float32)

    def scaled(h, block, value, gain):
        return value * jnp.concatenate([tcol[h, block, :]] * (share // LANES), axis=1) * gain_row(gain)

    def q_partner(s):
        return remote(q_mine.at[s, pl.ds(0, rows)], q_x.at[s], q_ss.at[1, s], q_rs.at[1, s], part)

    def start_qkv(h):
        for block in blocks:
            square_sums(h, block, hid_ref[h, block, :].astype(jnp.float32))
        scales(h, 3)
        for block in blocks:
            hp[h, block, :] = scaled(h, block, hid_ref[h, block, :].astype(jnp.float32), 3).astype(jnp.bfloat16)
        before = None
        for c in range(n_q):
            s = h * n_q + c
            sums = jnp.dot(hp[h], wi[:, c * QKV_CHUNK:(c + 1) * QKV_CHUNK], preferred_element_type=jnp.float32)
            q_out[s] = sums[:2 * rows]
            q_mine[s] = sums[2 * rows:]
            copy = send(q_out.at[s], q_in.at[s], q_ss.at[0, s], q_rs.at[0, s], sib)
            if c >= 1:
                before.wait_recv()
                q_mine[s - 1] = q_mine[s - 1] + q_in[s - 1]
                q_partner(s - 1).start()
            before = copy
        before.wait_recv()
        s = h * n_q + n_q - 1
        q_mine[s] = q_mine[s] + q_in[s]
        q_partner(s).start()

    def end_qkv():
        for h in range(GROUPS):
            for c in range(n_q):
                s = h * n_q + c
                q_partner(s).wait_recv()
                qkv_ref[mine_rows[h], c * QKV_CHUNK:(c + 1) * QKV_CHUNK] = q_mine[s, pl.ds(rows, rows), :] + q_x[s]
        for s in range(GROUPS * n_q):
            q_partner(s).wait_send()

    if not post:
        copies = []
        for h in range(GROUPS):
            for k, (dev, there) in enumerate(((sib, SIB), (part, PART), (diag, DIAG))):
                cols = pl.ds(pl.multiple_of(dev * share, LANES), share)
                copies.append(send(x_ref.at[mine_rows[h], cols], hid_ref.at[h, there, :], misc_ss.at[h * 3 + k], misc_rs.at[h * 3 + k], dev))
        relay_weights()
        for h in range(GROUPS):
            hid_ref[h, OWN, :] = x_ref[mine_rows[h], pl.ds(pl.multiple_of(me * share, LANES), share)]
            for copy in copies[h * 3:h * 3 + 3]:
                copy.wait_recv()
            start_qkv(h)
        end_qkv()
    else:
        to_part = send(x_ref, hall.at[2], misc_ss.at[0], misc_rs.at[0], part)
        to_sib = send(x_ref, hall.at[1], misc_ss.at[1], misc_rs.at[1], sib)
        wo_load.wait()
        y_copies = [[None] * 4 for _ in range(GROUPS)]

        def project(k, heads):
            sums = jnp.dot(heads, wo[...], preferred_element_type=jnp.float32)
            for h in range(GROUPS):
                apart[h, blocks[k], :] = sums[h * rows:(h + 1) * rows]

        def to_model(h, k):
            y_copies[h][k] = send(apart.at[h, blocks[k], :], arecv.at[h, blocks[k], :], y_ss.at[h * 4 + k], y_rs.at[h * 4 + k])

        project(0, x_ref[...])
        to_model(0, 0)
        to_sib.wait_recv()
        project(1, hall[1])
        to_model(0, 1)
        to_model(1, 0)
        to_part.wait_recv()
        forward = send(hall.at[2], hall.at[0], misc_ss.at[2], misc_rs.at[2], sib)
        project(2, hall[2])
        to_model(0, 2)
        forward.wait_recv()
        project(3, hall[0])
        to_model(0, 3)
        for h in range(1, GROUPS):
            for k in range(1, 4):
                to_model(h, k)

        def enter_ff(h):
            for k, block in enumerate(blocks):
                y_copies[h][k].wait_recv()
                total = apart[h, block, :] + arecv[h, block, :]
                arecv[h, block, :] = total
                square_sums(h, block, total)
            scales(h, 0)
            for block in blocks:
                residual = res_ref[h, block, :].astype(jnp.float32)
                mid = (residual + scaled(h, block, arecv[h, block, :], 0)).astype(jnp.bfloat16).astype(jnp.float32)
                arecv[h, block, :] = mid
            for block in blocks:
                square_sums(h, block, arecv[h, block, :])
            copies = start_scales(h, 1)
            mpart[h] = jnp.zeros((n_group, share), jnp.float32)
            end_scales(h, 1, copies)
            for block in blocks:
                hp[h, block, :] = scaled(h, block, arecv[h, block, :], 1).astype(jnp.bfloat16)

        def to_sibling(s):
            return remote(sib_out.at[s], sib_in.at[s], ff_ss.at[0, s], ff_rs.at[0, s], sib)

        def to_partner(s):
            return remote(mine.at[s, pl.ds(0, rows)], x_in.at[s], ff_ss.at[1, s], ff_rs.at[1, s], part)

        def act_partner(s):
            return remote(u_all.at[s, OWN], u_all.at[s, PART], ff_ss.at[2, s], ff_rs.at[2, s], part)

        def act_sibling(s):
            return remote(u_all.at[s, OWN], u_all.at[s, SIB], ff_ss.at[3, s], ff_rs.at[3, s], sib)

        def act_forward(s):
            return remote(u_all.at[s, PART], u_all.at[s, DIAG], ff_ss.at[4, s], ff_rs.at[4, s], sib)

        def add_sibling(s):
            to_sibling(s).wait_recv()
            mine[s] = mine[s] + sib_in[s]
            to_partner(s).start()

        def gate_up(h):
            @pl.loop(0, n_ff)
            def _(c):
                s = h * n_ff + c
                cols = pl.ds(pl.multiple_of(c * FF_CHUNK, FF_CHUNK), FF_CHUNK)
                for k, weight in enumerate((wg, wu)):
                    sums = jnp.dot(hp[h], weight[:, cols], preferred_element_type=jnp.float32)
                    sib_out[s, :, pl.ds(k * FF_CHUNK, FF_CHUNK)] = sums[:2 * rows]
                    mine[s, :, pl.ds(k * FF_CHUNK, FF_CHUNK)] = sums[2 * rows:]
                to_sibling(s).start()

                @pl.when(c >= 1)
                def _():
                    add_sibling(s - 1)

            add_sibling(h * n_ff + n_ff - 1)

        enter_ff(0)
        wg_load.wait()
        wu_load.wait()
        for h in range(GROUPS):
            gate_up(h)
            if h + 1 < GROUPS:
                enter_ff(h + 1)
        if qkv:
            relay_weights()

        @pl.loop(0, GROUPS * n_ff)
        def _(s):
            to_partner(s).wait_recv()
            both = mine[s, pl.ds(rows, rows), :] + x_in[s]
            u_all[s, OWN, :] = (jax.nn.gelu(both[:, :FF_CHUNK], approximate=True) * both[:, FF_CHUNK:]).astype(jnp.bfloat16)
            act_partner(s).start()
            act_sibling(s).start()

        wd_load.wait()

        def down(h, c):
            s = h * n_ff + c
            act_sibling(s).wait_recv()
            act_forward(s).wait_recv()
            deep = pl.ds(pl.multiple_of(c * FF_CHUNK, FF_CHUNK), FF_CHUNK)
            mpart[h] += jnp.dot(u_all[s], wd[deep, :], preferred_element_type=jnp.float32)

        m_copies = []
        for h in range(GROUPS):
            @pl.loop(0, n_ff)
            def _(c):
                act_partner(h * n_ff + c).wait_recv()
                act_forward(h * n_ff + c).start()

                @pl.when(c >= 1)
                def _():
                    down(h, c - 1)

            down(h, n_ff - 1)
            m_copies.append(send(mpart.at[h], mrecv.at[h], y_ss.at[4 * GROUPS + h], y_rs.at[4 * GROUPS + h]))

        out_copies = []
        for h in range(GROUPS):
            m_copies[h].wait_recv()
            for block in blocks:
                total = mpart[h, block, :] + mrecv[h, block, :]
                mrecv[h, block, :] = total
                square_sums(h, block, total)
            scales(h, 2)
            for block in blocks:
                value = (arecv[h, block, :] + scaled(h, block, mrecv[h, block, :], 2)).astype(jnp.bfloat16)
                if qkv:
                    hid_ref[h, block, :] = value
                else:
                    hp[h, block, :] = value
            if qkv:
                start_qkv(h)
            else:
                here = pl.ds(pl.multiple_of(me * share, LANES), share)
                for k, (dev, block) in enumerate(((sib, SIB), (part, PART), (diag, DIAG))):
                    out_copies.append(send(hp.at[h, block, :], out_ref.at[mine_rows[h], here], misc_ss.at[3 + h * 3 + k], misc_rs.at[3 + h * 3 + k], dev))
                out_ref[mine_rows[h], here] = hp[h, OWN, :]
        if qkv:
            end_qkv()
        for copy in out_copies:
            copy.wait_recv()

        @pl.loop(0, GROUPS * n_ff)
        def _(s):
            for copy in (to_sibling(s), to_partner(s), act_partner(s), act_sibling(s), act_forward(s)):
                copy.wait_send()
    for copy in sends:
        copy.wait_send()


def comm(x, gains, in_weights=None, post=None, layer=0, collective_id=0):
    rows = x.shape[0] // GROUPS
    share = gains.shape[2] // 4
    n_group = rows * 4
    f32, bf16, vmem, hbm = jnp.float32, jnp.bfloat16, pl.BlockSpec(memory_space=pltpu.VMEM), pl.BlockSpec(memory_space=pl.ANY)
    dma = pltpu.SemaphoreType.DMA
    args, specs = [x, gains], [vmem, vmem]
    n_stat = 4 * GROUPS
    scratch = [pltpu.VMEM((GROUPS, n_group, LANES), f32), pltpu.VMEM((n_stat, 8, n_group), f32), pltpu.VMEM((n_stat, 3, 8, n_group), f32), pltpu.VMEM((GROUPS, n_group, share), bf16),
               dma((n_stat, 3)), dma((n_stat, 3)), dma((3 + 3 * GROUPS,)), dma((3 + 3 * GROUPS,)), dma((7,))]
    n_ff = n_q = 0
    if post is not None:
        residual, w_o, w_gate, w_up, w_down = post
        args += list(post)
        specs += [vmem, hbm, hbm, hbm, hbm]
        ff = w_gate.shape[2]
        n_ff = ff // FF_CHUNK
        steps = GROUPS * n_ff
        scratch += [pltpu.VMEM((3, GROUPS * rows, w_o.shape[1]), bf16)] + [pltpu.VMEM((GROUPS, n_group, share), f32)] * 4
        scratch += [pltpu.VMEM(w_o.shape[1:], bf16), pltpu.VMEM((share, ff), bf16), pltpu.VMEM((share, ff), bf16), pltpu.VMEM((ff, share), bf16)]
        scratch += [pltpu.VMEM((steps, 2 * rows, 2 * FF_CHUNK), f32)] * 3 + [pltpu.VMEM((steps, rows, 2 * FF_CHUNK), f32), pltpu.VMEM((steps, n_group, FF_CHUNK), bf16)]
        scratch += [dma((5 * GROUPS,)), dma((5 * GROUPS,)), dma((5, steps)), dma((5, steps))]
    if in_weights is not None:
        args += list(in_weights)
        specs += [hbm] * 3
        n_in = sum(w.shape[2] * w.shape[3] for w in in_weights)
        n_q = n_in // QKV_CHUNK
        scratch += [pltpu.VMEM((share, n_in), bf16)] + [pltpu.VMEM(w.shape[1:], bf16) for w in in_weights]
        scratch += [pltpu.VMEM((GROUPS * n_q, 2 * rows, QKV_CHUNK), f32)] * 3 + [pltpu.VMEM((GROUPS * n_q, rows, QKV_CHUNK), f32), dma((2, GROUPS * n_q)), dma((2, GROUPS * n_q))]
        out_shape = (jax.ShapeDtypeStruct((GROUPS, n_group, share), bf16), jax.ShapeDtypeStruct((GROUPS * rows, n_in), f32))
        out_specs = (vmem, vmem)
    else:
        out_shape = jax.ShapeDtypeStruct((GROUPS * rows, 4 * share), bf16)
        out_specs = vmem
    cfg = {"post": post is not None, "qkv": in_weights is not None, "layer": layer, "rows": rows, "share": share, "width": 4 * share, "n_ff": n_ff, "n_q": n_q}
    return pl.pallas_call(
        functools.partial(comm_kernel, cfg),
        out_shape=out_shape, in_specs=specs, out_specs=out_specs, scratch_shapes=scratch,
        compiler_params=pltpu.CompilerParams(collective_id=collective_id, has_side_effects=True, vmem_limit_bytes=62 * 2**20),
        name=f"comm_{collective_id}",
    )(*args)


def solution(mesh):
    def device_step(hidden, positions, k_local, v_local, k_global, v_global, w_q, w_k, w_v, w_o, w_gate, w_up, w_down, norm_gains):
        share = w_q.shape[1]
        tables = rope_tables(positions, w_q.shape[3])
        in_weights = (w_q, w_k, w_v)
        post_weights = (w_o.reshape(2, -1, share), w_gate, w_up, w_down)
        residual, qkv = comm(hidden[:, 0, :], norm_gains, in_weights, layer=-1, collective_id=0)
        heads, k_local, v_local = attend(qkv, tables, positions, k_local, v_local)
        residual, qkv = comm(heads, norm_gains, in_weights, (residual,) + post_weights, layer=0, collective_id=1)
        heads, k_global, v_global = attend(qkv, tables, positions, k_global, v_global)
        final = comm(heads, norm_gains, None, (residual,) + post_weights, layer=1, collective_id=2)[:, None, :]
        return final, k_local, v_local, k_global, v_global

    in_specs = (ROW_SPEC, POS_SPEC, CACHE_SPEC, CACHE_SPEC, CACHE_SPEC, CACHE_SPEC, PROJ_IN_SPEC, PROJ_IN_SPEC, PROJ_IN_SPEC, PROJ_OUT_SPEC, FF_IN_SPEC, FF_IN_SPEC, FF_OUT_SPEC, GAIN_SPEC)
    out_specs = (ROW_SPEC, CACHE_SPEC, CACHE_SPEC, CACHE_SPEC, CACHE_SPEC)
    return jax.shard_map(device_step, mesh=mesh, in_specs=in_specs, out_specs=out_specs, check_vma=False)
```

```python
import functools

import jax
import jax.numpy as jnp
from jax import lax
from jax.experimental import pallas as pl
from jax.experimental.pallas import tpu as pltpu
from jax.sharding import PartitionSpec as P

SOFT_CAP = 50.0
NORM_EPS = 1e-6
ROPE_BASE = 10000.0

ROW_SPEC = P(("part", "data"), None, None)
POS_SPEC = P(("part", "data"))
CACHE_SPEC = P(("part", "data"), None, "model", None)
PROJ_IN_SPEC = P(None, "data", "model", None)
PROJ_OUT_SPEC = P(None, "model", None, "data")
FF_IN_SPEC = P(None, "data", "model")
FF_OUT_SPEC = P(None, "model", "data")
GAIN_SPEC = P(None, None, None)


def rope_tables(positions, head_dim):
    inv_freq = ROPE_BASE ** (-jnp.arange(0, head_dim, 2).astype(jnp.float32) / head_dim)
    angles = positions.astype(jnp.float32)[:, None] * inv_freq[None, :]
    return jnp.cos(angles), jnp.sin(angles)


LANES = 128


def attend_kernel(cache_len, n_rows, group, depth, pos_ref, qkv_ref, cos_ref, sin_ref, k_hbm, v_hbm, head_ref, ko_hbm, vo_hbm, kbuf, vbuf, q8, kn, vn, outs, sbuf, pbuf, rd_sem, wr_sem):
    n_steps = n_rows // group
    n_cols = cache_len * 4

    def reads(step):
        slot = lax.rem(step, depth)
        rows = pl.ds(step * group, group)
        return (pltpu.make_async_copy(k_hbm.at[rows], kbuf.at[slot], rd_sem.at[0, slot]),
                pltpu.make_async_copy(v_hbm.at[rows], vbuf.at[slot], rd_sem.at[1, slot]))

    def writes(step):
        slot = lax.rem(step, depth)
        rows = pl.ds(step * group, group)
        return (pltpu.make_async_copy(kbuf.at[slot], ko_hbm.at[rows], wr_sem.at[0, slot]),
                pltpu.make_async_copy(vbuf.at[slot], vo_hbm.at[rows], wr_sem.at[1, slot]))

    ahead = max(depth - 2, 1) if depth < n_steps else n_steps
    for step in range(ahead):
        for copy in reads(step):
            copy.start()

    cos_t, sin_t = cos_ref[...], sin_ref[...]
    scale = (2 * LANES) ** -0.5
    for h in range(4):
        first, second = qkv_ref[:, h * 256:h * 256 + LANES], qkv_ref[:, h * 256 + LANES:h * 256 + 256]
        q8[:, h, :] = (first * cos_t - second * sin_t) * scale
        q8[:, 4 + h, :] = (second * cos_t + first * sin_t) * scale
    for h in range(2):
        base = 1024 + h * 256
        first, second = qkv_ref[:, base:base + LANES], qkv_ref[:, base + LANES:base + 256]
        halves = (first * cos_t - second * sin_t, second * cos_t + first * sin_t)
        for half in range(2):
            value = qkv_ref[:, base + 512 + half * LANES:base + 512 + (half + 1) * LANES]
            for i in range(4):
                kn[:, i * 4 + half * 2 + h, :] = halves[half]
                vn[:, i * 4 + half * 2 + h, :] = value

    row_id = lax.broadcasted_iota(jnp.int32, (8, n_cols), 0)
    col_id = lax.broadcasted_iota(jnp.int32, (8, n_cols), 1)
    half_col = (col_id // 2) % 2
    same_half = row_id // 4 == half_col
    same_kv = (row_id // 2) % 2 == col_id % 2
    slot_col = col_id // 4
    sub_id = lax.broadcasted_iota(jnp.int32, (16, LANES), 0) // 4

    @pl.loop(0, n_steps)
    def _(step):
        slot = lax.rem(step, depth)
        if ahead < n_steps:
            @pl.when(step + ahead < n_steps)
            def _():
                @pl.when(step >= depth - ahead)
                def _():
                    for copy in writes(step - (depth - ahead)):
                        copy.wait()
                for copy in reads(step + ahead):
                    copy.start()

        for copy in reads(step):
            copy.wait()
        for i in range(group):
            row = step * group + i
            now = lax.rem(pos_ref[row], cache_len)
            window = pl.ds(pl.multiple_of(now // 4 * 16, 16), 16)
            hit = sub_id == lax.rem(now, 4)
            kbuf[slot, i, window, :] = jnp.where(hit, kn[row].astype(jnp.bfloat16), kbuf[slot, i, window, :])
            vbuf[slot, i, window, :] = jnp.where(hit, vn[row].astype(jnp.bfloat16), vbuf[slot, i, window, :])
        for i in range(group):
            part = lax.dot_general(q8[step * group + i].astype(jnp.bfloat16), kbuf[slot, i], (((1,), (1,)), ((), ())), preferred_element_type=jnp.float32)
            sbuf[i] = jnp.where(same_half & same_kv, part, 0.0)
        for i in range(group):
            part = sbuf[i]
            part = part + pltpu.roll(part, 4, 0)
            other = jnp.where(half_col == 0, pltpu.roll(part, n_cols - 2, 1), pltpu.roll(part, 2, 1))
            scores = SOFT_CAP * jnp.tanh((part + other) / SOFT_CAP)
            scores = jnp.where(same_kv & (slot_col <= pos_ref[step * group + i]), scores, -1e30)
            weights = jnp.exp(scores - jnp.max(scores, axis=1, keepdims=True))
            total = jnp.sum(jnp.where(same_half, weights, 0.0), axis=1, keepdims=True)
            pbuf[i] = jnp.where(same_half, weights / total, 0.0).astype(jnp.bfloat16)
        for i in range(group):
            outs[step * group + i] = jnp.dot(pbuf[i], vbuf[slot, i], preferred_element_type=jnp.float32)
        for copy in writes(step):
            copy.start()

    for h in range(4):
        for half in range(2):
            head_ref[:, h * 256 + half * LANES:h * 256 + (half + 1) * LANES] = outs[:, half * 4 + h, :].astype(jnp.bfloat16)
    for step in range(max(n_steps - depth, 0) if ahead < n_steps else 0, n_steps):
        for copy in writes(step):
            copy.wait()


def attend(qkv, tables, positions, k_cache, v_cache):
    n_rows, cache_len, kv_loc, head_dim = k_cache.shape
    halves = head_dim // LANES
    group = 16 if cache_len <= 64 else 4
    depth = 4 if cache_len <= 64 else 6
    f32, bf16 = jnp.float32, jnp.bfloat16

    def flat(cache):
        return cache.reshape(n_rows, cache_len, kv_loc, halves, LANES).transpose(0, 1, 3, 2, 4).reshape(n_rows, cache_len * halves * kv_loc, LANES)

    def unflat(cache):
        return cache.reshape(n_rows, cache_len, halves, kv_loc, LANES).transpose(0, 1, 3, 2, 4).reshape(n_rows, cache_len, kv_loc, head_dim)

    vmem, hbm = pl.BlockSpec(memory_space=pltpu.VMEM), pl.BlockSpec(memory_space=pl.ANY)
    k_flat, v_flat = flat(k_cache), flat(v_cache)
    n_cols = k_flat.shape[1]
    block = (depth, group, n_cols, LANES)
    dma = pltpu.SemaphoreType.DMA
    heads, k_out, v_out = pl.pallas_call(
        functools.partial(attend_kernel, cache_len, n_rows, group, depth),
        out_shape=(jax.ShapeDtypeStruct((n_rows, 4 * head_dim), bf16), jax.ShapeDtypeStruct(k_flat.shape, bf16), jax.ShapeDtypeStruct(v_flat.shape, bf16)),
        in_specs=[pl.BlockSpec(memory_space=pltpu.SMEM), vmem, vmem, vmem, hbm, hbm],
        out_specs=(vmem, hbm, hbm),
        scratch_shapes=[pltpu.VMEM(block, bf16), pltpu.VMEM(block, bf16), pltpu.VMEM((n_rows, 8, LANES), f32), pltpu.VMEM((n_rows, 16, LANES), f32),
                        pltpu.VMEM((n_rows, 16, LANES), f32), pltpu.VMEM((n_rows, 8, LANES), f32), pltpu.VMEM((group, 8, n_cols), f32), pltpu.VMEM((group, 8, n_cols), bf16),
                        dma((2, depth)), dma((2, depth))],
        compiler_params=pltpu.CompilerParams(vmem_limit_bytes=62 * 2**20),
        cost_estimate=pl.CostEstimate(flops=n_rows * 8 * n_cols * LANES * 4, bytes_accessed=4 * k_flat.size * 2, transcendentals=0),
        name=f"attend_{cache_len}",
    )(positions, qkv, *tables, k_flat, v_flat)
    return heads, unflat(k_out), unflat(v_out)


FF_CHUNK = 1024
QKV_CHUNK = 1024
MESH = pl.DeviceIdType.MESH


GROUPS = 4


def comm_kernel(cfg, *refs):
    it = iter(refs)
    post, layer, rows, share, width = cfg["post"], cfg["layer"], cfg["rows"], cfg["share"], cfg["width"]
    qkv, n_ff, n_q = cfg["qkv"], cfg["n_ff"], cfg["n_q"]
    raw = cfg["raw"]
    x_hbm, g_hbm = next(it), next(it)
    if post:
        res_hbm, wo_hbm, wg_hbm, wu_hbm, wd_hbm = (next(it) for _ in range(5))
    if qkv:
        wq_hbm, wk_hbm, wv_hbm = (next(it) for _ in range(3))
        if post:
            hid_ref = next(it)
        qkv_ref = next(it)
    else:
        out_ref = next(it)
    x_ref, g_ref, tcol, st_src, st_rcv, hp, st_ss, st_rs, misc_ss, misc_rs, ld_sem = (next(it) for _ in range(11))
    if not post:
        out_rows = next(it)
    if post:
        if raw:
            raw_ref = next(it)
        res_ref, hall, apart, arecv, mpart, mrecv, wo, wg, wu, wd, sib_out, sib_in, mine, x_in, u_all = (next(it) for _ in range(15))
        y_ss, y_rs, ff_ss, ff_rs = (next(it) for _ in range(4))
    if qkv:
        wi, wq, wk, wv, q_out, q_in, q_mine, q_x, q_ss, q_rs = (next(it) for _ in range(10))

    model, me = lax.axis_index("model"), lax.axis_index("data")
    x_pos, core = me // 2, lax.rem(me, 2)
    sib, part, diag = x_pos * 2 + 1 - core, (1 - x_pos) * 2 + core, (1 - x_pos) * 2 + 1 - core
    n_group = 4 * rows
    DIAG, SIB, PART, OWN = (pl.ds(i * rows, rows) for i in range(4))
    blocks = (OWN, SIB, PART, DIAG)
    mine_rows = [pl.ds(h * rows, rows) for h in range(GROUPS)]
    sends = []

    def remote(src, dst, send_sem, recv_sem, data=None):
        where = {"data": data} if data is not None else {"model": 1 - model}
        return pltpu.make_async_remote_copy(src_ref=src, dst_ref=dst, send_sem=send_sem, recv_sem=recv_sem, device_id=where, device_id_type=MESH)

    def send(*args):
        copy = remote(*args)
        copy.start()
        sends.append(copy)
        return copy

    def load(src, dst, sem):
        copy = pltpu.make_async_copy(src, dst, sem)
        copy.start()
        return copy

    early = [load(x_hbm, x_ref, ld_sem.at[7]), load(g_hbm, g_ref, ld_sem.at[8])]
    if post:
        early.append(load(res_hbm, raw_ref if raw else res_ref, ld_sem.at[9]))
        wo_load = load(wo_hbm.at[layer], wo, ld_sem.at[0])
        wg_load = load(wg_hbm.at[layer], wg, ld_sem.at[1])
        wu_load = load(wu_hbm.at[layer], wu, ld_sem.at[2])
        wd_load = load(wd_hbm.at[layer], wd, ld_sem.at[3])
    if qkv:
        in_loads = [load(src.at[layer + 1], dst, ld_sem.at[4 + k]) for k, (src, dst) in enumerate(((wq_hbm, wq), (wk_hbm, wk), (wv_hbm, wv)))]

    def relay_weights(c):
        col = c * QKV_CHUNK
        for k in ((0,), (1, 2))[c]:
            in_loads[k].wait()
            weight = (wq, wk, wv)[k]
            n_heads, head_dim = weight.shape[1:]
            for h in range(n_heads):
                wi[:, col:col + head_dim] = weight[:, h, :]
                col += head_dim

    barrier = pltpu.get_barrier_semaphore()
    for dev in (sib, part, diag):
        pl.semaphore_signal(barrier, inc=1, device_id={"data": dev}, device_id_type=MESH)
    pl.semaphore_signal(barrier, inc=1, device_id={"model": 1 - model}, device_id_type=MESH)
    tcol[...] = jnp.zeros_like(tcol)
    for copy in early:
        copy.wait()
    pl.semaphore_wait(barrier, 4)

    def square_sums(h, block, value):
        total = None
        for k in range(share // LANES):
            piece = value[:, k * LANES:(k + 1) * LANES]
            total = piece * piece if total is None else total + piece * piece
        tcol[h, block, :] = total

    lane_block = lax.broadcasted_iota(jnp.int32, (8, LANES), 1) // rows

    def start_scales(h, which):
        idx = which * GROUPS + h
        st_src[idx] = jnp.sum(jnp.transpose(tcol[h]).reshape(LANES // 8, 8, LANES), axis=0)
        return [send(st_src.at[idx], st_rcv.at[idx, k], st_ss.at[idx, k], st_rs.at[idx, k], dev) for k, dev in enumerate((sib, part, diag))]

    def end_scales(h, which, copies):
        idx = which * GROUPS + h
        for copy in copies:
            copy.wait_recv()

        def exchange(value, n):
            even = lax.rem(lane_block // n, 2) == 0
            return jnp.where(even, pltpu.roll(value, LANES - n * rows, 1), pltpu.roll(value, n * rows, 1))

        total = st_src[idx] + exchange(st_rcv[idx, 0], 2) + exchange(st_rcv[idx, 1], 1) + exchange(exchange(st_rcv[idx, 2], 1), 2)
        total = jnp.sum(total, axis=0, keepdims=True)
        inverse = lax.rsqrt(total / width + NORM_EPS)
        tcol[h] = jnp.transpose(jnp.broadcast_to(inverse, (LANES, LANES)))

    def gain_row(k):
        at, which = (layer + 1, 0) if k == 3 else (layer, k + 1)
        return 1.0 + g_ref[at, which:which + 1, pl.ds(pl.multiple_of(me * share, LANES), share)].astype(jnp.float32)

    def scaled(h, block, value, gain):
        return value * jnp.concatenate([tcol[h, block, :]] * (share // LANES), axis=1) * gain_row(gain)

    def q_partner(s):
        return remote(q_mine.at[s, pl.ds(0, rows)], q_x.at[s], q_ss.at[1, s], q_rs.at[1, s], part)

    def start_qkv(h, relay=False):
        before = None
        for c in range(n_q):
            s = h * n_q + c
            if relay:
                relay_weights(c)
            sums = jnp.dot(hp[h], wi[:, c * QKV_CHUNK:(c + 1) * QKV_CHUNK], preferred_element_type=jnp.float32)
            q_out[s] = sums[:2 * rows]
            q_mine[s] = sums[2 * rows:]
            copy = send(q_out.at[s], q_in.at[s], q_ss.at[0, s], q_rs.at[0, s], sib)
            if c >= 1:
                before.wait_recv()
                q_mine[s - 1] = q_mine[s - 1] + q_in[s - 1]
                q_partner(s - 1).start()
            before = copy
        before.wait_recv()
        s = h * n_q + n_q - 1
        q_mine[s] = q_mine[s] + q_in[s]
        q_partner(s).start()

    def end_qkv():
        for h in range(GROUPS):
            for c in range(n_q):
                s = h * n_q + c
                q_partner(s).wait_recv()
                qkv_ref[mine_rows[h], c * QKV_CHUNK:(c + 1) * QKV_CHUNK] = q_mine[s, pl.ds(rows, rows), :] + q_x[s]
        for s in range(GROUPS * n_q):
            q_partner(s).wait_send()

    def spread(src, dst, base):
        copies = []
        for h in range(GROUPS):
            for k, (dev, there) in enumerate(((sib, SIB), (part, PART), (diag, DIAG))):
                cols = pl.ds(pl.multiple_of(dev * share, LANES), share)
                i = base + h * 3 + k
                copies.append(send(src.at[mine_rows[h], cols], dst.at[h, there, :], misc_ss.at[i], misc_rs.at[i], dev))
        return copies

    my_cols = pl.ds(pl.multiple_of(me * share, LANES), share)
    if not post:
        xn = out_rows
        for h in range(GROUPS):
            value = x_ref[mine_rows[h], :].astype(jnp.float32)
            inverse = lax.rsqrt(jnp.mean(value * value, axis=1, keepdims=True) + NORM_EPS)
            xn[mine_rows[h], :] = (value * inverse * (1.0 + g_ref[0, 0:1, :].astype(jnp.float32))).astype(jnp.bfloat16)
        copies = spread(xn, hp, 0)
        for h in range(GROUPS):
            hp[h, OWN, :] = xn[mine_rows[h], my_cols]
            for copy in copies[h * 3:h * 3 + 3]:
                copy.wait_recv()
            start_qkv(h, relay=h == 0)
        end_qkv()
    else:
        to_part = send(x_ref, hall.at[2], misc_ss.at[0], misc_rs.at[0], part)
        to_sib = send(x_ref, hall.at[1], misc_ss.at[1], misc_rs.at[1], sib)
        if raw:
            raw_copies = spread(raw_ref, res_ref, 3)
            for h in range(GROUPS):
                res_ref[h, OWN, :] = raw_ref[mine_rows[h], my_cols]
        wo_load.wait()
        y_copies = [[None] * 4 for _ in range(GROUPS)]

        def project(k, heads):
            sums = jnp.dot(heads, wo[...], preferred_element_type=jnp.float32)
            for h in range(GROUPS):
                apart[h, blocks[k], :] = sums[h * rows:(h + 1) * rows]

        def to_model(*pairs):
            for h, k in pairs:
                y_copies[h][k] = send(apart.at[h, blocks[k], :], arecv.at[h, blocks[k], :], y_ss.at[h * 4 + k], y_rs.at[h * 4 + k])

        project(0, x_ref[...])
        to_model((0, 0), (1, 0))
        to_sib.wait_recv()
        project(1, hall[1])
        to_model((0, 1), (1, 1), (2, 0))
        to_part.wait_recv()
        forward = send(hall.at[2], hall.at[0], misc_ss.at[2], misc_rs.at[2], sib)
        project(2, hall[2])
        to_model((0, 2))
        forward.wait_recv()
        project(3, hall[0])
        to_model((0, 3), (1, 2), (1, 3), (2, 1), (2, 2), (2, 3), (3, 0), (3, 1), (3, 2), (3, 3))
        stats = {}

        def attn_sums(h):
            for k, block in enumerate(blocks):
                y_copies[h][k].wait_recv()
                total = apart[h, block, :] + arecv[h, block, :]
                arecv[h, block, :] = total
                square_sums(h, block, total)
            stats[h] = start_scales(h, 0)

        def attn_residual(h):
            end_scales(h, 0, stats[h])
            if raw:
                for copy in raw_copies[h * 3:h * 3 + 3]:
                    copy.wait_recv()
            for block in blocks:
                residual = res_ref[h, block, :].astype(jnp.float32)
                mid = (residual + scaled(h, block, arecv[h, block, :], 0)).astype(jnp.bfloat16).astype(jnp.float32)
                arecv[h, block, :] = mid
            for block in blocks:
                square_sums(h, block, arecv[h, block, :])
            stats[h] = start_scales(h, 1)

        def attn_normed(h):
            mpart[h] = jnp.zeros((n_group, share), jnp.float32)
            end_scales(h, 1, stats[h])
            for block in blocks:
                hp[h, block, :] = scaled(h, block, arecv[h, block, :], 1).astype(jnp.bfloat16)

        def to_sibling(s):
            return remote(sib_out.at[s], sib_in.at[s], ff_ss.at[0, s], ff_rs.at[0, s], sib)

        def to_partner(s):
            return remote(mine.at[s, pl.ds(0, rows)], x_in.at[s], ff_ss.at[1, s], ff_rs.at[1, s], part)

        def act_partner(s):
            return remote(u_all.at[s, OWN], u_all.at[s, PART], ff_ss.at[2, s], ff_rs.at[2, s], part)

        def act_sibling(s):
            return remote(u_all.at[s, OWN], u_all.at[s, SIB], ff_ss.at[3, s], ff_rs.at[3, s], sib)

        def act_forward(s):
            return remote(u_all.at[s, PART], u_all.at[s, DIAG], ff_ss.at[4, s], ff_rs.at[4, s], sib)

        def add_sibling(s):
            to_sibling(s).wait_recv()
            mine[s] = mine[s] + sib_in[s]
            to_partner(s).start()

        def gate_up(h):
            @pl.loop(0, n_ff)
            def _(c):
                s = h * n_ff + c
                cols = pl.ds(pl.multiple_of(c * FF_CHUNK, FF_CHUNK), FF_CHUNK)
                for k, weight in enumerate((wg, wu)):
                    sums = jnp.dot(hp[h], weight[:, cols], preferred_element_type=jnp.float32)
                    sib_out[s, :, pl.ds(k * FF_CHUNK, FF_CHUNK)] = sums[:2 * rows]
                    mine[s, :, pl.ds(k * FF_CHUNK, FF_CHUNK)] = sums[2 * rows:]
                to_sibling(s).start()

                @pl.when(c >= 1)
                def _():
                    add_sibling(s - 1)

            add_sibling(h * n_ff + n_ff - 1)

        attn_sums(0)
        attn_residual(0)
        attn_sums(1)
        attn_normed(0)
        wg_load.wait()
        wu_load.wait()
        gate_up(0)
        attn_residual(1)
        attn_sums(2)
        attn_normed(1)
        gate_up(1)
        attn_residual(2)
        attn_sums(3)
        attn_normed(2)
        gate_up(2)
        attn_residual(3)
        attn_normed(3)
        gate_up(3)
        if qkv:
            relay_weights(0)
            relay_weights(1)

        @pl.loop(0, GROUPS * n_ff)
        def _(s):
            to_partner(s).wait_recv()
            both = mine[s, pl.ds(rows, rows), :] + x_in[s]
            u_all[s, OWN, :] = (jax.nn.gelu(both[:, :FF_CHUNK], approximate=True) * both[:, FF_CHUNK:]).astype(jnp.bfloat16)
            act_partner(s).start()
            act_sibling(s).start()

        wd_load.wait()

        def down(h, c):
            s = h * n_ff + c
            act_sibling(s).wait_recv()
            act_forward(s).wait_recv()
            deep = pl.ds(pl.multiple_of(c * FF_CHUNK, FF_CHUNK), FF_CHUNK)
            mpart[h] += jnp.dot(u_all[s], wd[deep, :], preferred_element_type=jnp.float32)

        m_copies = []
        for h in range(GROUPS):
            @pl.loop(0, n_ff)
            def _(c):
                act_partner(h * n_ff + c).wait_recv()
                act_forward(h * n_ff + c).start()

                @pl.when(c >= 1)
                def _():
                    down(h, c - 1)

            down(h, n_ff - 1)
            m_copies.append(send(mpart.at[h], mrecv.at[h], y_ss.at[4 * GROUPS + h], y_rs.at[4 * GROUPS + h]))

        out_copies = []

        def ff_sums(h):
            m_copies[h].wait_recv()
            for block in blocks:
                total = mpart[h, block, :] + mrecv[h, block, :]
                mrecv[h, block, :] = total
                square_sums(h, block, total)
            stats[h] = start_scales(h, 2)

        def ff_residual(h):
            end_scales(h, 2, stats[h])
            for block in blocks:
                value = (arecv[h, block, :] + scaled(h, block, mrecv[h, block, :], 2)).astype(jnp.bfloat16)
                if qkv:
                    hid_ref[h, block, :] = value
                else:
                    hp[h, block, :] = value
            if qkv:
                for block in blocks:
                    square_sums(h, block, hid_ref[h, block, :].astype(jnp.float32))
                stats[h] = start_scales(h, 3)
            else:
                for k, (dev, block) in enumerate(((sib, SIB), (part, PART), (diag, DIAG))):
                    i = 3 + h * 3 + k
                    out_copies.append(send(hp.at[h, block, :], out_ref.at[mine_rows[h], my_cols], misc_ss.at[i], misc_rs.at[i], dev))
                out_ref[mine_rows[h], my_cols] = hp[h, OWN, :]

        def ff_normed(h):
            end_scales(h, 3, stats[h])
            for block in blocks:
                hp[h, block, :] = scaled(h, block, hid_ref[h, block, :].astype(jnp.float32), 3).astype(jnp.bfloat16)
            start_qkv(h)

        ff_sums(0)
        ff_sums(1)
        ff_residual(0)
        ff_sums(2)
        ff_residual(1)
        if qkv:
            ff_normed(0)
        ff_sums(3)
        ff_residual(2)
        if qkv:
            ff_normed(1)
        ff_residual(3)
        if qkv:
            ff_normed(2)
            ff_normed(3)
        if qkv:
            end_qkv()
        for copy in out_copies:
            copy.wait_recv()

        @pl.loop(0, GROUPS * n_ff)
        def _(s):
            for copy in (to_sibling(s), to_partner(s), act_partner(s), act_sibling(s), act_forward(s)):
                copy.wait_send()
    for copy in sends:
        copy.wait_send()


def comm(x, gains, in_weights=None, post=None, layer=0, collective_id=0):
    rows = x.shape[0] // GROUPS
    share = gains.shape[2] // 4
    n_group = rows * 4
    f32, bf16, vmem, hbm = jnp.float32, jnp.bfloat16, pl.BlockSpec(memory_space=pltpu.VMEM), pl.BlockSpec(memory_space=pl.ANY)
    dma = pltpu.SemaphoreType.DMA
    args, specs = [x, gains], [hbm, hbm]
    raw = post is not None and post[0].ndim == 2
    n_stat = 4 * GROUPS
    n_misc = 3 + 3 * GROUPS
    scratch = [pltpu.VMEM(x.shape, bf16), pltpu.VMEM(gains.shape, bf16), pltpu.VMEM((GROUPS, LANES, LANES), f32), pltpu.VMEM((n_stat, 8, LANES), f32), pltpu.VMEM((n_stat, 3, 8, LANES), f32), pltpu.VMEM((GROUPS, n_group, share), bf16),
               dma((n_stat, 3)), dma((n_stat, 3)), dma((n_misc,)), dma((n_misc,)), dma((10,))]
    if post is None:
        scratch.append(pltpu.VMEM(x.shape, bf16))
    n_ff = n_q = 0
    if post is not None:
        residual, w_o, w_gate, w_up, w_down = post
        args += list(post)
        specs += [hbm] * 5
        ff = w_gate.shape[2]
        n_ff = ff // FF_CHUNK
        steps = GROUPS * n_ff
        scratch += [pltpu.VMEM(residual.shape, bf16)] if raw else []
        scratch += [pltpu.VMEM((GROUPS, n_group, share), bf16), pltpu.VMEM((3, GROUPS * rows, w_o.shape[1]), bf16)] + [pltpu.VMEM((GROUPS, n_group, share), f32)] * 4
        scratch += [pltpu.VMEM(w_o.shape[1:], bf16), pltpu.VMEM((share, ff), bf16), pltpu.VMEM((share, ff), bf16), pltpu.VMEM((ff, share), bf16)]
        scratch += [pltpu.VMEM((steps, 2 * rows, 2 * FF_CHUNK), f32)] * 3 + [pltpu.VMEM((steps, rows, 2 * FF_CHUNK), f32), pltpu.VMEM((steps, n_group, FF_CHUNK), bf16)]
        scratch += [dma((5 * GROUPS,)), dma((5 * GROUPS,)), dma((5, steps)), dma((5, steps))]
    if in_weights is not None:
        args += list(in_weights)
        specs += [hbm] * 3
        n_in = sum(w.shape[2] * w.shape[3] for w in in_weights)
        n_q = n_in // QKV_CHUNK
        scratch += [pltpu.VMEM((share, n_in), bf16)] + [pltpu.VMEM(w.shape[1:], bf16) for w in in_weights]
        scratch += [pltpu.VMEM((GROUPS * n_q, 2 * rows, QKV_CHUNK), f32)] * 3 + [pltpu.VMEM((GROUPS * n_q, rows, QKV_CHUNK), f32), dma((2, GROUPS * n_q)), dma((2, GROUPS * n_q))]
        out_shape = [jax.ShapeDtypeStruct((GROUPS, n_group, share), bf16), jax.ShapeDtypeStruct((GROUPS * rows, n_in), f32)][post is None:]
        out_specs = [vmem, vmem][post is None:]
    else:
        out_shape = jax.ShapeDtypeStruct((GROUPS * rows, 4 * share), bf16)
        out_specs = vmem
    cfg = {"raw": raw, "post": post is not None, "qkv": in_weights is not None, "layer": layer, "rows": rows, "share": share, "width": 4 * share, "n_ff": n_ff, "n_q": n_q}
    return pl.pallas_call(
        functools.partial(comm_kernel, cfg),
        out_shape=out_shape, in_specs=specs, out_specs=out_specs, scratch_shapes=scratch,
        compiler_params=pltpu.CompilerParams(collective_id=collective_id, has_side_effects=True, vmem_limit_bytes=62 * 2**20),
        name=f"comm_{collective_id}",
    )(*args)


def solution(mesh):
    def device_step(hidden, positions, k_local, v_local, k_global, v_global, w_q, w_k, w_v, w_o, w_gate, w_up, w_down, norm_gains):
        share = w_q.shape[1]
        tables = rope_tables(positions, w_q.shape[3])
        in_weights = (w_q, w_k, w_v)
        post_weights = (w_o.reshape(2, -1, share), w_gate, w_up, w_down)
        hidden_rows = hidden[:, 0, :]
        qkv, = comm(hidden_rows, norm_gains, in_weights, layer=-1, collective_id=0)
        heads, k_local, v_local = attend(qkv, tables, positions, k_local, v_local)
        residual, qkv = comm(heads, norm_gains, in_weights, (hidden_rows,) + post_weights, layer=0, collective_id=1)
        heads, k_global, v_global = attend(qkv, tables, positions, k_global, v_global)
        final = comm(heads, norm_gains, None, (residual,) + post_weights, layer=1, collective_id=2)[:, None, :]
        return final, k_local, v_local, k_global, v_global

    in_specs = (ROW_SPEC, POS_SPEC, CACHE_SPEC, CACHE_SPEC, CACHE_SPEC, CACHE_SPEC, PROJ_IN_SPEC, PROJ_IN_SPEC, PROJ_IN_SPEC, PROJ_OUT_SPEC, FF_IN_SPEC, FF_IN_SPEC, FF_OUT_SPEC, GAIN_SPEC)
    out_specs = (ROW_SPEC, CACHE_SPEC, CACHE_SPEC, CACHE_SPEC, CACHE_SPEC)
    return jax.shard_map(device_step, mesh=mesh, in_specs=in_specs, out_specs=out_specs, check_vma=False)
```

```python
import functools

import jax
import jax.numpy as jnp
from jax import lax
from jax.experimental import pallas as pl
from jax.experimental.pallas import tpu as pltpu
from jax.sharding import PartitionSpec as P

SOFT_CAP = 50.0
NORM_EPS = 1e-6
ROPE_BASE = 10000.0

ROW_SPEC = P(("part", "data"), None, None)
POS_SPEC = P(("part", "data"))
CACHE_SPEC = P(("part", "data"), None, "model", None)
PROJ_IN_SPEC = P(None, "data", "model", None)
PROJ_OUT_SPEC = P(None, "model", None, "data")
FF_IN_SPEC = P(None, "data", "model")
FF_OUT_SPEC = P(None, "model", "data")
GAIN_SPEC = P(None, None, None)


def rope_tables(positions, head_dim):
    inv_freq = ROPE_BASE ** (-jnp.arange(0, head_dim, 2).astype(jnp.float32) / head_dim)
    angles = positions.astype(jnp.float32)[:, None] * inv_freq[None, :]
    return jnp.cos(angles), jnp.sin(angles)


LANES = 128


def attend_kernel(cache_len, n_rows, group, depth, pos_ref, qkv_ref, cos_ref, sin_ref, k_hbm, v_hbm, head_ref, ko_hbm, vo_hbm, kbuf, vbuf, q8, kn, vn, outs, sbuf, pbuf, rd_sem, wr_sem):
    n_steps = n_rows // group
    n_cols = cache_len * 4

    def reads(step):
        slot = lax.rem(step, depth)
        rows = pl.ds(step * group, group)
        return (pltpu.make_async_copy(k_hbm.at[rows], kbuf.at[slot], rd_sem.at[0, slot]),
                pltpu.make_async_copy(v_hbm.at[rows], vbuf.at[slot], rd_sem.at[1, slot]))

    def writes(step):
        slot = lax.rem(step, depth)
        rows = pl.ds(step * group, group)
        return (pltpu.make_async_copy(kbuf.at[slot], ko_hbm.at[rows], wr_sem.at[0, slot]),
                pltpu.make_async_copy(vbuf.at[slot], vo_hbm.at[rows], wr_sem.at[1, slot]))

    ahead = max(depth - 2, 1) if depth < n_steps else n_steps
    for step in range(ahead):
        for copy in reads(step):
            copy.start()

    cos_t, sin_t = cos_ref[...], sin_ref[...]
    scale = (2 * LANES) ** -0.5
    for h in range(4):
        first, second = qkv_ref[:, h * 256:h * 256 + LANES], qkv_ref[:, h * 256 + LANES:h * 256 + 256]
        q8[:, h, :] = (first * cos_t - second * sin_t) * scale
        q8[:, 4 + h, :] = (second * cos_t + first * sin_t) * scale
    for h in range(2):
        base = 1024 + h * 256
        first, second = qkv_ref[:, base:base + LANES], qkv_ref[:, base + LANES:base + 256]
        halves = (first * cos_t - second * sin_t, second * cos_t + first * sin_t)
        for half in range(2):
            value = qkv_ref[:, base + 512 + half * LANES:base + 512 + (half + 1) * LANES]
            for i in range(4):
                kn[:, i * 4 + half * 2 + h, :] = halves[half]
                vn[:, i * 4 + half * 2 + h, :] = value

    row_id = lax.broadcasted_iota(jnp.int32, (8, n_cols), 0)
    col_id = lax.broadcasted_iota(jnp.int32, (8, n_cols), 1)
    half_col = (col_id // 2) % 2
    same_half = row_id // 4 == half_col
    same_kv = (row_id // 2) % 2 == col_id % 2
    slot_col = col_id // 4
    sub_id = lax.broadcasted_iota(jnp.int32, (16, LANES), 0) // 4

    @pl.loop(0, n_steps)
    def _(step):
        slot = lax.rem(step, depth)
        if ahead < n_steps:
            @pl.when(step + ahead < n_steps)
            def _():
                @pl.when(step >= depth - ahead)
                def _():
                    for copy in writes(step - (depth - ahead)):
                        copy.wait()
                for copy in reads(step + ahead):
                    copy.start()

        for copy in reads(step):
            copy.wait()
        for i in range(group):
            row = step * group + i
            now = lax.rem(pos_ref[row], cache_len)
            window = pl.ds(pl.multiple_of(now // 4 * 16, 16), 16)
            hit = sub_id == lax.rem(now, 4)
            kbuf[slot, i, window, :] = jnp.where(hit, kn[row].astype(jnp.bfloat16), kbuf[slot, i, window, :])
            vbuf[slot, i, window, :] = jnp.where(hit, vn[row].astype(jnp.bfloat16), vbuf[slot, i, window, :])
        for i in range(group):
            part = lax.dot_general(q8[step * group + i].astype(jnp.bfloat16), kbuf[slot, i], (((1,), (1,)), ((), ())), preferred_element_type=jnp.float32)
            sbuf[i] = jnp.where(same_half & same_kv, part, 0.0)
        for i in range(group):
            part = sbuf[i]
            part = part + pltpu.roll(part, 4, 0)
            other = jnp.where(half_col == 0, pltpu.roll(part, n_cols - 2, 1), pltpu.roll(part, 2, 1))
            scores = SOFT_CAP * jnp.tanh((part + other) / SOFT_CAP)
            scores = jnp.where(same_kv & (slot_col <= pos_ref[step * group + i]), scores, -1e30)
            weights = jnp.exp(scores - jnp.max(scores, axis=1, keepdims=True))
            total = jnp.sum(jnp.where(same_half, weights, 0.0), axis=1, keepdims=True)
            pbuf[i] = jnp.where(same_half, weights / total, 0.0).astype(jnp.bfloat16)
        for i in range(group):
            outs[step * group + i] = jnp.dot(pbuf[i], vbuf[slot, i], preferred_element_type=jnp.float32)
        for copy in writes(step):
            copy.start()

    for h in range(4):
        for half in range(2):
            head_ref[:, h * 256 + half * LANES:h * 256 + (half + 1) * LANES] = outs[:, half * 4 + h, :].astype(jnp.bfloat16)
    for step in range(max(n_steps - depth, 0) if ahead < n_steps else 0, n_steps):
        for copy in writes(step):
            copy.wait()


def attend(qkv, tables, positions, k_cache, v_cache):
    n_rows, cache_len, kv_loc, head_dim = k_cache.shape
    halves = head_dim // LANES
    group = 16 if cache_len <= 64 else 2
    depth = 4 if cache_len <= 64 else 12
    f32, bf16 = jnp.float32, jnp.bfloat16

    def flat(cache):
        return cache.reshape(n_rows, cache_len, kv_loc, halves, LANES).transpose(0, 1, 3, 2, 4).reshape(n_rows, cache_len * halves * kv_loc, LANES)

    def unflat(cache):
        return cache.reshape(n_rows, cache_len, halves, kv_loc, LANES).transpose(0, 1, 3, 2, 4).reshape(n_rows, cache_len, kv_loc, head_dim)

    vmem, hbm = pl.BlockSpec(memory_space=pltpu.VMEM), pl.BlockSpec(memory_space=pl.ANY)
    k_flat, v_flat = flat(k_cache), flat(v_cache)
    n_cols = k_flat.shape[1]
    block = (depth, group, n_cols, LANES)
    dma = pltpu.SemaphoreType.DMA
    heads, k_out, v_out = pl.pallas_call(
        functools.partial(attend_kernel, cache_len, n_rows, group, depth),
        out_shape=(jax.ShapeDtypeStruct((n_rows, 4 * head_dim), bf16), jax.ShapeDtypeStruct(k_flat.shape, bf16), jax.ShapeDtypeStruct(v_flat.shape, bf16)),
        in_specs=[pl.BlockSpec(memory_space=pltpu.SMEM), vmem, vmem, vmem, hbm, hbm],
        out_specs=(vmem, hbm, hbm),
        scratch_shapes=[pltpu.VMEM(block, bf16), pltpu.VMEM(block, bf16), pltpu.VMEM((n_rows, 8, LANES), f32), pltpu.VMEM((n_rows, 16, LANES), f32),
                        pltpu.VMEM((n_rows, 16, LANES), f32), pltpu.VMEM((n_rows, 8, LANES), f32), pltpu.VMEM((group, 8, n_cols), f32), pltpu.VMEM((group, 8, n_cols), bf16),
                        dma((2, depth)), dma((2, depth))],
        compiler_params=pltpu.CompilerParams(vmem_limit_bytes=62 * 2**20),
        cost_estimate=pl.CostEstimate(flops=n_rows * 8 * n_cols * LANES * 4, bytes_accessed=4 * k_flat.size * 2, transcendentals=0),
        name=f"attend_{cache_len}",
    )(positions, qkv, *tables, k_flat, v_flat)
    return heads, unflat(k_out), unflat(v_out)


FF_CHUNK = 2560
QKV_CHUNK = 1024
MESH = pl.DeviceIdType.MESH


GROUPS = 4


def comm_kernel(cfg, *refs):
    it = iter(refs)
    post, layer, rows, share, width = cfg["post"], cfg["layer"], cfg["rows"], cfg["share"], cfg["width"]
    qkv, n_ff, n_q = cfg["qkv"], cfg["n_ff"], cfg["n_q"]
    raw = cfg["raw"]
    x_hbm, g_hbm = next(it), next(it)
    if post:
        res_hbm, wo_hbm, wg_hbm, wu_hbm, wd_hbm = (next(it) for _ in range(5))
    if qkv:
        wq_hbm, wk_hbm, wv_hbm = (next(it) for _ in range(3))
        if post:
            hid_ref = next(it)
        qkv_ref = next(it)
    else:
        out_ref = next(it)
    x_ref, g_ref, tcol, st_src, st_rcv, hp, st_ss, st_rs, misc_ss, misc_rs, ld_sem = (next(it) for _ in range(11))
    if not post:
        out_rows = next(it)
    if post:
        if raw:
            raw_ref = next(it)
        res_ref, hall, apart, arecv, mpart, mrecv, wo, wg, wu, wd, sib_out, sib_in, mine, x_in, u_all = (next(it) for _ in range(15))
        y_ss, y_rs, ff_ss, ff_rs = (next(it) for _ in range(4))
    if qkv:
        wi, wq, wk, wv, q_out, q_in, q_mine, q_x, q_ss, q_rs = (next(it) for _ in range(10))

    model, me = lax.axis_index("model"), lax.axis_index("data")
    x_pos, core = me // 2, lax.rem(me, 2)
    sib, part, diag = x_pos * 2 + 1 - core, (1 - x_pos) * 2 + core, (1 - x_pos) * 2 + 1 - core
    n_group = 4 * rows
    DIAG, SIB, PART, OWN = (pl.ds(i * rows, rows) for i in range(4))
    blocks = (OWN, SIB, PART, DIAG)
    mine_rows = [pl.ds(h * rows, rows) for h in range(GROUPS)]
    sends = []

    def remote(src, dst, send_sem, recv_sem, data=None):
        where = {"data": data} if data is not None else {"model": 1 - model}
        return pltpu.make_async_remote_copy(src_ref=src, dst_ref=dst, send_sem=send_sem, recv_sem=recv_sem, device_id=where, device_id_type=MESH)

    def send(*args):
        copy = remote(*args)
        copy.start()
        sends.append(copy)
        return copy

    def load(src, dst, sem):
        copy = pltpu.make_async_copy(src, dst, sem)
        copy.start()
        return copy

    early = [load(x_hbm, x_ref, ld_sem.at[7]), load(g_hbm, g_ref, ld_sem.at[8])]
    if post:
        early.append(load(res_hbm, raw_ref if raw else res_ref, ld_sem.at[9]))
        wo_load = load(wo_hbm.at[layer], wo, ld_sem.at[0])
        wg_load = load(wg_hbm.at[layer], wg, ld_sem.at[1])
        wu_load = load(wu_hbm.at[layer], wu, ld_sem.at[2])
        wd_load = load(wd_hbm.at[layer], wd, ld_sem.at[3])
    if qkv:
        in_loads = [load(src.at[layer + 1], dst, ld_sem.at[4 + k]) for k, (src, dst) in enumerate(((wq_hbm, wq), (wk_hbm, wk), (wv_hbm, wv)))]

    def relay_weights(c):
        col = c * QKV_CHUNK
        for k in ((0,), (1, 2))[c]:
            in_loads[k].wait()
            weight = (wq, wk, wv)[k]
            n_heads, head_dim = weight.shape[1:]
            for h in range(n_heads):
                wi[:, col:col + head_dim] = weight[:, h, :]
                col += head_dim

    barrier = pltpu.get_barrier_semaphore()
    for dev in (sib, part, diag):
        pl.semaphore_signal(barrier, inc=1, device_id={"data": dev}, device_id_type=MESH)
    pl.semaphore_signal(barrier, inc=1, device_id={"model": 1 - model}, device_id_type=MESH)
    tcol[...] = jnp.zeros_like(tcol)
    for copy in early:
        copy.wait()
    pl.semaphore_wait(barrier, 4)

    def square_sums(h, block, value):
        total = None
        for k in range(share // LANES):
            piece = value[:, k * LANES:(k + 1) * LANES]
            total = piece * piece if total is None else total + piece * piece
        tcol[h, block, :] = total

    lane_block = lax.broadcasted_iota(jnp.int32, (8, LANES), 1) // rows

    def start_scales(h, which):
        idx = which * GROUPS + h
        st_src[idx] = jnp.sum(jnp.transpose(tcol[h]).reshape(LANES // 8, 8, LANES), axis=0)
        return [send(st_src.at[idx], st_rcv.at[idx, k], st_ss.at[idx, k], st_rs.at[idx, k], dev) for k, dev in enumerate((sib, part, diag))]

    def end_scales(h, which, copies):
        idx = which * GROUPS + h
        for copy in copies:
            copy.wait_recv()

        def exchange(value, n):
            even = lax.rem(lane_block // n, 2) == 0
            return jnp.where(even, pltpu.roll(value, LANES - n * rows, 1), pltpu.roll(value, n * rows, 1))

        total = st_src[idx] + exchange(st_rcv[idx, 0], 2) + exchange(st_rcv[idx, 1], 1) + exchange(exchange(st_rcv[idx, 2], 1), 2)
        total = jnp.sum(total, axis=0, keepdims=True)
        inverse = lax.rsqrt(total / width + NORM_EPS)
        tcol[h] = jnp.transpose(jnp.broadcast_to(inverse, (LANES, LANES)))

    def gain_row(k):
        at, which = (layer + 1, 0) if k == 3 else (layer, k + 1)
        return 1.0 + g_ref[at, which:which + 1, pl.ds(pl.multiple_of(me * share, LANES), share)].astype(jnp.float32)

    def scaled(h, block, value, gain):
        return value * jnp.concatenate([tcol[h, block, :]] * (share // LANES), axis=1) * gain_row(gain)

    def q_partner(s):
        return remote(q_mine.at[s, pl.ds(0, rows)], q_x.at[s], q_ss.at[1, s], q_rs.at[1, s], part)

    def start_qkv(h, relay=False):
        before = None
        for c in range(n_q):
            s = h * n_q + c
            if relay:
                relay_weights(c)
            sums = jnp.dot(hp[h], wi[:, c * QKV_CHUNK:(c + 1) * QKV_CHUNK], preferred_element_type=jnp.float32)
            q_out[s] = sums[:2 * rows]
            q_mine[s] = sums[2 * rows:]
            copy = send(q_out.at[s], q_in.at[s], q_ss.at[0, s], q_rs.at[0, s], sib)
            if c >= 1:
                before.wait_recv()
                q_mine[s - 1] = q_mine[s - 1] + q_in[s - 1]
                q_partner(s - 1).start()
            before = copy
        before.wait_recv()
        s = h * n_q + n_q - 1
        q_mine[s] = q_mine[s] + q_in[s]
        q_partner(s).start()

    def end_qkv():
        for h in range(GROUPS):
            for c in range(n_q):
                s = h * n_q + c
                q_partner(s).wait_recv()
                qkv_ref[mine_rows[h], c * QKV_CHUNK:(c + 1) * QKV_CHUNK] = q_mine[s, pl.ds(rows, rows), :] + q_x[s]
        for s in range(GROUPS * n_q):
            q_partner(s).wait_send()

    def spread(src, dst, base):
        copies = []
        for h in range(GROUPS):
            for k, (dev, there) in enumerate(((sib, SIB), (part, PART), (diag, DIAG))):
                cols = pl.ds(pl.multiple_of(dev * share, LANES), share)
                i = base + h * 3 + k
                copies.append(send(src.at[mine_rows[h], cols], dst.at[h, there, :], misc_ss.at[i], misc_rs.at[i], dev))
        return copies

    my_cols = pl.ds(pl.multiple_of(me * share, LANES), share)
    if not post:
        xn = out_rows
        for h in range(GROUPS):
            value = x_ref[mine_rows[h], :].astype(jnp.float32)
            inverse = lax.rsqrt(jnp.mean(value * value, axis=1, keepdims=True) + NORM_EPS)
            xn[mine_rows[h], :] = (value * inverse * (1.0 + g_ref[0, 0:1, :].astype(jnp.float32))).astype(jnp.bfloat16)
        copies = spread(xn, hp, 0)
        for h in range(GROUPS):
            hp[h, OWN, :] = xn[mine_rows[h], my_cols]
            for copy in copies[h * 3:h * 3 + 3]:
                copy.wait_recv()
            start_qkv(h, relay=h == 0)
        end_qkv()
    else:
        to_part = send(x_ref, hall.at[2], misc_ss.at[0], misc_rs.at[0], part)
        to_sib = send(x_ref, hall.at[1], misc_ss.at[1], misc_rs.at[1], sib)
        if raw:
            raw_copies = spread(raw_ref, res_ref, 3)
            for h in range(GROUPS):
                res_ref[h, OWN, :] = raw_ref[mine_rows[h], my_cols]
        wo_load.wait()
        y_copies = [[None] * 4 for _ in range(GROUPS)]

        def project(k, heads):
            sums = jnp.dot(heads, wo[...], preferred_element_type=jnp.float32)
            for h in range(GROUPS):
                apart[h, blocks[k], :] = sums[h * rows:(h + 1) * rows]

        def to_model(*pairs):
            for h, k in pairs:
                y_copies[h][k] = send(apart.at[h, blocks[k], :], arecv.at[h, blocks[k], :], y_ss.at[h * 4 + k], y_rs.at[h * 4 + k])

        project(0, x_ref[...])
        to_model((0, 0), (1, 0))
        to_sib.wait_recv()
        project(1, hall[1])
        to_model((0, 1), (1, 1), (2, 0))
        to_part.wait_recv()
        forward = send(hall.at[2], hall.at[0], misc_ss.at[2], misc_rs.at[2], sib)
        project(2, hall[2])
        to_model((0, 2))
        forward.wait_recv()
        project(3, hall[0])
        to_model((0, 3), (1, 2), (1, 3), (2, 1), (2, 2), (2, 3), (3, 0), (3, 1), (3, 2), (3, 3))
        stats = {}

        def attn_sums(h):
            for k, block in enumerate(blocks):
                y_copies[h][k].wait_recv()
                total = apart[h, block, :] + arecv[h, block, :]
                arecv[h, block, :] = total
                square_sums(h, block, total)
            stats[h] = start_scales(h, 0)

        def attn_residual(h):
            end_scales(h, 0, stats[h])
            if raw:
                for copy in raw_copies[h * 3:h * 3 + 3]:
                    copy.wait_recv()
            for block in blocks:
                residual = res_ref[h, block, :].astype(jnp.float32)
                mid = (residual + scaled(h, block, arecv[h, block, :], 0)).astype(jnp.bfloat16).astype(jnp.float32)
                arecv[h, block, :] = mid
            for block in blocks:
                square_sums(h, block, arecv[h, block, :])
            stats[h] = start_scales(h, 1)

        def attn_normed(h):
            mpart[h] = jnp.zeros((n_group, share), jnp.float32)
            end_scales(h, 1, stats[h])
            for block in blocks:
                hp[h, block, :] = scaled(h, block, arecv[h, block, :], 1).astype(jnp.bfloat16)

        def to_sibling(s):
            return remote(sib_out.at[s], sib_in.at[s], ff_ss.at[0, s], ff_rs.at[0, s], sib)

        def to_partner(s):
            return remote(mine.at[s, pl.ds(0, rows)], x_in.at[s], ff_ss.at[1, s], ff_rs.at[1, s], part)

        def act_partner(s):
            return remote(u_all.at[s, OWN], u_all.at[s, PART], ff_ss.at[2, s], ff_rs.at[2, s], part)

        def act_sibling(s):
            return remote(u_all.at[s, OWN], u_all.at[s, SIB], ff_ss.at[3, s], ff_rs.at[3, s], sib)

        def act_forward(s):
            return remote(u_all.at[s, PART], u_all.at[s, DIAG], ff_ss.at[4, s], ff_rs.at[4, s], sib)

        def add_sibling(s):
            to_sibling(s).wait_recv()
            mine[s] = mine[s] + sib_in[s]
            to_partner(s).start()

        def gate_up(h):
            @pl.loop(0, n_ff)
            def _(c):
                s = h * n_ff + c
                cols = pl.ds(pl.multiple_of(c * FF_CHUNK, FF_CHUNK), FF_CHUNK)
                for k, weight in enumerate((wg, wu)):
                    sums = jnp.dot(hp[h], weight[:, cols], preferred_element_type=jnp.float32)
                    sib_out[s, :, pl.ds(k * FF_CHUNK, FF_CHUNK)] = sums[:2 * rows]
                    mine[s, :, pl.ds(k * FF_CHUNK, FF_CHUNK)] = sums[2 * rows:]
                to_sibling(s).start()

                @pl.when(c >= 1)
                def _():
                    add_sibling(s - 1)

            add_sibling(h * n_ff + n_ff - 1)

        attn_sums(0)
        attn_residual(0)
        attn_sums(1)
        attn_normed(0)
        wg_load.wait()
        wu_load.wait()
        gate_up(0)
        attn_residual(1)
        attn_sums(2)
        attn_normed(1)
        gate_up(1)
        attn_residual(2)
        attn_sums(3)
        attn_normed(2)
        gate_up(2)
        attn_residual(3)
        attn_normed(3)
        gate_up(3)
        if qkv:
            relay_weights(0)
            relay_weights(1)

        @pl.loop(0, GROUPS * n_ff)
        def _(s):
            to_partner(s).wait_recv()
            both = mine[s, pl.ds(rows, rows), :] + x_in[s]
            u_all[s, OWN, :] = (jax.nn.gelu(both[:, :FF_CHUNK], approximate=True) * both[:, FF_CHUNK:]).astype(jnp.bfloat16)
            act_partner(s).start()
            act_sibling(s).start()

        wd_load.wait()

        def down(h, c):
            s = h * n_ff + c
            act_sibling(s).wait_recv()
            act_forward(s).wait_recv()
            deep = pl.ds(pl.multiple_of(c * FF_CHUNK, FF_CHUNK), FF_CHUNK)
            mpart[h] += jnp.dot(u_all[s], wd[deep, :], preferred_element_type=jnp.float32)

        m_copies = []
        for h in range(GROUPS):
            @pl.loop(0, n_ff)
            def _(c):
                act_partner(h * n_ff + c).wait_recv()
                act_forward(h * n_ff + c).start()

                @pl.when(c >= 1)
                def _():
                    down(h, c - 1)

            down(h, n_ff - 1)
            m_copies.append(send(mpart.at[h], mrecv.at[h], y_ss.at[4 * GROUPS + h], y_rs.at[4 * GROUPS + h]))

        out_copies = []

        def ff_sums(h):
            m_copies[h].wait_recv()
            for block in blocks:
                total = mpart[h, block, :] + mrecv[h, block, :]
                mrecv[h, block, :] = total
                square_sums(h, block, total)
            stats[h] = start_scales(h, 2)

        def ff_residual(h):
            end_scales(h, 2, stats[h])
            for block in blocks:
                value = (arecv[h, block, :] + scaled(h, block, mrecv[h, block, :], 2)).astype(jnp.bfloat16)
                if qkv:
                    hid_ref[h, block, :] = value
                else:
                    hp[h, block, :] = value
            if qkv:
                for block in blocks:
                    square_sums(h, block, hid_ref[h, block, :].astype(jnp.float32))
                stats[h] = start_scales(h, 3)
            else:
                for k, (dev, block) in enumerate(((sib, SIB), (part, PART), (diag, DIAG))):
                    i = 3 + h * 3 + k
                    out_copies.append(send(hp.at[h, block, :], out_ref.at[mine_rows[h], my_cols], misc_ss.at[i], misc_rs.at[i], dev))
                out_ref[mine_rows[h], my_cols] = hp[h, OWN, :]

        def ff_normed(h):
            end_scales(h, 3, stats[h])
            for block in blocks:
                hp[h, block, :] = scaled(h, block, hid_ref[h, block, :].astype(jnp.float32), 3).astype(jnp.bfloat16)
            start_qkv(h)

        ff_sums(0)
        ff_sums(1)
        ff_residual(0)
        ff_sums(2)
        ff_residual(1)
        if qkv:
            ff_normed(0)
        ff_sums(3)
        ff_residual(2)
        if qkv:
            ff_normed(1)
        ff_residual(3)
        if qkv:
            ff_normed(2)
            ff_normed(3)
        if qkv:
            end_qkv()
        for copy in out_copies:
            copy.wait_recv()

        @pl.loop(0, GROUPS * n_ff)
        def _(s):
            for copy in (to_sibling(s), to_partner(s), act_partner(s), act_sibling(s), act_forward(s)):
                copy.wait_send()
    for copy in sends:
        copy.wait_send()


def comm(x, gains, in_weights=None, post=None, layer=0, collective_id=0):
    rows = x.shape[0] // GROUPS
    share = gains.shape[2] // 4
    n_group = rows * 4
    f32, bf16, vmem, hbm = jnp.float32, jnp.bfloat16, pl.BlockSpec(memory_space=pltpu.VMEM), pl.BlockSpec(memory_space=pl.ANY)
    dma = pltpu.SemaphoreType.DMA
    args, specs = [x, gains], [hbm, hbm]
    raw = post is not None and post[0].ndim == 2
    n_stat = 4 * GROUPS
    n_misc = 3 + 3 * GROUPS
    scratch = [pltpu.VMEM(x.shape, bf16), pltpu.VMEM(gains.shape, bf16), pltpu.VMEM((GROUPS, LANES, LANES), f32), pltpu.VMEM((n_stat, 8, LANES), f32), pltpu.VMEM((n_stat, 3, 8, LANES), f32), pltpu.VMEM((GROUPS, n_group, share), bf16),
               dma((n_stat, 3)), dma((n_stat, 3)), dma((n_misc,)), dma((n_misc,)), dma((10,))]
    if post is None:
        scratch.append(pltpu.VMEM(x.shape, bf16))
    n_ff = n_q = 0
    if post is not None:
        residual, w_o, w_gate, w_up, w_down = post
        args += list(post)
        specs += [hbm] * 5
        ff = w_gate.shape[2]
        n_ff = ff // FF_CHUNK
        steps = GROUPS * n_ff
        scratch += [pltpu.VMEM(residual.shape, bf16)] if raw else []
        scratch += [pltpu.VMEM((GROUPS, n_group, share), bf16), pltpu.VMEM((3, GROUPS * rows, w_o.shape[1]), bf16)] + [pltpu.VMEM((GROUPS, n_group, share), f32)] * 4
        scratch += [pltpu.VMEM(w_o.shape[1:], bf16), pltpu.VMEM((share, ff), bf16), pltpu.VMEM((share, ff), bf16), pltpu.VMEM((ff, share), bf16)]
        scratch += [pltpu.VMEM((steps, 2 * rows, 2 * FF_CHUNK), f32)] * 3 + [pltpu.VMEM((steps, rows, 2 * FF_CHUNK), f32), pltpu.VMEM((steps, n_group, FF_CHUNK), bf16)]
        scratch += [dma((5 * GROUPS,)), dma((5 * GROUPS,)), dma((5, steps)), dma((5, steps))]
    if in_weights is not None:
        args += list(in_weights)
        specs += [hbm] * 3
        n_in = sum(w.shape[2] * w.shape[3] for w in in_weights)
        n_q = n_in // QKV_CHUNK
        scratch += [pltpu.VMEM((share, n_in), bf16)] + [pltpu.VMEM(w.shape[1:], bf16) for w in in_weights]
        scratch += [pltpu.VMEM((GROUPS * n_q, 2 * rows, QKV_CHUNK), f32)] * 3 + [pltpu.VMEM((GROUPS * n_q, rows, QKV_CHUNK), f32), dma((2, GROUPS * n_q)), dma((2, GROUPS * n_q))]
        out_shape = [jax.ShapeDtypeStruct((GROUPS, n_group, share), bf16), jax.ShapeDtypeStruct((GROUPS * rows, n_in), f32)][post is None:]
        out_specs = [vmem, vmem][post is None:]
    else:
        out_shape = jax.ShapeDtypeStruct((GROUPS * rows, 4 * share), bf16)
        out_specs = vmem
    cfg = {"raw": raw, "post": post is not None, "qkv": in_weights is not None, "layer": layer, "rows": rows, "share": share, "width": 4 * share, "n_ff": n_ff, "n_q": n_q}
    return pl.pallas_call(
        functools.partial(comm_kernel, cfg),
        out_shape=out_shape, in_specs=specs, out_specs=out_specs, scratch_shapes=scratch,
        compiler_params=pltpu.CompilerParams(collective_id=collective_id, has_side_effects=True, vmem_limit_bytes=62 * 2**20),
        name=f"comm_{collective_id}",
    )(*args)


def solution(mesh):
    def device_step(hidden, positions, k_local, v_local, k_global, v_global, w_q, w_k, w_v, w_o, w_gate, w_up, w_down, norm_gains):
        share = w_q.shape[1]
        tables = rope_tables(positions, w_q.shape[3])
        in_weights = (w_q, w_k, w_v)
        post_weights = (w_o.reshape(2, -1, share), w_gate, w_up, w_down)
        hidden_rows = hidden[:, 0, :]
        qkv, = comm(hidden_rows, norm_gains, in_weights, layer=-1, collective_id=0)
        heads, k_local, v_local = attend(qkv, tables, positions, k_local, v_local)
        residual, qkv = comm(heads, norm_gains, in_weights, (hidden_rows,) + post_weights, layer=0, collective_id=1)
        heads, k_global, v_global = attend(qkv, tables, positions, k_global, v_global)
        final = comm(heads, norm_gains, None, (residual,) + post_weights, layer=1, collective_id=2)[:, None, :]
        return final, k_local, v_local, k_global, v_global

    in_specs = (ROW_SPEC, POS_SPEC, CACHE_SPEC, CACHE_SPEC, CACHE_SPEC, CACHE_SPEC, PROJ_IN_SPEC, PROJ_IN_SPEC, PROJ_IN_SPEC, PROJ_OUT_SPEC, FF_IN_SPEC, FF_IN_SPEC, FF_OUT_SPEC, GAIN_SPEC)
    out_specs = (ROW_SPEC, CACHE_SPEC, CACHE_SPEC, CACHE_SPEC, CACHE_SPEC)
    return jax.shard_map(device_step, mesh=mesh, in_specs=in_specs, out_specs=out_specs, check_vma=False)
```

```python
import functools

import jax
import jax.numpy as jnp
from jax import lax
from jax.experimental import pallas as pl
from jax.experimental.pallas import tpu as pltpu
from jax.sharding import PartitionSpec as P

SOFT_CAP = 50.0
NORM_EPS = 1e-6
ROPE_BASE = 10000.0

ROW_SPEC = P(("part", "data"), None, None)
POS_SPEC = P(("part", "data"))
CACHE_SPEC = P(("part", "data"), None, "model", None)
PROJ_IN_SPEC = P(None, "data", "model", None)
PROJ_OUT_SPEC = P(None, "model", None, "data")
FF_IN_SPEC = P(None, "data", "model")
FF_OUT_SPEC = P(None, "model", "data")
GAIN_SPEC = P(None, None, None)


def rope_tables(positions, head_dim):
    inv_freq = ROPE_BASE ** (-jnp.arange(0, head_dim, 2).astype(jnp.float32) / head_dim)
    angles = positions.astype(jnp.float32)[:, None] * inv_freq[None, :]
    return jnp.cos(angles), jnp.sin(angles)


LANES = 128


def attend_kernel(cache_len, n_rows, group, depth, pos_ref, qkv_ref, cos_ref, sin_ref, k_hbm, v_hbm, head_ref, ko_hbm, vo_hbm, kbuf, vbuf, q8, kn, vn, outs, sbuf, pbuf, rd_sem, wr_sem):
    n_steps = n_rows // group
    n_cols = cache_len * 4

    def reads(step):
        slot = lax.rem(step, depth)
        rows = pl.ds(step * group, group)
        return (pltpu.make_async_copy(k_hbm.at[rows], kbuf.at[slot], rd_sem.at[0, slot]),
                pltpu.make_async_copy(v_hbm.at[rows], vbuf.at[slot], rd_sem.at[1, slot]))

    def writes(step):
        slot = lax.rem(step, depth)
        rows = pl.ds(step * group, group)
        return (pltpu.make_async_copy(kbuf.at[slot], ko_hbm.at[rows], wr_sem.at[0, slot]),
                pltpu.make_async_copy(vbuf.at[slot], vo_hbm.at[rows], wr_sem.at[1, slot]))

    ahead = depth // 2 if depth < n_steps else n_steps
    for step in range(ahead):
        for copy in reads(step):
            copy.start()

    cos_t, sin_t = cos_ref[...], sin_ref[...]
    scale = (2 * LANES) ** -0.5
    for h in range(4):
        first, second = qkv_ref[:, h * 256:h * 256 + LANES], qkv_ref[:, h * 256 + LANES:h * 256 + 256]
        q8[:, h, :] = (first * cos_t - second * sin_t) * scale
        q8[:, 4 + h, :] = (second * cos_t + first * sin_t) * scale
    for h in range(2):
        base = 1024 + h * 256
        first, second = qkv_ref[:, base:base + LANES], qkv_ref[:, base + LANES:base + 256]
        halves = (first * cos_t - second * sin_t, second * cos_t + first * sin_t)
        for half in range(2):
            value = qkv_ref[:, base + 512 + half * LANES:base + 512 + (half + 1) * LANES]
            for i in range(4):
                kn[:, i * 4 + half * 2 + h, :] = halves[half]
                vn[:, i * 4 + half * 2 + h, :] = value

    row_id = lax.broadcasted_iota(jnp.int32, (8, n_cols), 0)
    col_id = lax.broadcasted_iota(jnp.int32, (8, n_cols), 1)
    half_col = (col_id // 2) % 2
    same_half = row_id // 4 == half_col
    same_kv = (row_id // 2) % 2 == col_id % 2
    slot_col = col_id // 4
    sub_id = lax.broadcasted_iota(jnp.int32, (16, LANES), 0) // 4

    @pl.loop(0, n_steps)
    def _(step):
        slot = lax.rem(step, depth)
        if ahead < n_steps:
            @pl.when(step + ahead < n_steps)
            def _():
                @pl.when(step >= depth - ahead)
                def _():
                    for copy in writes(step - (depth - ahead)):
                        copy.wait()
                for copy in reads(step + ahead):
                    copy.start()

        for copy in reads(step):
            copy.wait()
        for i in range(group):
            row = step * group + i
            now = lax.rem(pos_ref[row], cache_len)
            window = pl.ds(pl.multiple_of(now // 4 * 16, 16), 16)
            hit = sub_id == lax.rem(now, 4)
            kbuf[slot, i, window, :] = jnp.where(hit, kn[row].astype(jnp.bfloat16), kbuf[slot, i, window, :])
            vbuf[slot, i, window, :] = jnp.where(hit, vn[row].astype(jnp.bfloat16), vbuf[slot, i, window, :])
        for i in range(group):
            part = lax.dot_general(q8[step * group + i].astype(jnp.bfloat16), kbuf[slot, i], (((1,), (1,)), ((), ())), preferred_element_type=jnp.float32)
            sbuf[i] = jnp.where(same_half & same_kv, part, 0.0)
        for i in range(group):
            part = sbuf[i]
            part = part + pltpu.roll(part, 4, 0)
            other = jnp.where(half_col == 0, pltpu.roll(part, n_cols - 2, 1), pltpu.roll(part, 2, 1))
            scores = SOFT_CAP * jnp.tanh((part + other) / SOFT_CAP)
            scores = jnp.where(same_kv & (slot_col <= pos_ref[step * group + i]), scores, -1e30)
            weights = jnp.exp(scores - jnp.max(scores, axis=1, keepdims=True))
            total = jnp.sum(jnp.where(same_half, weights, 0.0), axis=1, keepdims=True)
            pbuf[i] = jnp.where(same_half, weights / total, 0.0).astype(jnp.bfloat16)
        for i in range(group):
            outs[step * group + i] = jnp.dot(pbuf[i], vbuf[slot, i], preferred_element_type=jnp.float32)
        for copy in writes(step):
            copy.start()

    for h in range(4):
        for half in range(2):
            head_ref[:, h * 256 + half * LANES:h * 256 + (half + 1) * LANES] = outs[:, half * 4 + h, :].astype(jnp.bfloat16)
    for step in range(max(n_steps - depth, 0) if ahead < n_steps else 0, n_steps):
        for copy in writes(step):
            copy.wait()


def attend(qkv, tables, positions, k_cache, v_cache):
    n_rows, cache_len, kv_loc, head_dim = k_cache.shape
    halves = head_dim // LANES
    group = 16 if cache_len <= 64 else 4
    depth = 4 if cache_len <= 64 else 6
    f32, bf16 = jnp.float32, jnp.bfloat16

    def flat(cache):
        return cache.reshape(n_rows, cache_len, kv_loc, halves, LANES).transpose(0, 1, 3, 2, 4).reshape(n_rows, cache_len * halves * kv_loc, LANES)

    def unflat(cache):
        return cache.reshape(n_rows, cache_len, halves, kv_loc, LANES).transpose(0, 1, 3, 2, 4).reshape(n_rows, cache_len, kv_loc, head_dim)

    vmem, hbm = pl.BlockSpec(memory_space=pltpu.VMEM), pl.BlockSpec(memory_space=pl.ANY)
    k_flat, v_flat = flat(k_cache), flat(v_cache)
    n_cols = k_flat.shape[1]
    block = (depth, group, n_cols, LANES)
    dma = pltpu.SemaphoreType.DMA
    heads, k_out, v_out = pl.pallas_call(
        functools.partial(attend_kernel, cache_len, n_rows, group, depth),
        out_shape=(jax.ShapeDtypeStruct((n_rows, 4 * head_dim), bf16), jax.ShapeDtypeStruct(k_flat.shape, bf16), jax.ShapeDtypeStruct(v_flat.shape, bf16)),
        in_specs=[pl.BlockSpec(memory_space=pltpu.SMEM), vmem, vmem, vmem, hbm, hbm],
        out_specs=(vmem, hbm, hbm),
        scratch_shapes=[pltpu.VMEM(block, bf16), pltpu.VMEM(block, bf16), pltpu.VMEM((n_rows, 8, LANES), f32), pltpu.VMEM((n_rows, 16, LANES), f32),
                        pltpu.VMEM((n_rows, 16, LANES), f32), pltpu.VMEM((n_rows, 8, LANES), f32), pltpu.VMEM((group, 8, n_cols), f32), pltpu.VMEM((group, 8, n_cols), bf16),
                        dma((2, depth)), dma((2, depth))],
        compiler_params=pltpu.CompilerParams(vmem_limit_bytes=62 * 2**20),
        cost_estimate=pl.CostEstimate(flops=n_rows * 8 * n_cols * LANES * 4, bytes_accessed=4 * k_flat.size * 2, transcendentals=0),
        name=f"attend_{cache_len}",
    )(positions, qkv, *tables, k_flat, v_flat)
    return heads, unflat(k_out), unflat(v_out)


FF_CHUNK = 512
IN_FLIGHT = 2
QKV_CHUNK = 1024
MESH = pl.DeviceIdType.MESH


GROUPS = 4


def comm_kernel(cfg, *refs):
    it = iter(refs)
    post, layer, rows, share, width = cfg["post"], cfg["layer"], cfg["rows"], cfg["share"], cfg["width"]
    qkv, n_ff, n_q = cfg["qkv"], cfg["n_ff"], cfg["n_q"]
    raw = cfg["raw"]
    x_hbm, g_hbm = next(it), next(it)
    if post:
        res_hbm, wo_hbm, wg_hbm, wu_hbm, wd_hbm = (next(it) for _ in range(5))
    if qkv:
        wq_hbm, wk_hbm, wv_hbm = (next(it) for _ in range(3))
        if post:
            hid_ref = next(it)
        qkv_ref = next(it)
    else:
        out_ref = next(it)
    x_ref, g_ref, tcol, st_src, st_rcv, hp, st_ss, st_rs, misc_ss, misc_rs, ld_sem = (next(it) for _ in range(11))
    if not post:
        out_rows = next(it)
    if post:
        if raw:
            raw_ref = next(it)
        res_ref, hall, apart, arecv, mpart, mrecv, wo, wg, wu, wd, sib_out, sib_in, mine, x_in, u_all = (next(it) for _ in range(15))
        y_ss, y_rs, ff_ss, ff_rs = (next(it) for _ in range(4))
    if qkv:
        wi, wq, wk, wv, q_out, q_in, q_mine, q_x, q_ss, q_rs = (next(it) for _ in range(10))

    model, me = lax.axis_index("model"), lax.axis_index("data")
    x_pos, core = me // 2, lax.rem(me, 2)
    sib, part, diag = x_pos * 2 + 1 - core, (1 - x_pos) * 2 + core, (1 - x_pos) * 2 + 1 - core
    n_group = 4 * rows
    DIAG, SIB, PART, OWN = (pl.ds(i * rows, rows) for i in range(4))
    blocks = (OWN, SIB, PART, DIAG)
    mine_rows = [pl.ds(h * rows, rows) for h in range(GROUPS)]
    sends = []

    def remote(src, dst, send_sem, recv_sem, data=None):
        where = {"data": data} if data is not None else {"model": 1 - model}
        return pltpu.make_async_remote_copy(src_ref=src, dst_ref=dst, send_sem=send_sem, recv_sem=recv_sem, device_id=where, device_id_type=MESH)

    def send(*args):
        copy = remote(*args)
        copy.start()
        sends.append(copy)
        return copy

    def load(src, dst, sem):
        copy = pltpu.make_async_copy(src, dst, sem)
        copy.start()
        return copy

    early = [load(x_hbm, x_ref, ld_sem.at[7]), load(g_hbm, g_ref, ld_sem.at[8])]
    if post:
        early.append(load(res_hbm, raw_ref if raw else res_ref, ld_sem.at[9]))
        wo_load = load(wo_hbm.at[layer], wo, ld_sem.at[0])
        wg_load = load(wg_hbm.at[layer], wg, ld_sem.at[1])
        wu_load = load(wu_hbm.at[layer], wu, ld_sem.at[2])
        wd_load = load(wd_hbm.at[layer], wd, ld_sem.at[3])
    if qkv:
        in_loads = [load(src.at[layer + 1], dst, ld_sem.at[4 + k]) for k, (src, dst) in enumerate(((wq_hbm, wq), (wk_hbm, wk), (wv_hbm, wv)))]

    def relay_weights(c):
        col = c * QKV_CHUNK
        for k in ((0,), (1, 2))[c]:
            in_loads[k].wait()
            weight = (wq, wk, wv)[k]
            n_heads, head_dim = weight.shape[1:]
            for h in range(n_heads):
                wi[:, col:col + head_dim] = weight[:, h, :]
                col += head_dim

    barrier = pltpu.get_barrier_semaphore()
    for dev in (sib, part, diag):
        pl.semaphore_signal(barrier, inc=1, device_id={"data": dev}, device_id_type=MESH)
    pl.semaphore_signal(barrier, inc=1, device_id={"model": 1 - model}, device_id_type=MESH)
    tcol[...] = jnp.zeros_like(tcol)
    for copy in early:
        copy.wait()
    pl.semaphore_wait(barrier, 4)

    def square_sums(h, block, value):
        total = None
        for k in range(share // LANES):
            piece = value[:, k * LANES:(k + 1) * LANES]
            total = piece * piece if total is None else total + piece * piece
        tcol[h, block, :] = total

    lane_block = lax.broadcasted_iota(jnp.int32, (8, LANES), 1) // rows

    def start_scales(h, which):
        idx = which * GROUPS + h
        st_src[idx] = jnp.sum(jnp.transpose(tcol[h]).reshape(LANES // 8, 8, LANES), axis=0)
        return [send(st_src.at[idx], st_rcv.at[idx, k], st_ss.at[idx, k], st_rs.at[idx, k], dev) for k, dev in enumerate((sib, part, diag))]

    def end_scales(h, which, copies):
        idx = which * GROUPS + h
        for copy in copies:
            copy.wait_recv()

        def exchange(value, n):
            even = lax.rem(lane_block // n, 2) == 0
            return jnp.where(even, pltpu.roll(value, LANES - n * rows, 1), pltpu.roll(value, n * rows, 1))

        total = st_src[idx] + exchange(st_rcv[idx, 0], 2) + exchange(st_rcv[idx, 1], 1) + exchange(exchange(st_rcv[idx, 2], 1), 2)
        total = jnp.sum(total, axis=0, keepdims=True)
        inverse = lax.rsqrt(total / width + NORM_EPS)
        tcol[h] = jnp.transpose(jnp.broadcast_to(inverse, (LANES, LANES)))

    def gain_row(k):
        at, which = (layer + 1, 0) if k == 3 else (layer, k + 1)
        return 1.0 + g_ref[at, which:which + 1, pl.ds(pl.multiple_of(me * share, LANES), share)].astype(jnp.float32)

    def scaled(h, block, value, gain):
        return value * jnp.concatenate([tcol[h, block, :]] * (share // LANES), axis=1) * gain_row(gain)

    def q_partner(s):
        return remote(q_mine.at[s, pl.ds(0, rows)], q_x.at[s], q_ss.at[1, s], q_rs.at[1, s], part)

    def start_qkv(h):
        before = None
        for c in range(n_q):
            s = h * n_q + c
            sums = jnp.dot(hp[h], wi[:, c * QKV_CHUNK:(c + 1) * QKV_CHUNK], preferred_element_type=jnp.float32)
            q_out[s] = sums[:2 * rows]
            q_mine[s] = sums[2 * rows:]
            copy = send(q_out.at[s], q_in.at[s], q_ss.at[0, s], q_rs.at[0, s], sib)
            if c >= 1:
                before.wait_recv()
                q_mine[s - 1] = q_mine[s - 1] + q_in[s - 1]
                q_partner(s - 1).start()
            before = copy
        before.wait_recv()
        s = h * n_q + n_q - 1
        q_mine[s] = q_mine[s] + q_in[s]
        q_partner(s).start()

    def end_qkv():
        for h in range(GROUPS):
            for c in range(n_q):
                s = h * n_q + c
                q_partner(s).wait_recv()
                qkv_ref[mine_rows[h], c * QKV_CHUNK:(c + 1) * QKV_CHUNK] = q_mine[s, pl.ds(rows, rows), :] + q_x[s]
        for s in range(GROUPS * n_q):
            q_partner(s).wait_send()

    def spread(src, dst, base):
        copies = []
        for h in range(GROUPS):
            for k, (dev, there) in enumerate(((sib, SIB), (part, PART), (diag, DIAG))):
                cols = pl.ds(pl.multiple_of(dev * share, LANES), share)
                i = base + h * 3 + k
                copies.append(send(src.at[mine_rows[h], cols], dst.at[h, there, :], misc_ss.at[i], misc_rs.at[i], dev))
        return copies

    my_cols = pl.ds(pl.multiple_of(me * share, LANES), share)
    if not post:
        xn = out_rows
        for h in range(GROUPS):
            value = x_ref[mine_rows[h], :].astype(jnp.float32)
            inverse = lax.rsqrt(jnp.mean(value * value, axis=1, keepdims=True) + NORM_EPS)
            xn[mine_rows[h], :] = (value * inverse * (1.0 + g_ref[0, 0:1, :].astype(jnp.float32))).astype(jnp.bfloat16)
        copies = spread(xn, hp, 0)
        relay_weights(0)
        relay_weights(1)
        for h in range(GROUPS):
            hp[h, OWN, :] = xn[mine_rows[h], my_cols]
            for copy in copies[h * 3:h * 3 + 3]:
                copy.wait_recv()
            start_qkv(h)
        end_qkv()
    else:
        to_part = send(x_ref, hall.at[2], misc_ss.at[0], misc_rs.at[0], part)
        to_sib = send(x_ref, hall.at[1], misc_ss.at[1], misc_rs.at[1], sib)
        if raw:
            raw_copies = spread(raw_ref, res_ref, 3)
            for h in range(GROUPS):
                res_ref[h, OWN, :] = raw_ref[mine_rows[h], my_cols]
        wo_load.wait()
        y_copies = [[None] * 4 for _ in range(GROUPS)]

        def project(k, heads):
            sums = jnp.dot(heads, wo[...], preferred_element_type=jnp.float32)
            for h in range(GROUPS):
                apart[h, blocks[k], :] = sums[h * rows:(h + 1) * rows]

        def to_model(*pairs):
            for h, k in pairs:
                y_copies[h][k] = send(apart.at[h, blocks[k], :], arecv.at[h, blocks[k], :], y_ss.at[h * 4 + k], y_rs.at[h * 4 + k])

        project(0, x_ref[...])
        to_model((0, 0), (1, 0))
        to_sib.wait_recv()
        project(1, hall[1])
        to_model((0, 1), (1, 1), (2, 0))
        to_part.wait_recv()
        forward = send(hall.at[2], hall.at[0], misc_ss.at[2], misc_rs.at[2], sib)
        project(2, hall[2])
        to_model((0, 2))
        forward.wait_recv()
        project(3, hall[0])
        to_model((0, 3), (1, 2), (1, 3), (2, 1), (2, 2), (2, 3), (3, 0), (3, 1), (3, 2), (3, 3))
        stats = {}

        def attn_sums(h):
            for k, block in enumerate(blocks):
                y_copies[h][k].wait_recv()
                total = apart[h, block, :] + arecv[h, block, :]
                arecv[h, block, :] = total
                square_sums(h, block, total)
            stats[h] = start_scales(h, 0)

        def attn_residual(h):
            end_scales(h, 0, stats[h])
            if raw:
                for copy in raw_copies[h * 3:h * 3 + 3]:
                    copy.wait_recv()
            for block in blocks:
                residual = res_ref[h, block, :].astype(jnp.float32)
                mid = (residual + scaled(h, block, arecv[h, block, :], 0)).astype(jnp.bfloat16).astype(jnp.float32)
                arecv[h, block, :] = mid
            for block in blocks:
                square_sums(h, block, arecv[h, block, :])
            stats[h] = start_scales(h, 1)

        def attn_normed(h):
            mpart[h] = jnp.zeros((n_group, share), jnp.float32)
            end_scales(h, 1, stats[h])
            for block in blocks:
                hp[h, block, :] = scaled(h, block, arecv[h, block, :], 1).astype(jnp.bfloat16)

        def to_sibling(s):
            return remote(sib_out.at[s], sib_in.at[s], ff_ss.at[0, s], ff_rs.at[0, s], sib)

        def to_partner(s):
            return remote(mine.at[s, pl.ds(0, rows)], x_in.at[s], ff_ss.at[1, s], ff_rs.at[1, s], part)

        def act_partner(s):
            return remote(u_all.at[s, OWN], u_all.at[s, PART], ff_ss.at[2, s], ff_rs.at[2, s], part)

        def act_sibling(s):
            return remote(u_all.at[s, OWN], u_all.at[s, SIB], ff_ss.at[3, s], ff_rs.at[3, s], sib)

        def act_forward(s):
            return remote(u_all.at[s, PART], u_all.at[s, DIAG], ff_ss.at[4, s], ff_rs.at[4, s], sib)

        def add_sibling(s):
            to_sibling(s).wait_recv()
            mine[s] = mine[s] + sib_in[s]

            @pl.when(s >= IN_FLIGHT)
            def _():
                to_partner(s - IN_FLIGHT).wait_send()
            to_partner(s).start()

        def gate_up(h, start, end):
            @pl.loop(start, end)
            def _(c):
                s = h * n_ff + c
                cols = pl.ds(pl.multiple_of(c * FF_CHUNK, FF_CHUNK), FF_CHUNK)
                for k, weight in enumerate((wg, wu)):
                    sums = jnp.dot(hp[h], weight[:, cols], preferred_element_type=jnp.float32)
                    sib_out[s, :, pl.ds(k * FF_CHUNK, FF_CHUNK)] = sums[:2 * rows]
                    mine[s, :, pl.ds(k * FF_CHUNK, FF_CHUNK)] = sums[2 * rows:]
                to_sibling(s).start()

                @pl.when(s >= 1)
                def _():
                    add_sibling(s - 1)

        attn_sums(0)
        attn_residual(0)
        attn_sums(1)
        attn_normed(0)
        wg_load.wait()
        wu_load.wait()
        cuts = (n_ff * 3 // 10, n_ff * 7 // 10)
        for h in range(GROUPS):
            if h + 1 < GROUPS:
                gate_up(h, 0, cuts[0])
                attn_residual(h + 1)
                gate_up(h, cuts[0], cuts[1])
                attn_normed(h + 1)
                if h + 2 < GROUPS:
                    attn_sums(h + 2)
                gate_up(h, cuts[1], n_ff)
            else:
                gate_up(h, 0, n_ff)
        add_sibling(GROUPS * n_ff - 1)
        if qkv:
            relay_weights(0)
            relay_weights(1)

        @pl.loop(0, GROUPS * n_ff)
        def _(s):
            to_partner(s).wait_recv()
            both = mine[s, pl.ds(rows, rows), :] + x_in[s]
            u_all[s, OWN, :] = (jax.nn.gelu(both[:, :FF_CHUNK], approximate=True) * both[:, FF_CHUNK:]).astype(jnp.bfloat16)
            act_partner(s).start()
            act_sibling(s).start()

        wd_load.wait()

        def down(h, c):
            s = h * n_ff + c
            act_sibling(s).wait_recv()
            act_forward(s).wait_recv()
            deep = pl.ds(pl.multiple_of(c * FF_CHUNK, FF_CHUNK), FF_CHUNK)
            mpart[h] += jnp.dot(u_all[s], wd[deep, :], preferred_element_type=jnp.float32)

        m_copies = []
        for h in range(GROUPS):
            @pl.loop(0, n_ff)
            def _(c):
                act_partner(h * n_ff + c).wait_recv()
                act_forward(h * n_ff + c).start()

                @pl.when(c >= 1)
                def _():
                    down(h, c - 1)

            down(h, n_ff - 1)
            m_copies.append(send(mpart.at[h], mrecv.at[h], y_ss.at[4 * GROUPS + h], y_rs.at[4 * GROUPS + h]))

        out_copies = []

        def ff_sums(h):
            m_copies[h].wait_recv()
            for block in blocks:
                total = mpart[h, block, :] + mrecv[h, block, :]
                mrecv[h, block, :] = total
                square_sums(h, block, total)
            stats[h] = start_scales(h, 2)

        def ff_residual(h):
            end_scales(h, 2, stats[h])
            for block in blocks:
                value = (arecv[h, block, :] + scaled(h, block, mrecv[h, block, :], 2)).astype(jnp.bfloat16)
                if qkv:
                    hid_ref[h, block, :] = value
                else:
                    hp[h, block, :] = value
            if qkv:
                for block in blocks:
                    square_sums(h, block, hid_ref[h, block, :].astype(jnp.float32))
                stats[h] = start_scales(h, 3)
            else:
                for k, (dev, block) in enumerate(((sib, SIB), (part, PART), (diag, DIAG))):
                    i = 3 + h * 3 + k
                    out_copies.append(send(hp.at[h, block, :], out_ref.at[mine_rows[h], my_cols], misc_ss.at[i], misc_rs.at[i], dev))
                out_ref[mine_rows[h], my_cols] = hp[h, OWN, :]

        def ff_normed(h):
            end_scales(h, 3, stats[h])
            for block in blocks:
                hp[h, block, :] = scaled(h, block, hid_ref[h, block, :].astype(jnp.float32), 3).astype(jnp.bfloat16)
            start_qkv(h)

        ff_sums(0)
        ff_sums(1)
        ff_residual(0)
        ff_sums(2)
        ff_residual(1)
        if qkv:
            ff_normed(0)
        ff_sums(3)
        ff_residual(2)
        if qkv:
            ff_normed(1)
        ff_residual(3)
        if qkv:
            ff_normed(2)
            ff_normed(3)
        if qkv:
            end_qkv()
        for copy in out_copies:
            copy.wait_recv()

        @pl.loop(0, GROUPS * n_ff)
        def _(s):
            for copy in (to_sibling(s), act_partner(s), act_sibling(s), act_forward(s)):
                copy.wait_send()
        for s in range(GROUPS * n_ff - IN_FLIGHT, GROUPS * n_ff):
            to_partner(s).wait_send()
    for copy in sends:
        copy.wait_send()


def comm(x, gains, in_weights=None, post=None, layer=0, collective_id=0):
    rows = x.shape[0] // GROUPS
    share = gains.shape[2] // 4
    n_group = rows * 4
    f32, bf16, vmem, hbm = jnp.float32, jnp.bfloat16, pl.BlockSpec(memory_space=pltpu.VMEM), pl.BlockSpec(memory_space=pl.ANY)
    dma = pltpu.SemaphoreType.DMA
    args, specs = [x, gains], [hbm, hbm]
    raw = post is not None and post[0].ndim == 2
    n_stat = 4 * GROUPS
    n_misc = 3 + 3 * GROUPS
    scratch = [pltpu.VMEM(x.shape, bf16), pltpu.VMEM(gains.shape, bf16), pltpu.VMEM((GROUPS, LANES, LANES), f32), pltpu.VMEM((n_stat, 8, LANES), f32), pltpu.VMEM((n_stat, 3, 8, LANES), f32), pltpu.VMEM((GROUPS, n_group, share), bf16),
               dma((n_stat, 3)), dma((n_stat, 3)), dma((n_misc,)), dma((n_misc,)), dma((10,))]
    if post is None:
        scratch.append(pltpu.VMEM(x.shape, bf16))
    n_ff = n_q = 0
    if post is not None:
        residual, w_o, w_gate, w_up, w_down = post
        args += list(post)
        specs += [hbm] * 5
        ff = w_gate.shape[2]
        n_ff = ff // FF_CHUNK
        steps = GROUPS * n_ff
        scratch += [pltpu.VMEM(residual.shape, bf16)] if raw else []
        scratch += [pltpu.VMEM((GROUPS, n_group, share), bf16), pltpu.VMEM((3, GROUPS * rows, w_o.shape[1]), bf16)] + [pltpu.VMEM((GROUPS, n_group, share), f32)] * 4
        scratch += [pltpu.VMEM(w_o.shape[1:], bf16), pltpu.VMEM((share, ff), bf16), pltpu.VMEM((share, ff), bf16), pltpu.VMEM((ff, share), bf16)]
        scratch += [pltpu.VMEM((steps, 2 * rows, 2 * FF_CHUNK), f32)] * 3 + [pltpu.VMEM((steps, rows, 2 * FF_CHUNK), f32), pltpu.VMEM((steps, n_group, FF_CHUNK), bf16)]
        scratch += [dma((5 * GROUPS,)), dma((5 * GROUPS,)), dma((5, steps)), dma((5, steps))]
    if in_weights is not None:
        args += list(in_weights)
        specs += [hbm] * 3
        n_in = sum(w.shape[2] * w.shape[3] for w in in_weights)
        n_q = n_in // QKV_CHUNK
        scratch += [pltpu.VMEM((share, n_in), bf16)] + [pltpu.VMEM(w.shape[1:], bf16) for w in in_weights]
        scratch += [pltpu.VMEM((GROUPS * n_q, 2 * rows, QKV_CHUNK), f32)] * 3 + [pltpu.VMEM((GROUPS * n_q, rows, QKV_CHUNK), f32), dma((2, GROUPS * n_q)), dma((2, GROUPS * n_q))]
        out_shape = [jax.ShapeDtypeStruct((GROUPS, n_group, share), bf16), jax.ShapeDtypeStruct((GROUPS * rows, n_in), f32)][post is None:]
        out_specs = [vmem, vmem][post is None:]
    else:
        out_shape = jax.ShapeDtypeStruct((GROUPS * rows, 4 * share), bf16)
        out_specs = vmem
    cfg = {"raw": raw, "post": post is not None, "qkv": in_weights is not None, "layer": layer, "rows": rows, "share": share, "width": 4 * share, "n_ff": n_ff, "n_q": n_q}
    return pl.pallas_call(
        functools.partial(comm_kernel, cfg),
        out_shape=out_shape, in_specs=specs, out_specs=out_specs, scratch_shapes=scratch,
        compiler_params=pltpu.CompilerParams(collective_id=collective_id, has_side_effects=True, vmem_limit_bytes=62 * 2**20),
        name=f"comm_{collective_id}",
    )(*args)


def solution(mesh):
    def device_step(hidden, positions, k_local, v_local, k_global, v_global, w_q, w_k, w_v, w_o, w_gate, w_up, w_down, norm_gains):
        share = w_q.shape[1]
        tables = rope_tables(positions, w_q.shape[3])
        in_weights = (w_q, w_k, w_v)
        post_weights = (w_o.reshape(2, -1, share), w_gate, w_up, w_down)
        hidden_rows = hidden[:, 0, :]
        qkv, = comm(hidden_rows, norm_gains, in_weights, layer=-1, collective_id=0)
        heads, k_local, v_local = attend(qkv, tables, positions, k_local, v_local)
        residual, qkv = comm(heads, norm_gains, in_weights, (hidden_rows,) + post_weights, layer=0, collective_id=1)
        heads, k_global, v_global = attend(qkv, tables, positions, k_global, v_global)
        final = comm(heads, norm_gains, None, (residual,) + post_weights, layer=1, collective_id=2)[:, None, :]
        return final, k_local, v_local, k_global, v_global

    in_specs = (ROW_SPEC, POS_SPEC, CACHE_SPEC, CACHE_SPEC, CACHE_SPEC, CACHE_SPEC, PROJ_IN_SPEC, PROJ_IN_SPEC, PROJ_IN_SPEC, PROJ_OUT_SPEC, FF_IN_SPEC, FF_IN_SPEC, FF_OUT_SPEC, GAIN_SPEC)
    out_specs = (ROW_SPEC, CACHE_SPEC, CACHE_SPEC, CACHE_SPEC, CACHE_SPEC)
    return jax.shard_map(device_step, mesh=mesh, in_specs=in_specs, out_specs=out_specs, check_vma=False)
```

```python
import functools

import jax
import jax.numpy as jnp
from jax import lax
from jax.experimental import pallas as pl
from jax.experimental.pallas import tpu as pltpu
from jax.sharding import PartitionSpec as P

SOFT_CAP = 50.0
NORM_EPS = 1e-6
ROPE_BASE = 10000.0

ROW_SPEC = P(("part", "data"), None, None)
POS_SPEC = P(("part", "data"))
CACHE_SPEC = P(("part", "data"), None, "model", None)
PROJ_IN_SPEC = P(None, "data", "model", None)
PROJ_OUT_SPEC = P(None, "model", None, "data")
FF_IN_SPEC = P(None, "data", "model")
FF_OUT_SPEC = P(None, "model", "data")
GAIN_SPEC = P(None, None, None)


def rope_tables(positions, head_dim):
    inv_freq = ROPE_BASE ** (-jnp.arange(0, head_dim, 2).astype(jnp.float32) / head_dim)
    angles = positions.astype(jnp.float32)[:, None] * inv_freq[None, :]
    return jnp.cos(angles), jnp.sin(angles)


LANES = 128


def attend_kernel(cache_len, n_rows, group, depth, pos_ref, qkv_hbm, cos_hbm, sin_hbm, k_hbm, v_hbm, head_hbm, ko_hbm, vo_hbm, qkv_ref, cos_ref, sin_ref, head_ref, kbuf, vbuf, q8, kn, vn, outs, sbuf, pbuf, io_sem, rd_sem, wr_sem):
    n_steps = n_rows // group
    n_cols = cache_len * 4

    def reads(step):
        slot = lax.rem(step, depth)
        rows = pl.ds(step * group, group)
        return (pltpu.make_async_copy(k_hbm.at[rows], kbuf.at[slot], rd_sem.at[0, slot]),
                pltpu.make_async_copy(v_hbm.at[rows], vbuf.at[slot], rd_sem.at[1, slot]))

    def writes(step):
        slot = lax.rem(step, depth)
        rows = pl.ds(step * group, group)
        return (pltpu.make_async_copy(kbuf.at[slot], ko_hbm.at[rows], wr_sem.at[0, slot]),
                pltpu.make_async_copy(vbuf.at[slot], vo_hbm.at[rows], wr_sem.at[1, slot]))

    loads = [pltpu.make_async_copy(src, dst, io_sem.at[k]) for k, (src, dst) in enumerate(((qkv_hbm, qkv_ref), (cos_hbm, cos_ref), (sin_hbm, sin_ref)))]
    for copy in loads:
        copy.start()
    ahead = depth // 2 if depth < n_steps else n_steps
    for step in range(ahead):
        for copy in reads(step):
            copy.start()
    for copy in loads:
        copy.wait()

    cos_t, sin_t = cos_ref[...], sin_ref[...]
    scale = (2 * LANES) ** -0.5
    for h in range(4):
        first, second = qkv_ref[:, h * 256:h * 256 + LANES], qkv_ref[:, h * 256 + LANES:h * 256 + 256]
        q8[:, h, :] = (first * cos_t - second * sin_t) * scale
        q8[:, 4 + h, :] = (second * cos_t + first * sin_t) * scale
    for h in range(2):
        base = 1024 + h * 256
        first, second = qkv_ref[:, base:base + LANES], qkv_ref[:, base + LANES:base + 256]
        halves = (first * cos_t - second * sin_t, second * cos_t + first * sin_t)
        for half in range(2):
            value = qkv_ref[:, base + 512 + half * LANES:base + 512 + (half + 1) * LANES]
            for i in range(4):
                kn[:, i * 4 + half * 2 + h, :] = halves[half]
                vn[:, i * 4 + half * 2 + h, :] = value

    row_id = lax.broadcasted_iota(jnp.int32, (8, n_cols), 0)
    col_id = lax.broadcasted_iota(jnp.int32, (8, n_cols), 1)
    half_col = (col_id // 2) % 2
    same_half = row_id // 4 == half_col
    same_kv = (row_id // 2) % 2 == col_id % 2
    slot_col = col_id // 4
    sub_id = lax.broadcasted_iota(jnp.int32, (16, LANES), 0) // 4

    @pl.loop(0, n_steps)
    def _(step):
        slot = lax.rem(step, depth)
        if ahead < n_steps:
            @pl.when(step + ahead < n_steps)
            def _():
                @pl.when(step >= depth - ahead)
                def _():
                    for copy in writes(step - (depth - ahead)):
                        copy.wait()
                for copy in reads(step + ahead):
                    copy.start()

        for copy in reads(step):
            copy.wait()
        for i in range(group):
            row = step * group + i
            now = lax.rem(pos_ref[row], cache_len)
            window = pl.ds(pl.multiple_of(now // 4 * 16, 16), 16)
            hit = sub_id == lax.rem(now, 4)
            kbuf[slot, i, window, :] = jnp.where(hit, kn[row].astype(jnp.bfloat16), kbuf[slot, i, window, :])
            vbuf[slot, i, window, :] = jnp.where(hit, vn[row].astype(jnp.bfloat16), vbuf[slot, i, window, :])
        for i in range(group):
            part = lax.dot_general(q8[step * group + i].astype(jnp.bfloat16), kbuf[slot, i], (((1,), (1,)), ((), ())), preferred_element_type=jnp.float32)
            sbuf[i] = jnp.where(same_half & same_kv, part, 0.0)
        for i in range(group):
            part = sbuf[i]
            part = part + pltpu.roll(part, 4, 0)
            other = jnp.where(half_col == 0, pltpu.roll(part, n_cols - 2, 1), pltpu.roll(part, 2, 1))
            scores = SOFT_CAP * jnp.tanh((part + other) / SOFT_CAP)
            scores = jnp.where(same_kv & (slot_col <= pos_ref[step * group + i]), scores, -1e30)
            weights = jnp.exp(scores - jnp.max(scores, axis=1, keepdims=True))
            total = jnp.sum(jnp.where(same_half, weights, 0.0), axis=1, keepdims=True)
            pbuf[i] = jnp.where(same_half, weights / total, 0.0).astype(jnp.bfloat16)
        for i in range(group):
            outs[step * group + i] = jnp.dot(pbuf[i], vbuf[slot, i], preferred_element_type=jnp.float32)
        for copy in writes(step):
            copy.start()

    for h in range(4):
        for half in range(2):
            head_ref[:, h * 256 + half * LANES:h * 256 + (half + 1) * LANES] = outs[:, half * 4 + h, :].astype(jnp.bfloat16)
    heads_out = pltpu.make_async_copy(head_ref, head_hbm, io_sem.at[3])
    heads_out.start()
    for step in range(max(n_steps - depth, 0) if ahead < n_steps else 0, n_steps):
        for copy in writes(step):
            copy.wait()
    heads_out.wait()


def attend(qkv, tables, positions, k_cache, v_cache):
    n_rows, cache_len, kv_loc, head_dim = k_cache.shape
    halves = head_dim // LANES
    group = 16 if cache_len <= 64 else 4
    depth = 4 if cache_len <= 64 else 6
    f32, bf16 = jnp.float32, jnp.bfloat16

    def flat(cache):
        return cache.reshape(n_rows, cache_len, kv_loc, halves, LANES).transpose(0, 1, 3, 2, 4).reshape(n_rows, cache_len * halves * kv_loc, LANES)

    def unflat(cache):
        return cache.reshape(n_rows, cache_len, halves, kv_loc, LANES).transpose(0, 1, 3, 2, 4).reshape(n_rows, cache_len, kv_loc, head_dim)

    hbm = pl.BlockSpec(memory_space=pl.ANY)
    k_flat, v_flat = flat(k_cache), flat(v_cache)
    n_cols = k_flat.shape[1]
    block = (depth, group, n_cols, LANES)
    dma = pltpu.SemaphoreType.DMA
    heads, k_out, v_out = pl.pallas_call(
        functools.partial(attend_kernel, cache_len, n_rows, group, depth),
        out_shape=(jax.ShapeDtypeStruct((n_rows, 4 * head_dim), bf16), jax.ShapeDtypeStruct(k_flat.shape, bf16), jax.ShapeDtypeStruct(v_flat.shape, bf16)),
        in_specs=[pl.BlockSpec(memory_space=pltpu.SMEM), hbm, hbm, hbm, hbm, hbm],
        out_specs=(hbm, hbm, hbm),
        scratch_shapes=[pltpu.VMEM(qkv.shape, f32), pltpu.VMEM(tables[0].shape, f32), pltpu.VMEM(tables[0].shape, f32), pltpu.VMEM((n_rows, 4 * head_dim), bf16),
                        pltpu.VMEM(block, bf16), pltpu.VMEM(block, bf16), pltpu.VMEM((n_rows, 8, LANES), f32), pltpu.VMEM((n_rows, 16, LANES), f32),
                        pltpu.VMEM((n_rows, 16, LANES), f32), pltpu.VMEM((n_rows, 8, LANES), f32), pltpu.VMEM((group, 8, n_cols), f32), pltpu.VMEM((group, 8, n_cols), bf16),
                        dma((4,)), dma((2, depth)), dma((2, depth))],
        compiler_params=pltpu.CompilerParams(vmem_limit_bytes=62 * 2**20),
        cost_estimate=pl.CostEstimate(flops=n_rows * 8 * n_cols * LANES * 4, bytes_accessed=4 * k_flat.size * 2, transcendentals=0),
        name=f"attend_{cache_len}",
    )(positions, qkv, *tables, k_flat, v_flat)
    return heads, unflat(k_out), unflat(v_out)


FF_CHUNK = 512
IN_FLIGHT = 2
QKV_CHUNK = 1024
MESH = pl.DeviceIdType.MESH


GROUPS = 4


def comm_kernel(cfg, *refs):
    it = iter(refs)
    post, layer, rows, share, width = cfg["post"], cfg["layer"], cfg["rows"], cfg["share"], cfg["width"]
    qkv, n_ff, n_q = cfg["qkv"], cfg["n_ff"], cfg["n_q"]
    raw = cfg["raw"]
    x_hbm, g_hbm = next(it), next(it)
    if post:
        res_hbm, wo_hbm, wg_hbm, wu_hbm, wd_hbm = (next(it) for _ in range(5))
    if qkv:
        wq_hbm, wk_hbm, wv_hbm = (next(it) for _ in range(3))
        if post:
            hid_ref = next(it)
        qkv_ref = next(it)
    else:
        out_ref = next(it)
    x_ref, g_ref, tcol, st_src, st_rcv, hp, st_ss, st_rs, misc_ss, misc_rs, ld_sem = (next(it) for _ in range(11))
    if not post:
        out_rows = next(it)
    if post:
        if raw:
            raw_ref = next(it)
        res_ref, hall, apart, arecv, mpart, mrecv, wo, wg, wu, wd, sib_out, sib_in, mine, x_in, u_all = (next(it) for _ in range(15))
        y_ss, y_rs, ff_ss, ff_rs = (next(it) for _ in range(4))
    if qkv:
        wi, wq, wk, wv, q_out, q_in, q_mine, q_x, q_ss, q_rs = (next(it) for _ in range(10))

    model, me = lax.axis_index("model"), lax.axis_index("data")
    x_pos, core = me // 2, lax.rem(me, 2)
    sib, part, diag = x_pos * 2 + 1 - core, (1 - x_pos) * 2 + core, (1 - x_pos) * 2 + 1 - core
    n_group = 4 * rows
    DIAG, SIB, PART, OWN = (pl.ds(i * rows, rows) for i in range(4))
    blocks = (OWN, SIB, PART, DIAG)
    mine_rows = [pl.ds(h * rows, rows) for h in range(GROUPS)]
    sends = []

    def remote(src, dst, send_sem, recv_sem, data=None):
        where = {"data": data} if data is not None else {"model": 1 - model}
        return pltpu.make_async_remote_copy(src_ref=src, dst_ref=dst, send_sem=send_sem, recv_sem=recv_sem, device_id=where, device_id_type=MESH)

    def send(*args):
        copy = remote(*args)
        copy.start()
        sends.append(copy)
        return copy

    def load(src, dst, sem):
        copy = pltpu.make_async_copy(src, dst, sem)
        copy.start()
        return copy

    early = [load(x_hbm, x_ref, ld_sem.at[7]), load(g_hbm, g_ref, ld_sem.at[8])]
    if post:
        early.append(load(res_hbm, raw_ref if raw else res_ref, ld_sem.at[9]))
        wo_load = load(wo_hbm.at[layer], wo, ld_sem.at[0])
        wg_load = load(wg_hbm.at[layer], wg, ld_sem.at[1])
        wu_load = load(wu_hbm.at[layer], wu, ld_sem.at[2])
        wd_load = load(wd_hbm.at[layer], wd, ld_sem.at[3])
    if qkv:
        in_loads = [load(src.at[layer + 1], dst, ld_sem.at[4 + k]) for k, (src, dst) in enumerate(((wq_hbm, wq), (wk_hbm, wk), (wv_hbm, wv)))]

    def relay_weights(c):
        col = c * QKV_CHUNK
        for k in ((0,), (1, 2))[c]:
            in_loads[k].wait()
            weight = (wq, wk, wv)[k]
            n_heads, head_dim = weight.shape[1:]
            for h in range(n_heads):
                wi[:, col:col + head_dim] = weight[:, h, :]
                col += head_dim

    barrier = pltpu.get_barrier_semaphore()
    for dev in (sib, part, diag):
        pl.semaphore_signal(barrier, inc=1, device_id={"data": dev}, device_id_type=MESH)
    pl.semaphore_signal(barrier, inc=1, device_id={"model": 1 - model}, device_id_type=MESH)
    tcol[...] = jnp.zeros_like(tcol)
    for copy in early:
        copy.wait()
    pl.semaphore_wait(barrier, 4)

    def square_sums(h, block, value):
        total = None
        for k in range(share // LANES):
            piece = value[:, k * LANES:(k + 1) * LANES]
            total = piece * piece if total is None else total + piece * piece
        tcol[h, block, :] = total

    lane_block = lax.broadcasted_iota(jnp.int32, (8, LANES), 1) // rows

    def start_scales(h, which):
        idx = which * GROUPS + h
        st_src[idx] = jnp.sum(jnp.transpose(tcol[h]).reshape(LANES // 8, 8, LANES), axis=0)
        return [send(st_src.at[idx], st_rcv.at[idx, k], st_ss.at[idx, k], st_rs.at[idx, k], dev) for k, dev in enumerate((sib, part, diag))]

    def end_scales(h, which, copies):
        idx = which * GROUPS + h
        for copy in copies:
            copy.wait_recv()

        def exchange(value, n):
            even = lax.rem(lane_block // n, 2) == 0
            return jnp.where(even, pltpu.roll(value, LANES - n * rows, 1), pltpu.roll(value, n * rows, 1))

        total = st_src[idx] + exchange(st_rcv[idx, 0], 2) + exchange(st_rcv[idx, 1], 1) + exchange(exchange(st_rcv[idx, 2], 1), 2)
        total = jnp.sum(total, axis=0, keepdims=True)
        inverse = lax.rsqrt(total / width + NORM_EPS)
        tcol[h] = jnp.transpose(jnp.broadcast_to(inverse, (LANES, LANES)))

    def gain_row(k):
        at, which = (layer + 1, 0) if k == 3 else (layer, k + 1)
        return 1.0 + g_ref[at, which:which + 1, pl.ds(pl.multiple_of(me * share, LANES), share)].astype(jnp.float32)

    def scaled(h, block, value, gain):
        return value * jnp.concatenate([tcol[h, block, :]] * (share // LANES), axis=1) * gain_row(gain)

    def q_partner(s):
        return remote(q_mine.at[s, pl.ds(0, rows)], q_x.at[s], q_ss.at[1, s], q_rs.at[1, s], part)

    def start_qkv(h):
        before = None
        for c in range(n_q):
            s = h * n_q + c
            sums = jnp.dot(hp[h], wi[:, c * QKV_CHUNK:(c + 1) * QKV_CHUNK], preferred_element_type=jnp.float32)
            q_out[s] = sums[:2 * rows]
            q_mine[s] = sums[2 * rows:]
            copy = send(q_out.at[s], q_in.at[s], q_ss.at[0, s], q_rs.at[0, s], sib)
            if c >= 1:
                before.wait_recv()
                q_mine[s - 1] = q_mine[s - 1] + q_in[s - 1]
                q_partner(s - 1).start()
            before = copy
        before.wait_recv()
        s = h * n_q + n_q - 1
        q_mine[s] = q_mine[s] + q_in[s]
        q_partner(s).start()

    def end_qkv():
        for h in range(GROUPS):
            for c in range(n_q):
                s = h * n_q + c
                q_partner(s).wait_recv()
                qkv_ref[mine_rows[h], c * QKV_CHUNK:(c + 1) * QKV_CHUNK] = q_mine[s, pl.ds(rows, rows), :] + q_x[s]
        for s in range(GROUPS * n_q):
            q_partner(s).wait_send()

    def spread(src, dst, base):
        copies = []
        for h in range(GROUPS):
            for k, (dev, there) in enumerate(((sib, SIB), (part, PART), (diag, DIAG))):
                cols = pl.ds(pl.multiple_of(dev * share, LANES), share)
                i = base + h * 3 + k
                copies.append(send(src.at[mine_rows[h], cols], dst.at[h, there, :], misc_ss.at[i], misc_rs.at[i], dev))
        return copies

    my_cols = pl.ds(pl.multiple_of(me * share, LANES), share)
    if not post:
        xn = out_rows
        for h in range(GROUPS):
            value = x_ref[mine_rows[h], :].astype(jnp.float32)
            inverse = lax.rsqrt(jnp.mean(value * value, axis=1, keepdims=True) + NORM_EPS)
            xn[mine_rows[h], :] = (value * inverse * (1.0 + g_ref[0, 0:1, :].astype(jnp.float32))).astype(jnp.bfloat16)
        copies = spread(xn, hp, 0)
        relay_weights(0)
        relay_weights(1)
        for h in range(GROUPS):
            hp[h, OWN, :] = xn[mine_rows[h], my_cols]
            for copy in copies[h * 3:h * 3 + 3]:
                copy.wait_recv()
            start_qkv(h)
        end_qkv()
    else:
        head_cuts = (pl.ds(0, rows), pl.ds(rows, (GROUPS - 1) * rows))
        to_part = [send(x_ref.at[cut], hall.at[2, cut], misc_ss.at[n], misc_rs.at[n], part) for n, cut in enumerate(head_cuts)]
        to_sib = send(x_ref, hall.at[1], misc_ss.at[2], misc_rs.at[2], sib)
        if raw:
            raw_copies = spread(raw_ref, res_ref, 5)
            for h in range(GROUPS):
                res_ref[h, OWN, :] = raw_ref[mine_rows[h], my_cols]
        wo_load.wait()
        y_copies = [[None] * 4 for _ in range(GROUPS)]

        def project(heads, places):
            sums = jnp.dot(heads, wo[...], preferred_element_type=jnp.float32)
            for n, (h, k) in enumerate(places):
                apart[h, blocks[k], :] = sums[n * rows:(n + 1) * rows]

        def to_model(*pairs):
            for h, k in pairs:
                y_copies[h][k] = send(apart.at[h, blocks[k], :], arecv.at[h, blocks[k], :], y_ss.at[h * 4 + k], y_rs.at[h * 4 + k])

        def forward(n):
            to_part[n].wait_recv()
            return send(hall.at[2, head_cuts[n]], hall.at[0, head_cuts[n]], misc_ss.at[3 + n], misc_rs.at[3 + n], sib)

        project(x_ref[...], [(h, 0) for h in range(GROUPS)])
        to_model((0, 0), (1, 0))
        to_sib.wait_recv()
        project(hall[1], [(h, 1) for h in range(GROUPS)])
        to_model((0, 1), (1, 1))
        forward(0).wait_recv()
        project(jnp.concatenate([hall[2, head_cuts[0], :], hall[0, head_cuts[0], :]], axis=0), [(0, 2), (0, 3)])
        to_model((0, 2), (0, 3), (2, 0), (2, 1))
        rest = forward(1)
        project(hall[2, head_cuts[1], :], [(h, 2) for h in range(1, GROUPS)])
        to_model((1, 2))
        rest.wait_recv()
        project(hall[0, head_cuts[1], :], [(h, 3) for h in range(1, GROUPS)])
        to_model((1, 3), (2, 2), (2, 3), (3, 0), (3, 1), (3, 2), (3, 3))
        stats = {}

        def attn_sums(h):
            for k, block in enumerate(blocks):
                y_copies[h][k].wait_recv()
                total = apart[h, block, :] + arecv[h, block, :]
                arecv[h, block, :] = total
                square_sums(h, block, total)
            stats[h] = start_scales(h, 0)

        def attn_residual(h):
            end_scales(h, 0, stats[h])
            if raw:
                for copy in raw_copies[h * 3:h * 3 + 3]:
                    copy.wait_recv()
            for block in blocks:
                residual = res_ref[h, block, :].astype(jnp.float32)
                mid = (residual + scaled(h, block, arecv[h, block, :], 0)).astype(jnp.bfloat16).astype(jnp.float32)
                arecv[h, block, :] = mid
            for block in blocks:
                square_sums(h, block, arecv[h, block, :])
            stats[h] = start_scales(h, 1)

        def attn_normed(h):
            mpart[h] = jnp.zeros((n_group, share), jnp.float32)
            end_scales(h, 1, stats[h])
            for block in blocks:
                hp[h, block, :] = scaled(h, block, arecv[h, block, :], 1).astype(jnp.bfloat16)

        def to_sibling(s):
            return remote(sib_out.at[s], sib_in.at[s], ff_ss.at[0, s], ff_rs.at[0, s], sib)

        def to_partner(s):
            return remote(mine.at[s, pl.ds(0, rows)], x_in.at[s], ff_ss.at[1, s], ff_rs.at[1, s], part)

        def act_partner(s):
            return remote(u_all.at[s, OWN], u_all.at[s, PART], ff_ss.at[2, s], ff_rs.at[2, s], part)

        def act_sibling(s):
            return remote(u_all.at[s, OWN], u_all.at[s, SIB], ff_ss.at[3, s], ff_rs.at[3, s], sib)

        def act_forward(s):
            return remote(u_all.at[s, PART], u_all.at[s, DIAG], ff_ss.at[4, s], ff_rs.at[4, s], sib)

        def add_sibling(s):
            to_sibling(s).wait_recv()
            mine[s] = mine[s] + sib_in[s]

            @pl.when(s >= IN_FLIGHT)
            def _():
                to_partner(s - IN_FLIGHT).wait_send()
            to_partner(s).start()

        def gate_up(h, start, end):
            @pl.loop(start, end)
            def _(c):
                s = h * n_ff + c
                cols = pl.ds(pl.multiple_of(c * FF_CHUNK, FF_CHUNK), FF_CHUNK)
                for k, weight in enumerate((wg, wu)):
                    sums = jnp.dot(hp[h], weight[:, cols], preferred_element_type=jnp.float32)
                    sib_out[s, :, pl.ds(k * FF_CHUNK, FF_CHUNK)] = sums[:2 * rows]
                    mine[s, :, pl.ds(k * FF_CHUNK, FF_CHUNK)] = sums[2 * rows:]
                to_sibling(s).start()

                @pl.when(s >= 1)
                def _():
                    add_sibling(s - 1)

        attn_sums(0)
        if qkv:
            relay_weights(0)
        attn_residual(0)
        if qkv:
            relay_weights(1)
        attn_sums(1)
        attn_normed(0)
        wg_load.wait()
        wu_load.wait()
        cuts = (n_ff * 3 // 10, n_ff * 7 // 10)
        for h in range(GROUPS):
            if h + 1 < GROUPS:
                gate_up(h, 0, cuts[0])
                attn_residual(h + 1)
                gate_up(h, cuts[0], cuts[1])
                attn_normed(h + 1)
                if h + 2 < GROUPS:
                    attn_sums(h + 2)
                gate_up(h, cuts[1], n_ff)
            else:
                gate_up(h, 0, n_ff)
        add_sibling(GROUPS * n_ff - 1)
        @pl.loop(0, GROUPS * n_ff)
        def _(s):
            to_partner(s).wait_recv()
            both = mine[s, pl.ds(rows, rows), :] + x_in[s]
            u_all[s, OWN, :] = (jax.nn.gelu(both[:, :FF_CHUNK], approximate=True) * both[:, FF_CHUNK:]).astype(jnp.bfloat16)
            act_partner(s).start()
            act_sibling(s).start()

        wd_load.wait()

        def down(h, c):
            s = h * n_ff + c
            act_sibling(s).wait_recv()
            act_forward(s).wait_recv()
            deep = pl.ds(pl.multiple_of(c * FF_CHUNK, FF_CHUNK), FF_CHUNK)
            mpart[h] += jnp.dot(u_all[s], wd[deep, :], preferred_element_type=jnp.float32)

        m_copies = []
        for h in range(GROUPS):
            @pl.loop(0, n_ff)
            def _(c):
                act_partner(h * n_ff + c).wait_recv()
                act_forward(h * n_ff + c).start()

                @pl.when(c >= 1)
                def _():
                    down(h, c - 1)

            down(h, n_ff - 1)
            m_copies.append(send(mpart.at[h], mrecv.at[h], y_ss.at[4 * GROUPS + h], y_rs.at[4 * GROUPS + h]))

        out_copies = []

        def ff_sums(h):
            m_copies[h].wait_recv()
            for block in blocks:
                total = mpart[h, block, :] + mrecv[h, block, :]
                mrecv[h, block, :] = total
                square_sums(h, block, total)
            stats[h] = start_scales(h, 2)

        def ff_residual(h):
            end_scales(h, 2, stats[h])
            for block in blocks:
                value = (arecv[h, block, :] + scaled(h, block, mrecv[h, block, :], 2)).astype(jnp.bfloat16)
                if qkv:
                    hid_ref[h, block, :] = value
                else:
                    hp[h, block, :] = value
            if qkv:
                for block in blocks:
                    square_sums(h, block, hid_ref[h, block, :].astype(jnp.float32))
                stats[h] = start_scales(h, 3)
            else:
                for k, (dev, block) in enumerate(((sib, SIB), (part, PART), (diag, DIAG))):
                    i = 5 + h * 3 + k
                    out_copies.append(send(hp.at[h, block, :], out_ref.at[mine_rows[h], my_cols], misc_ss.at[i], misc_rs.at[i], dev))
                out_ref[mine_rows[h], my_cols] = hp[h, OWN, :]

        def ff_normed(h):
            end_scales(h, 3, stats[h])
            for block in blocks:
                hp[h, block, :] = scaled(h, block, hid_ref[h, block, :].astype(jnp.float32), 3).astype(jnp.bfloat16)
            start_qkv(h)

        ff_sums(0)
        ff_sums(1)
        ff_residual(0)
        ff_sums(2)
        ff_residual(1)
        if qkv:
            ff_normed(0)
        ff_sums(3)
        ff_residual(2)
        if qkv:
            ff_normed(1)
        ff_residual(3)
        if qkv:
            ff_normed(2)
            ff_normed(3)
        if qkv:
            end_qkv()
        for copy in out_copies:
            copy.wait_recv()

        @pl.loop(0, GROUPS * n_ff)
        def _(s):
            for copy in (to_sibling(s), act_partner(s), act_sibling(s), act_forward(s)):
                copy.wait_send()
        for s in range(GROUPS * n_ff - IN_FLIGHT, GROUPS * n_ff):
            to_partner(s).wait_send()
    for copy in sends:
        copy.wait_send()


def comm(x, gains, in_weights=None, post=None, layer=0, collective_id=0):
    rows = x.shape[0] // GROUPS
    share = gains.shape[2] // 4
    n_group = rows * 4
    f32, bf16, vmem, hbm = jnp.float32, jnp.bfloat16, pl.BlockSpec(memory_space=pltpu.VMEM), pl.BlockSpec(memory_space=pl.ANY)
    dma = pltpu.SemaphoreType.DMA
    args, specs = [x, gains], [hbm, hbm]
    raw = post is not None and post[0].ndim == 2
    n_stat = 4 * GROUPS
    n_misc = 5 + 3 * GROUPS
    scratch = [pltpu.VMEM(x.shape, bf16), pltpu.VMEM(gains.shape, bf16), pltpu.VMEM((GROUPS, LANES, LANES), f32), pltpu.VMEM((n_stat, 8, LANES), f32), pltpu.VMEM((n_stat, 3, 8, LANES), f32), pltpu.VMEM((GROUPS, n_group, share), bf16),
               dma((n_stat, 3)), dma((n_stat, 3)), dma((n_misc,)), dma((n_misc,)), dma((10,))]
    if post is None:
        scratch.append(pltpu.VMEM(x.shape, bf16))
    n_ff = n_q = 0
    if post is not None:
        residual, w_o, w_gate, w_up, w_down = post
        args += list(post)
        specs += [hbm] * 5
        ff = w_gate.shape[2]
        n_ff = ff // FF_CHUNK
        steps = GROUPS * n_ff
        scratch += [pltpu.VMEM(residual.shape, bf16)] if raw else []
        scratch += [pltpu.VMEM((GROUPS, n_group, share), bf16), pltpu.VMEM((3, GROUPS * rows, w_o.shape[1]), bf16)] + [pltpu.VMEM((GROUPS, n_group, share), f32)] * 4
        scratch += [pltpu.VMEM(w_o.shape[1:], bf16), pltpu.VMEM((share, ff), bf16), pltpu.VMEM((share, ff), bf16), pltpu.VMEM((ff, share), bf16)]
        scratch += [pltpu.VMEM((steps, 2 * rows, 2 * FF_CHUNK), f32)] * 3 + [pltpu.VMEM((steps, rows, 2 * FF_CHUNK), f32), pltpu.VMEM((steps, n_group, FF_CHUNK), bf16)]
        scratch += [dma((5 * GROUPS,)), dma((5 * GROUPS,)), dma((5, steps)), dma((5, steps))]
    if in_weights is not None:
        args += list(in_weights)
        specs += [hbm] * 3
        n_in = sum(w.shape[2] * w.shape[3] for w in in_weights)
        n_q = n_in // QKV_CHUNK
        scratch += [pltpu.VMEM((share, n_in), bf16)] + [pltpu.VMEM(w.shape[1:], bf16) for w in in_weights]
        scratch += [pltpu.VMEM((GROUPS * n_q, 2 * rows, QKV_CHUNK), f32)] * 3 + [pltpu.VMEM((GROUPS * n_q, rows, QKV_CHUNK), f32), dma((2, GROUPS * n_q)), dma((2, GROUPS * n_q))]
        out_shape = [jax.ShapeDtypeStruct((GROUPS, n_group, share), bf16), jax.ShapeDtypeStruct((GROUPS * rows, n_in), f32)][post is None:]
        out_specs = [vmem, vmem][post is None:]
    else:
        out_shape = jax.ShapeDtypeStruct((GROUPS * rows, 4 * share), bf16)
        out_specs = vmem
    cfg = {"raw": raw, "post": post is not None, "qkv": in_weights is not None, "layer": layer, "rows": rows, "share": share, "width": 4 * share, "n_ff": n_ff, "n_q": n_q}
    return pl.pallas_call(
        functools.partial(comm_kernel, cfg),
        out_shape=out_shape, in_specs=specs, out_specs=out_specs, scratch_shapes=scratch,
        compiler_params=pltpu.CompilerParams(collective_id=collective_id, has_side_effects=True, vmem_limit_bytes=62 * 2**20),
        name=f"comm_{collective_id}",
    )(*args)


def solution(mesh):
    def device_step(hidden, positions, k_local, v_local, k_global, v_global, w_q, w_k, w_v, w_o, w_gate, w_up, w_down, norm_gains):
        share = w_q.shape[1]
        tables = rope_tables(positions, w_q.shape[3])
        in_weights = (w_q, w_k, w_v)
        post_weights = (w_o.reshape(2, -1, share), w_gate, w_up, w_down)
        hidden_rows = hidden[:, 0, :]
        qkv, = comm(hidden_rows, norm_gains, in_weights, layer=-1, collective_id=0)
        heads, k_local, v_local = attend(qkv, tables, positions, k_local, v_local)
        residual, qkv = comm(heads, norm_gains, in_weights, (hidden_rows,) + post_weights, layer=0, collective_id=1)
        heads, k_global, v_global = attend(qkv, tables, positions, k_global, v_global)
        final = comm(heads, norm_gains, None, (residual,) + post_weights, layer=1, collective_id=2)[:, None, :]
        return final, k_local, v_local, k_global, v_global

    in_specs = (ROW_SPEC, POS_SPEC, CACHE_SPEC, CACHE_SPEC, CACHE_SPEC, CACHE_SPEC, PROJ_IN_SPEC, PROJ_IN_SPEC, PROJ_IN_SPEC, PROJ_OUT_SPEC, FF_IN_SPEC, FF_IN_SPEC, FF_OUT_SPEC, GAIN_SPEC)
    out_specs = (ROW_SPEC, CACHE_SPEC, CACHE_SPEC, CACHE_SPEC, CACHE_SPEC)
    return jax.shard_map(device_step, mesh=mesh, in_specs=in_specs, out_specs=out_specs, check_vma=False)
```

```python
import functools

import jax
import jax.numpy as jnp
from jax import lax
from jax.experimental import pallas as pl
from jax.experimental.pallas import tpu as pltpu
from jax.sharding import PartitionSpec as P

SOFT_CAP = 50.0
NORM_EPS = 1e-6
ROPE_BASE = 10000.0

ROW_SPEC = P(("part", "data"), None, None)
POS_SPEC = P(("part", "data"))
CACHE_SPEC = P(("part", "data"), None, "model", None)
PROJ_IN_SPEC = P(None, "data", "model", None)
PROJ_OUT_SPEC = P(None, "model", None, "data")
FF_IN_SPEC = P(None, "data", "model")
FF_OUT_SPEC = P(None, "model", "data")
GAIN_SPEC = P(None, None, None)


def rope_tables(positions, head_dim):
    inv_freq = ROPE_BASE ** (-jnp.arange(0, head_dim, 2).astype(jnp.float32) / head_dim)
    angles = positions.astype(jnp.float32)[:, None] * inv_freq[None, :]
    return jnp.cos(angles), jnp.sin(angles)


LANES = 128


def attend_kernel(cache_len, n_rows, group, depth, pos_ref, qkv_ref, cos_ref, sin_ref, k_hbm, v_hbm, head_ref, ko_hbm, vo_hbm, kbuf, vbuf, q8, kn, vn, outs, sbuf, pbuf, rd_sem, wr_sem):
    n_steps = n_rows // group
    n_cols = cache_len * 4

    def reads(step):
        slot = lax.rem(step, depth)
        rows = pl.ds(step * group, group)
        return (pltpu.make_async_copy(k_hbm.at[rows], kbuf.at[slot], rd_sem.at[0, slot]),
                pltpu.make_async_copy(v_hbm.at[rows], vbuf.at[slot], rd_sem.at[1, slot]))

    def writes(step):
        slot = lax.rem(step, depth)
        rows = pl.ds(step * group, group)
        return (pltpu.make_async_copy(kbuf.at[slot], ko_hbm.at[rows], wr_sem.at[0, slot]),
                pltpu.make_async_copy(vbuf.at[slot], vo_hbm.at[rows], wr_sem.at[1, slot]))

    ahead = depth // 2 if depth < n_steps else n_steps
    for step in range(ahead):
        for copy in reads(step):
            copy.start()

    cos_t, sin_t = cos_ref[...], sin_ref[...]
    scale = (2 * LANES) ** -0.5
    for h in range(4):
        first, second = qkv_ref[:, h * 256:h * 256 + LANES], qkv_ref[:, h * 256 + LANES:h * 256 + 256]
        q8[:, h, :] = (first * cos_t - second * sin_t) * scale
        q8[:, 4 + h, :] = (second * cos_t + first * sin_t) * scale
    for h in range(2):
        base = 1024 + h * 256
        first, second = qkv_ref[:, base:base + LANES], qkv_ref[:, base + LANES:base + 256]
        halves = (first * cos_t - second * sin_t, second * cos_t + first * sin_t)
        for half in range(2):
            value = qkv_ref[:, base + 512 + half * LANES:base + 512 + (half + 1) * LANES]
            for i in range(4):
                kn[:, i * 4 + half * 2 + h, :] = halves[half]
                vn[:, i * 4 + half * 2 + h, :] = value

    row_id = lax.broadcasted_iota(jnp.int32, (8, n_cols), 0)
    col_id = lax.broadcasted_iota(jnp.int32, (8, n_cols), 1)
    half_col = (col_id // 2) % 2
    same_half = row_id // 4 == half_col
    same_kv = (row_id // 2) % 2 == col_id % 2
    slot_col = col_id // 4
    sub_id = lax.broadcasted_iota(jnp.int32, (16, LANES), 0) // 4

    @pl.loop(0, n_steps)
    def _(step):
        slot = lax.rem(step, depth)
        if ahead < n_steps:
            @pl.when(step + ahead < n_steps)
            def _():
                @pl.when(step >= depth - ahead)
                def _():
                    for copy in writes(step - (depth - ahead)):
                        copy.wait()
                for copy in reads(step + ahead):
                    copy.start()

        for copy in reads(step):
            copy.wait()
        for i in range(group):
            row = step * group + i
            now = lax.rem(pos_ref[row], cache_len)
            window = pl.ds(pl.multiple_of(now // 4 * 16, 16), 16)
            hit = sub_id == lax.rem(now, 4)
            kbuf[slot, i, window, :] = jnp.where(hit, kn[row].astype(jnp.bfloat16), kbuf[slot, i, window, :])
            vbuf[slot, i, window, :] = jnp.where(hit, vn[row].astype(jnp.bfloat16), vbuf[slot, i, window, :])
        for i in range(group):
            part = lax.dot_general(q8[step * group + i].astype(jnp.bfloat16), kbuf[slot, i], (((1,), (1,)), ((), ())), preferred_element_type=jnp.float32)
            sbuf[i] = jnp.where(same_half & same_kv, part, 0.0)
        for i in range(group):
            part = sbuf[i]
            part = part + pltpu.roll(part, 4, 0)
            other = jnp.where(half_col == 0, pltpu.roll(part, n_cols - 2, 1), pltpu.roll(part, 2, 1))
            scores = SOFT_CAP * jnp.tanh((part + other) / SOFT_CAP)
            scores = jnp.where(same_kv & (slot_col <= pos_ref[step * group + i]), scores, -1e30)
            weights = jnp.exp(scores - jnp.max(scores, axis=1, keepdims=True))
            total = jnp.sum(jnp.where(same_half, weights, 0.0), axis=1, keepdims=True)
            pbuf[i] = jnp.where(same_half, weights / total, 0.0).astype(jnp.bfloat16)
        for i in range(group):
            outs[step * group + i] = jnp.dot(pbuf[i], vbuf[slot, i], preferred_element_type=jnp.float32)
        for copy in writes(step):
            copy.start()

    for h in range(4):
        for half in range(2):
            head_ref[:, h * 256 + half * LANES:h * 256 + (half + 1) * LANES] = outs[:, half * 4 + h, :].astype(jnp.bfloat16)
    for step in range(max(n_steps - depth, 0) if ahead < n_steps else 0, n_steps):
        for copy in writes(step):
            copy.wait()


def attend(qkv, tables, positions, k_cache, v_cache):
    n_rows, cache_len, kv_loc, head_dim = k_cache.shape
    halves = head_dim // LANES
    group = 16 if cache_len <= 64 else 4
    depth = 4 if cache_len <= 64 else 6
    f32, bf16 = jnp.float32, jnp.bfloat16

    def flat(cache):
        return cache.reshape(n_rows, cache_len, kv_loc, halves, LANES).transpose(0, 1, 3, 2, 4).reshape(n_rows, cache_len * halves * kv_loc, LANES)

    def unflat(cache):
        return cache.reshape(n_rows, cache_len, halves, kv_loc, LANES).transpose(0, 1, 3, 2, 4).reshape(n_rows, cache_len, kv_loc, head_dim)

    vmem, hbm = pl.BlockSpec(memory_space=pltpu.VMEM), pl.BlockSpec(memory_space=pltpu.HBM)
    k_flat, v_flat = flat(k_cache), flat(v_cache)
    n_cols = k_flat.shape[1]
    block = (depth, group, n_cols, LANES)
    dma = pltpu.SemaphoreType.DMA
    heads, k_out, v_out = pl.pallas_call(
        functools.partial(attend_kernel, cache_len, n_rows, group, depth),
        out_shape=(jax.ShapeDtypeStruct((n_rows, 4 * head_dim), bf16), jax.ShapeDtypeStruct(k_flat.shape, bf16), jax.ShapeDtypeStruct(v_flat.shape, bf16)),
        in_specs=[pl.BlockSpec(memory_space=pltpu.SMEM), vmem, vmem, vmem, hbm, hbm],
        out_specs=(vmem, hbm, hbm),
        scratch_shapes=[pltpu.VMEM(block, bf16), pltpu.VMEM(block, bf16), pltpu.VMEM((n_rows, 8, LANES), f32), pltpu.VMEM((n_rows, 16, LANES), f32),
                        pltpu.VMEM((n_rows, 16, LANES), f32), pltpu.VMEM((n_rows, 8, LANES), f32), pltpu.VMEM((group, 8, n_cols), f32), pltpu.VMEM((group, 8, n_cols), bf16),
                        dma((2, depth)), dma((2, depth))],
        compiler_params=pltpu.CompilerParams(vmem_limit_bytes=int((62 if cache_len <= 64 else 34) * 2**20)),
        cost_estimate=pl.CostEstimate(flops=n_rows * 8 * n_cols * LANES * 4, bytes_accessed=4 * k_flat.size * 2, transcendentals=0),
        name=f"attend_{cache_len}",
    )(positions, qkv, *tables, k_flat, v_flat)
    return heads, unflat(k_out), unflat(v_out)


FF_CHUNK = 512
IN_FLIGHT = 2
QKV_CHUNK = 1024
MESH = pl.DeviceIdType.MESH


GROUPS = 4


def comm_kernel(cfg, *refs):
    it = iter(refs)
    post, layer, rows, share, width = cfg["post"], cfg["layer"], cfg["rows"], cfg["share"], cfg["width"]
    qkv, n_ff, n_q = cfg["qkv"], cfg["n_ff"], cfg["n_q"]
    raw = cfg["raw"]
    x_any, g_hbm = next(it), next(it)
    if post:
        res_any, wo_any, wg_hbm, wu_hbm, wd_hbm = (next(it) for _ in range(5))
    if qkv:
        wq_hbm, wk_hbm, wv_hbm = (next(it) for _ in range(3))
        if post:
            hid_ref = next(it)
        qkv_ref = next(it)
    else:
        out_ref = next(it)
    if not post:
        x_ref = next(it)
    g_ref, tcol, st_src, st_rcv, hp, st_ss, st_rs, misc_ss, misc_rs, ld_sem = (next(it) for _ in range(10))
    if not post:
        out_rows = next(it)
    if post:
        if raw:
            raw_ref, res_ref, wo = (next(it) for _ in range(3))
        hall, apart, arecv, mpart, mrecv, wg, wu, wd, sib_out, sib_in, mine, x_in, u_all = (next(it) for _ in range(13))
        y_ss, y_rs, ff_ss, ff_rs = (next(it) for _ in range(4))
    if qkv:
        wi, wq, wk, wv, q_out, q_in, q_mine, q_x, q_ss, q_rs = (next(it) for _ in range(10))

    model, me = lax.axis_index("model"), lax.axis_index("data")
    x_pos, core = me // 2, lax.rem(me, 2)
    sib, part, diag = x_pos * 2 + 1 - core, (1 - x_pos) * 2 + core, (1 - x_pos) * 2 + 1 - core
    n_group = 4 * rows
    DIAG, SIB, PART, OWN = (pl.ds(i * rows, rows) for i in range(4))
    blocks = (OWN, SIB, PART, DIAG)
    mine_rows = [pl.ds(h * rows, rows) for h in range(GROUPS)]
    sends = []

    def remote(src, dst, send_sem, recv_sem, data=None):
        where = {"data": data} if data is not None else {"model": 1 - model}
        return pltpu.make_async_remote_copy(src_ref=src, dst_ref=dst, send_sem=send_sem, recv_sem=recv_sem, device_id=where, device_id_type=MESH)

    def send(*args):
        copy = remote(*args)
        copy.start()
        sends.append(copy)
        return copy

    def load(src, dst, sem):
        copy = pltpu.make_async_copy(src, dst, sem)
        copy.start()
        return copy

    early = [load(g_hbm, g_ref, ld_sem.at[8])]
    if post:
        x_ref = x_any
    else:
        early.append(load(x_any, x_ref, ld_sem.at[7]))
    if post:
        if raw:
            early.append(load(res_any, raw_ref, ld_sem.at[9]))
        else:
            res_ref = res_any
        if raw:
            wo_load = load(wo_any.at[layer], wo, ld_sem.at[0])
        else:
            wo = wo_any.at[layer]
        wg_load = load(wg_hbm.at[layer], wg, ld_sem.at[1])
        wu_load = load(wu_hbm.at[layer], wu, ld_sem.at[2])
        wd_load = load(wd_hbm.at[layer], wd, ld_sem.at[3])
    if qkv:
        in_loads = [load(src.at[layer + 1], dst, ld_sem.at[4 + k]) for k, (src, dst) in enumerate(((wq_hbm, wq), (wk_hbm, wk), (wv_hbm, wv)))]

    def relay_weights(c):
        col = c * QKV_CHUNK
        for k in ((0,), (1, 2))[c]:
            in_loads[k].wait()
            weight = (wq, wk, wv)[k]
            n_heads, head_dim = weight.shape[1:]
            for h in range(n_heads):
                wi[:, col:col + head_dim] = weight[:, h, :]
                col += head_dim

    barrier = pltpu.get_barrier_semaphore()
    for dev in (sib, part, diag):
        pl.semaphore_signal(barrier, inc=1, device_id={"data": dev}, device_id_type=MESH)
    pl.semaphore_signal(barrier, inc=1, device_id={"model": 1 - model}, device_id_type=MESH)
    tcol[...] = jnp.zeros_like(tcol)
    for copy in early:
        copy.wait()
    pl.semaphore_wait(barrier, 4)

    def square_sums(h, block, value):
        total = None
        for k in range(share // LANES):
            piece = value[:, k * LANES:(k + 1) * LANES]
            total = piece * piece if total is None else total + piece * piece
        tcol[h, block, :] = total

    lane_block = lax.broadcasted_iota(jnp.int32, (8, LANES), 1) // rows

    def start_scales(h, which):
        idx = which * GROUPS + h
        st_src[idx] = jnp.sum(jnp.transpose(tcol[h]).reshape(LANES // 8, 8, LANES), axis=0)
        return [send(st_src.at[idx], st_rcv.at[idx, k], st_ss.at[idx, k], st_rs.at[idx, k], dev) for k, dev in enumerate((sib, part, diag))]

    def end_scales(h, which, copies):
        idx = which * GROUPS + h
        for copy in copies:
            copy.wait_recv()

        def exchange(value, n):
            even = lax.rem(lane_block // n, 2) == 0
            return jnp.where(even, pltpu.roll(value, LANES - n * rows, 1), pltpu.roll(value, n * rows, 1))

        total = st_src[idx] + exchange(st_rcv[idx, 0], 2) + exchange(st_rcv[idx, 1], 1) + exchange(exchange(st_rcv[idx, 2], 1), 2)
        total = jnp.sum(total, axis=0, keepdims=True)
        inverse = lax.rsqrt(total / width + NORM_EPS)
        tcol[h] = jnp.transpose(jnp.broadcast_to(inverse, (LANES, LANES)))

    def gain_row(k):
        at, which = (layer + 1, 0) if k == 3 else (layer, k + 1)
        return 1.0 + g_ref[at, which:which + 1, pl.ds(pl.multiple_of(me * share, LANES), share)].astype(jnp.float32)

    def scaled(h, block, value, gain):
        return value * jnp.concatenate([tcol[h, block, :]] * (share // LANES), axis=1) * gain_row(gain)

    def q_partner(s):
        return remote(q_mine.at[s, pl.ds(0, rows)], q_x.at[s], q_ss.at[1, s], q_rs.at[1, s], part)

    def start_qkv(h):
        before = None
        for c in range(n_q):
            s = h * n_q + c
            sums = jnp.dot(hp[h], wi[:, c * QKV_CHUNK:(c + 1) * QKV_CHUNK], preferred_element_type=jnp.float32)
            q_out[s] = sums[:2 * rows]
            q_mine[s] = sums[2 * rows:]
            copy = send(q_out.at[s], q_in.at[s], q_ss.at[0, s], q_rs.at[0, s], sib)
            if c >= 1:
                before.wait_recv()
                q_mine[s - 1] = q_mine[s - 1] + q_in[s - 1]
                q_partner(s - 1).start()
            before = copy
        before.wait_recv()
        s = h * n_q + n_q - 1
        q_mine[s] = q_mine[s] + q_in[s]
        q_partner(s).start()

    def end_qkv():
        for h in range(GROUPS):
            for c in range(n_q):
                s = h * n_q + c
                q_partner(s).wait_recv()
                qkv_ref[mine_rows[h], c * QKV_CHUNK:(c + 1) * QKV_CHUNK] = q_mine[s, pl.ds(rows, rows), :] + q_x[s]
        for s in range(GROUPS * n_q):
            q_partner(s).wait_send()

    def spread(src, dst, base):
        copies = []
        for h in range(GROUPS):
            for k, (dev, there) in enumerate(((sib, SIB), (part, PART), (diag, DIAG))):
                cols = pl.ds(pl.multiple_of(dev * share, LANES), share)
                i = base + h * 3 + k
                copies.append(send(src.at[mine_rows[h], cols], dst.at[h, there, :], misc_ss.at[i], misc_rs.at[i], dev))
        return copies

    my_cols = pl.ds(pl.multiple_of(me * share, LANES), share)
    if not post:
        xn = out_rows
        for h in range(GROUPS):
            value = x_ref[mine_rows[h], :].astype(jnp.float32)
            inverse = lax.rsqrt(jnp.mean(value * value, axis=1, keepdims=True) + NORM_EPS)
            xn[mine_rows[h], :] = (value * inverse * (1.0 + g_ref[0, 0:1, :].astype(jnp.float32))).astype(jnp.bfloat16)
        copies = spread(xn, hp, 0)
        relay_weights(0)
        relay_weights(1)
        for h in range(GROUPS):
            hp[h, OWN, :] = xn[mine_rows[h], my_cols]
            for copy in copies[h * 3:h * 3 + 3]:
                copy.wait_recv()
            start_qkv(h)
        end_qkv()
    else:
        head_cuts = (pl.ds(0, rows), pl.ds(rows, (GROUPS - 1) * rows))
        to_part = [send(x_ref.at[cut], hall.at[2, cut], misc_ss.at[n], misc_rs.at[n], part) for n, cut in enumerate(head_cuts)]
        to_sib = send(x_ref, hall.at[1], misc_ss.at[2], misc_rs.at[2], sib)
        if raw:
            raw_copies = spread(raw_ref, res_ref, 5)
            for h in range(GROUPS):
                res_ref[h, OWN, :] = raw_ref[mine_rows[h], my_cols]
        if raw:
            wo_load.wait()
        y_copies = [[None] * 4 for _ in range(GROUPS)]

        def project(heads, places):
            sums = jnp.dot(heads, wo[...], preferred_element_type=jnp.float32)
            for n, (h, k) in enumerate(places):
                apart[h, blocks[k], :] = sums[n * rows:(n + 1) * rows]

        def to_model(*pairs):
            for h, k in pairs:
                y_copies[h][k] = send(apart.at[h, blocks[k], :], arecv.at[h, blocks[k], :], y_ss.at[h * 4 + k], y_rs.at[h * 4 + k])

        def forward(n):
            to_part[n].wait_recv()
            return send(hall.at[2, head_cuts[n]], hall.at[0, head_cuts[n]], misc_ss.at[3 + n], misc_rs.at[3 + n], sib)

        project(x_ref[...], [(h, 0) for h in range(GROUPS)])
        to_model((0, 0), (1, 0))
        to_sib.wait_recv()
        project(hall[1], [(h, 1) for h in range(GROUPS)])
        to_model((0, 1), (1, 1))
        forward(0).wait_recv()
        project(jnp.concatenate([hall[2, head_cuts[0], :], hall[0, head_cuts[0], :]], axis=0), [(0, 2), (0, 3)])
        to_model((0, 2), (0, 3), (2, 0), (2, 1))
        rest = forward(1)
        project(hall[2, head_cuts[1], :], [(h, 2) for h in range(1, GROUPS)])
        to_model((1, 2))
        rest.wait_recv()
        project(hall[0, head_cuts[1], :], [(h, 3) for h in range(1, GROUPS)])
        to_model((1, 3), (2, 2), (2, 3), (3, 0), (3, 1), (3, 2), (3, 3))
        stats = {}

        def attn_sums(h):
            for k, block in enumerate(blocks):
                y_copies[h][k].wait_recv()
                total = apart[h, block, :] + arecv[h, block, :]
                arecv[h, block, :] = total
                square_sums(h, block, total)
            stats[h] = start_scales(h, 0)

        def attn_residual(h):
            end_scales(h, 0, stats[h])
            if raw:
                for copy in raw_copies[h * 3:h * 3 + 3]:
                    copy.wait_recv()
            for block in blocks:
                residual = res_ref[h, block, :].astype(jnp.float32)
                mid = (residual + scaled(h, block, arecv[h, block, :], 0)).astype(jnp.bfloat16).astype(jnp.float32)
                arecv[h, block, :] = mid
            for block in blocks:
                square_sums(h, block, arecv[h, block, :])
            stats[h] = start_scales(h, 1)

        def attn_normed(h):
            mpart[h] = jnp.zeros((n_group, share), jnp.float32)
            end_scales(h, 1, stats[h])
            for block in blocks:
                hp[h, block, :] = scaled(h, block, arecv[h, block, :], 1).astype(jnp.bfloat16)

        def to_sibling(s):
            return remote(sib_out.at[s], sib_in.at[s], ff_ss.at[0, s], ff_rs.at[0, s], sib)

        def to_partner(s):
            return remote(mine.at[s, pl.ds(0, rows)], x_in.at[s], ff_ss.at[1, s], ff_rs.at[1, s], part)

        def act_partner(s):
            return remote(u_all.at[s, OWN], u_all.at[s, PART], ff_ss.at[2, s], ff_rs.at[2, s], part)

        def act_sibling(s):
            return remote(u_all.at[s, OWN], u_all.at[s, SIB], ff_ss.at[3, s], ff_rs.at[3, s], sib)

        def act_forward(s):
            return remote(u_all.at[s, PART], u_all.at[s, DIAG], ff_ss.at[4, s], ff_rs.at[4, s], sib)

        def add_sibling(s):
            to_sibling(s).wait_recv()
            mine[s] = mine[s] + sib_in[s]

            @pl.when(s >= IN_FLIGHT)
            def _():
                to_partner(s - IN_FLIGHT).wait_send()
            to_partner(s).start()

        def gate_up(h, start, end):
            @pl.loop(start, end)
            def _(c):
                s = h * n_ff + c
                cols = pl.ds(pl.multiple_of(c * FF_CHUNK, FF_CHUNK), FF_CHUNK)
                for k, weight in enumerate((wg, wu)):
                    sums = jnp.dot(hp[h], weight[:, cols], preferred_element_type=jnp.float32)
                    sib_out[s, :, pl.ds(k * FF_CHUNK, FF_CHUNK)] = sums[:2 * rows]
                    mine[s, :, pl.ds(k * FF_CHUNK, FF_CHUNK)] = sums[2 * rows:]
                to_sibling(s).start()

                @pl.when(s >= 1)
                def _():
                    add_sibling(s - 1)

        attn_sums(0)
        if qkv:
            relay_weights(0)
        attn_residual(0)
        if qkv:
            relay_weights(1)
        attn_sums(1)
        attn_normed(0)
        wg_load.wait()
        wu_load.wait()
        cuts = (n_ff * 3 // 10, n_ff * 7 // 10)
        for h in range(GROUPS):
            if h + 1 < GROUPS:
                gate_up(h, 0, cuts[0])
                attn_residual(h + 1)
                gate_up(h, cuts[0], cuts[1])
                attn_normed(h + 1)
                if h + 2 < GROUPS:
                    attn_sums(h + 2)
                gate_up(h, cuts[1], n_ff)
            else:
                gate_up(h, 0, n_ff)
        add_sibling(GROUPS * n_ff - 1)
        @pl.loop(0, GROUPS * n_ff)
        def _(s):
            to_partner(s).wait_recv()
            both = mine[s, pl.ds(rows, rows), :] + x_in[s]
            u_all[s, OWN, :] = (jax.nn.gelu(both[:, :FF_CHUNK], approximate=True) * both[:, FF_CHUNK:]).astype(jnp.bfloat16)
            act_partner(s).start()
            act_sibling(s).start()

        wd_load.wait()

        def down(h, c):
            s = h * n_ff + c
            act_sibling(s).wait_recv()
            act_forward(s).wait_recv()
            deep = pl.ds(pl.multiple_of(c * FF_CHUNK, FF_CHUNK), FF_CHUNK)
            mpart[h] += jnp.dot(u_all[s], wd[deep, :], preferred_element_type=jnp.float32)

        m_copies = []
        for h in range(GROUPS):
            @pl.loop(0, n_ff)
            def _(c):
                act_partner(h * n_ff + c).wait_recv()
                act_forward(h * n_ff + c).start()

                @pl.when(c >= 1)
                def _():
                    down(h, c - 1)

            down(h, n_ff - 1)
            m_copies.append(send(mpart.at[h], mrecv.at[h], y_ss.at[4 * GROUPS + h], y_rs.at[4 * GROUPS + h]))

        out_copies = []

        def ff_sums(h):
            m_copies[h].wait_recv()
            for block in blocks:
                total = mpart[h, block, :] + mrecv[h, block, :]
                mrecv[h, block, :] = total
                square_sums(h, block, total)
            stats[h] = start_scales(h, 2)

        def ff_residual(h):
            end_scales(h, 2, stats[h])
            for block in blocks:
                value = (arecv[h, block, :] + scaled(h, block, mrecv[h, block, :], 2)).astype(jnp.bfloat16)
                if qkv:
                    hid_ref[h, block, :] = value
                else:
                    hp[h, block, :] = value
            if qkv:
                for block in blocks:
                    square_sums(h, block, hid_ref[h, block, :].astype(jnp.float32))
                stats[h] = start_scales(h, 3)
            else:
                for k, (dev, block) in enumerate(((sib, SIB), (part, PART), (diag, DIAG))):
                    i = 5 + h * 3 + k
                    out_copies.append(send(hp.at[h, block, :], out_ref.at[mine_rows[h], my_cols], misc_ss.at[i], misc_rs.at[i], dev))
                out_ref[mine_rows[h], my_cols] = hp[h, OWN, :]

        def ff_normed(h):
            end_scales(h, 3, stats[h])
            for block in blocks:
                hp[h, block, :] = scaled(h, block, hid_ref[h, block, :].astype(jnp.float32), 3).astype(jnp.bfloat16)
            start_qkv(h)

        ff_sums(0)
        ff_sums(1)
        ff_residual(0)
        ff_sums(2)
        ff_residual(1)
        if qkv:
            ff_normed(0)
        ff_sums(3)
        ff_residual(2)
        if qkv:
            ff_normed(1)
        ff_residual(3)
        if qkv:
            ff_normed(2)
            ff_normed(3)
        if qkv:
            end_qkv()
        for copy in out_copies:
            copy.wait_recv()

        @pl.loop(0, GROUPS * n_ff)
        def _(s):
            for copy in (to_sibling(s), act_partner(s), act_sibling(s), act_forward(s)):
                copy.wait_send()
        for s in range(GROUPS * n_ff - IN_FLIGHT, GROUPS * n_ff):
            to_partner(s).wait_send()
    for copy in sends:
        copy.wait_send()


def comm(x, gains, in_weights=None, post=None, layer=0, collective_id=0):
    rows = x.shape[0] // GROUPS
    share = gains.shape[2] // 4
    n_group = rows * 4
    f32, bf16, vmem, hbm = jnp.float32, jnp.bfloat16, pl.BlockSpec(memory_space=pltpu.VMEM), pl.BlockSpec(memory_space=pltpu.HBM)
    dma = pltpu.SemaphoreType.DMA
    args, specs = [x, gains], [hbm if post is None else vmem, hbm]
    raw = post is not None and post[0].ndim == 2
    n_stat = 4 * GROUPS
    n_misc = 5 + 3 * GROUPS
    scratch = [pltpu.VMEM(x.shape, bf16)] if post is None else []
    scratch += [pltpu.VMEM(gains.shape, bf16), pltpu.VMEM((GROUPS, LANES, LANES), f32), pltpu.VMEM((n_stat, 8, LANES), f32), pltpu.VMEM((n_stat, 3, 8, LANES), f32), pltpu.VMEM((GROUPS, n_group, share), bf16),
               dma((n_stat, 3)), dma((n_stat, 3)), dma((n_misc,)), dma((n_misc,)), dma((10,))]
    if post is None:
        scratch.append(pltpu.VMEM(x.shape, bf16))
    n_ff = n_q = 0
    if post is not None:
        residual, w_o, w_gate, w_up, w_down = post
        args += list(post)
        specs += [hbm if raw else vmem] * 2 + [hbm] * 3
        ff = w_gate.shape[2]
        n_ff = ff // FF_CHUNK
        steps = GROUPS * n_ff
        scratch += [pltpu.VMEM(residual.shape, bf16), pltpu.VMEM((GROUPS, n_group, share), bf16), pltpu.VMEM(w_o.shape[1:], bf16)] if raw else []
        scratch += [pltpu.VMEM((3, GROUPS * rows, w_o.shape[1]), bf16)] + [pltpu.VMEM((GROUPS, n_group, share), f32)] * 4
        scratch += [pltpu.VMEM((share, ff), bf16), pltpu.VMEM((share, ff), bf16), pltpu.VMEM((ff, share), bf16)]
        scratch += [pltpu.VMEM((steps, 2 * rows, 2 * FF_CHUNK), f32)] * 3 + [pltpu.VMEM((steps, rows, 2 * FF_CHUNK), f32), pltpu.VMEM((steps, n_group, FF_CHUNK), bf16)]
        scratch += [dma((5 * GROUPS,)), dma((5 * GROUPS,)), dma((5, steps)), dma((5, steps))]
    if in_weights is not None:
        args += list(in_weights)
        specs += [hbm] * 3
        n_in = sum(w.shape[2] * w.shape[3] for w in in_weights)
        n_q = n_in // QKV_CHUNK
        scratch += [pltpu.VMEM((share, n_in), bf16)] + [pltpu.VMEM(w.shape[1:], bf16) for w in in_weights]
        scratch += [pltpu.VMEM((GROUPS * n_q, 2 * rows, QKV_CHUNK), f32)] * 3 + [pltpu.VMEM((GROUPS * n_q, rows, QKV_CHUNK), f32), dma((2, GROUPS * n_q)), dma((2, GROUPS * n_q))]
        out_shape = [jax.ShapeDtypeStruct((GROUPS, n_group, share), bf16), jax.ShapeDtypeStruct((GROUPS * rows, n_in), f32)][post is None:]
        out_specs = [vmem, vmem][post is None:]
    else:
        out_shape = jax.ShapeDtypeStruct((GROUPS * rows, 4 * share), bf16)
        out_specs = vmem
    cfg = {"raw": raw, "post": post is not None, "qkv": in_weights is not None, "layer": layer, "rows": rows, "share": share, "width": 4 * share, "n_ff": n_ff, "n_q": n_q}
    return pl.pallas_call(
        functools.partial(comm_kernel, cfg),
        out_shape=out_shape, in_specs=specs, out_specs=out_specs, scratch_shapes=scratch,
        compiler_params=pltpu.CompilerParams(collective_id=collective_id, has_side_effects=True, vmem_limit_bytes=int((62, 62, 49)[collective_id] * 2**20)),
        name=f"comm_{collective_id}",
    )(*args)


def solution(mesh):
    def device_step(hidden, positions, k_local, v_local, k_global, v_global, w_q, w_k, w_v, w_o, w_gate, w_up, w_down, norm_gains):
        share = w_q.shape[1]
        tables = rope_tables(positions, w_q.shape[3])
        in_weights = (w_q, w_k, w_v)
        post_weights = (w_o.reshape(2, -1, share), w_gate, w_up, w_down)
        hidden_rows = hidden[:, 0, :]
        qkv, = comm(hidden_rows, norm_gains, in_weights, layer=-1, collective_id=0)
        heads, k_local, v_local = attend(qkv, tables, positions, k_local, v_local)
        residual, qkv = comm(heads, norm_gains, in_weights, (hidden_rows,) + post_weights, layer=0, collective_id=1)
        heads, k_global, v_global = attend(qkv, tables, positions, k_global, v_global)
        final = comm(heads, norm_gains, None, (residual,) + post_weights, layer=1, collective_id=2)[:, None, :]
        return final, k_local, v_local, k_global, v_global

    in_specs = (ROW_SPEC, POS_SPEC, CACHE_SPEC, CACHE_SPEC, CACHE_SPEC, CACHE_SPEC, PROJ_IN_SPEC, PROJ_IN_SPEC, PROJ_IN_SPEC, PROJ_OUT_SPEC, FF_IN_SPEC, FF_IN_SPEC, FF_OUT_SPEC, GAIN_SPEC)
    out_specs = (ROW_SPEC, CACHE_SPEC, CACHE_SPEC, CACHE_SPEC, CACHE_SPEC)
    return jax.shard_map(device_step, mesh=mesh, in_specs=in_specs, out_specs=out_specs, check_vma=False)
```

```python
import functools

import jax
import jax.numpy as jnp
from jax import lax
from jax.experimental import pallas as pl
from jax.experimental.pallas import tpu as pltpu
from jax.sharding import PartitionSpec as P

SOFT_CAP = 50.0
NORM_EPS = 1e-6
ROPE_BASE = 10000.0

ROW_SPEC = P(("part", "data"), None, None)
POS_SPEC = P(("part", "data"))
CACHE_SPEC = P(("part", "data"), None, "model", None)
PROJ_IN_SPEC = P(None, "data", "model", None)
PROJ_OUT_SPEC = P(None, "model", None, "data")
FF_IN_SPEC = P(None, "data", "model")
FF_OUT_SPEC = P(None, "model", "data")
GAIN_SPEC = P(None, None, None)


def rope_tables(positions, head_dim):
    inv_freq = ROPE_BASE ** (-jnp.arange(0, head_dim, 2).astype(jnp.float32) / head_dim)
    angles = positions.astype(jnp.float32)[:, None] * inv_freq[None, :]
    return jnp.cos(angles), jnp.sin(angles)


LANES = 128


def attend_kernel(cache_len, n_rows, group, depth, pos_ref, qkv_ref, cos_ref, sin_ref, k_hbm, v_hbm, head_ref, ko_hbm, vo_hbm, kbuf, vbuf, q8, kn, vn, outs, sbuf, pbuf, rd_sem, wr_sem):
    n_steps = n_rows // group
    n_cols = cache_len * 4

    def reads(step):
        slot = lax.rem(step, depth)
        rows = pl.ds(step * group, group)
        return (pltpu.make_async_copy(k_hbm.at[rows], kbuf.at[slot], rd_sem.at[0, slot]),
                pltpu.make_async_copy(v_hbm.at[rows], vbuf.at[slot], rd_sem.at[1, slot]))

    def writes(step):
        slot = lax.rem(step, depth)
        rows = pl.ds(step * group, group)
        return (pltpu.make_async_copy(kbuf.at[slot], ko_hbm.at[rows], wr_sem.at[0, slot]),
                pltpu.make_async_copy(vbuf.at[slot], vo_hbm.at[rows], wr_sem.at[1, slot]))

    ahead = depth // 2 if depth < n_steps else n_steps
    for step in range(ahead):
        for copy in reads(step):
            copy.start()

    cos_t, sin_t = cos_ref[...], sin_ref[...]
    scale = (2 * LANES) ** -0.5
    for h in range(4):
        first, second = qkv_ref[:, h * 256:h * 256 + LANES], qkv_ref[:, h * 256 + LANES:h * 256 + 256]
        q8[:, h, :] = (first * cos_t - second * sin_t) * scale
        q8[:, 4 + h, :] = (second * cos_t + first * sin_t) * scale
    for h in range(2):
        base = 1024 + h * 256
        first, second = qkv_ref[:, base:base + LANES], qkv_ref[:, base + LANES:base + 256]
        halves = (first * cos_t - second * sin_t, second * cos_t + first * sin_t)
        for half in range(2):
            value = qkv_ref[:, base + 512 + half * LANES:base + 512 + (half + 1) * LANES]
            for i in range(4):
                kn[:, i * 4 + half * 2 + h, :] = halves[half]
                vn[:, i * 4 + half * 2 + h, :] = value

    row_id = lax.broadcasted_iota(jnp.int32, (8, n_cols), 0)
    col_id = lax.broadcasted_iota(jnp.int32, (8, n_cols), 1)
    half_col = (col_id // 2) % 2
    same_half = row_id // 4 == half_col
    same_kv = (row_id // 2) % 2 == col_id % 2
    slot_col = col_id // 4
    sub_id = lax.broadcasted_iota(jnp.int32, (16, LANES), 0) // 4

    @pl.loop(0, n_steps)
    def _(step):
        slot = lax.rem(step, depth)
        if ahead < n_steps:
            @pl.when(step + ahead < n_steps)
            def _():
                @pl.when(step >= depth - ahead)
                def _():
                    for copy in writes(step - (depth - ahead)):
                        copy.wait()
                for copy in reads(step + ahead):
                    copy.start()

        for copy in reads(step):
            copy.wait()
        for i in range(group):
            row = step * group + i
            now = lax.rem(pos_ref[row], cache_len)
            window = pl.ds(pl.multiple_of(now // 4 * 16, 16), 16)
            hit = sub_id == lax.rem(now, 4)
            kbuf[slot, i, window, :] = jnp.where(hit, kn[row].astype(jnp.bfloat16), kbuf[slot, i, window, :])
            vbuf[slot, i, window, :] = jnp.where(hit, vn[row].astype(jnp.bfloat16), vbuf[slot, i, window, :])
        for i in range(group):
            part = lax.dot_general(q8[step * group + i].astype(jnp.bfloat16), kbuf[slot, i], (((1,), (1,)), ((), ())), preferred_element_type=jnp.float32)
            sbuf[i] = jnp.where(same_half & same_kv, part, 0.0)
        for i in range(group):
            part = sbuf[i]
            part = part + pltpu.roll(part, 4, 0)
            other = jnp.where(half_col == 0, pltpu.roll(part, n_cols - 2, 1), pltpu.roll(part, 2, 1))
            scores = SOFT_CAP * jnp.tanh((part + other) / SOFT_CAP)
            scores = jnp.where(same_kv & (slot_col <= pos_ref[step * group + i]), scores, -1e30)
            weights = jnp.exp(scores - jnp.max(scores, axis=1, keepdims=True))
            total = jnp.sum(jnp.where(same_half, weights, 0.0), axis=1, keepdims=True)
            pbuf[i] = jnp.where(same_half, weights / total, 0.0).astype(jnp.bfloat16)
        for i in range(group):
            outs[step * group + i] = jnp.dot(pbuf[i], vbuf[slot, i], preferred_element_type=jnp.float32)
        for copy in writes(step):
            copy.start()

    for h in range(4):
        for half in range(2):
            head_ref[:, h * 256 + half * LANES:h * 256 + (half + 1) * LANES] = outs[:, half * 4 + h, :].astype(jnp.bfloat16)
    for step in range(max(n_steps - depth, 0) if ahead < n_steps else 0, n_steps):
        for copy in writes(step):
            copy.wait()


def attend(qkv, tables, positions, k_cache, v_cache):
    n_rows, cache_len, kv_loc, head_dim = k_cache.shape
    halves = head_dim // LANES
    group = 8 if cache_len <= 64 else 4
    depth = 8 if cache_len <= 64 else 6
    f32, bf16 = jnp.float32, jnp.bfloat16

    def flat(cache):
        return cache.reshape(n_rows, cache_len, kv_loc, halves, LANES).transpose(0, 1, 3, 2, 4).reshape(n_rows, cache_len * halves * kv_loc, LANES)

    def unflat(cache):
        return cache.reshape(n_rows, cache_len, halves, kv_loc, LANES).transpose(0, 1, 3, 2, 4).reshape(n_rows, cache_len, kv_loc, head_dim)

    vmem, hbm = pl.BlockSpec(memory_space=pltpu.VMEM), pl.BlockSpec(memory_space=pltpu.HBM)
    k_flat, v_flat = flat(k_cache), flat(v_cache)
    n_cols = k_flat.shape[1]
    block = (depth, group, n_cols, LANES)
    dma = pltpu.SemaphoreType.DMA
    heads, k_out, v_out = pl.pallas_call(
        functools.partial(attend_kernel, cache_len, n_rows, group, depth),
        out_shape=(jax.ShapeDtypeStruct((n_rows, 4 * head_dim), bf16), jax.ShapeDtypeStruct(k_flat.shape, bf16), jax.ShapeDtypeStruct(v_flat.shape, bf16)),
        in_specs=[pl.BlockSpec(memory_space=pltpu.SMEM), vmem, vmem, vmem, hbm, hbm],
        out_specs=(vmem, hbm, hbm),
        scratch_shapes=[pltpu.VMEM(block, bf16), pltpu.VMEM(block, bf16), pltpu.VMEM((n_rows, 8, LANES), f32), pltpu.VMEM((n_rows, 16, LANES), f32),
                        pltpu.VMEM((n_rows, 16, LANES), f32), pltpu.VMEM((n_rows, 8, LANES), f32), pltpu.VMEM((group, 8, n_cols), f32), pltpu.VMEM((group, 8, n_cols), bf16),
                        dma((2, depth)), dma((2, depth))],
        compiler_params=pltpu.CompilerParams(vmem_limit_bytes=int((62 if cache_len <= 64 else 34) * 2**20)),
        cost_estimate=pl.CostEstimate(flops=n_rows * 8 * n_cols * LANES * 4, bytes_accessed=4 * k_flat.size * 2, transcendentals=0),
        name=f"attend_{cache_len}",
    )(positions, qkv, *tables, k_flat, v_flat)
    return heads, unflat(k_out), unflat(v_out)


FF_CHUNK = 512
IN_FLIGHT = 4
QKV_CHUNK = 1024
MESH = pl.DeviceIdType.MESH


GROUPS = 4


def comm_kernel(cfg, *refs):
    it = iter(refs)
    post, layer, rows, share, width = cfg["post"], cfg["layer"], cfg["rows"], cfg["share"], cfg["width"]
    qkv, n_ff, n_q = cfg["qkv"], cfg["n_ff"], cfg["n_q"]
    raw = cfg["raw"]
    x_any, g_hbm = next(it), next(it)
    if post:
        res_any, wo_any, wg_hbm, wu_hbm, wd_hbm = (next(it) for _ in range(5))
    if qkv:
        wq_hbm, wk_hbm, wv_hbm = (next(it) for _ in range(3))
        if post:
            hid_ref = next(it)
        qkv_ref = next(it)
    else:
        out_ref = next(it)
    if raw or not post:
        x_ref = next(it)
    g_ref, tcol, st_src, st_rcv, hp, st_ss, st_rs, misc_ss, misc_rs, ld_sem = (next(it) for _ in range(10))
    if not post:
        out_rows = next(it)
    if post:
        if raw:
            raw_ref, res_ref, wo = (next(it) for _ in range(3))
        hall, apart, arecv, mpart, mrecv, wg, wu, wd, sib_out, sib_in, mine, x_in, u_all = (next(it) for _ in range(13))
        y_ss, y_rs, ff_ss, ff_rs = (next(it) for _ in range(4))
    if qkv:
        wi, wq, wk, wv, q_out, q_in, q_mine, q_x, q_ss, q_rs = (next(it) for _ in range(10))

    model, me = lax.axis_index("model"), lax.axis_index("data")
    x_pos, core = me // 2, lax.rem(me, 2)
    sib, part, diag = x_pos * 2 + 1 - core, (1 - x_pos) * 2 + core, (1 - x_pos) * 2 + 1 - core
    n_group = 4 * rows
    DIAG, SIB, PART, OWN = (pl.ds(i * rows, rows) for i in range(4))
    blocks = (OWN, SIB, PART, DIAG)
    mine_rows = [pl.ds(h * rows, rows) for h in range(GROUPS)]
    sends = []

    def remote(src, dst, send_sem, recv_sem, data=None):
        where = {"data": data} if data is not None else {"model": 1 - model}
        return pltpu.make_async_remote_copy(src_ref=src, dst_ref=dst, send_sem=send_sem, recv_sem=recv_sem, device_id=where, device_id_type=MESH)

    def send(*args):
        copy = remote(*args)
        copy.start()
        sends.append(copy)
        return copy

    def load(src, dst, sem):
        copy = pltpu.make_async_copy(src, dst, sem)
        copy.start()
        return copy

    early = [load(g_hbm, g_ref, ld_sem.at[8])]
    if post and not raw:
        x_ref = x_any
    else:
        early.append(load(x_any, x_ref, ld_sem.at[7]))
    if post:
        if raw:
            early.append(load(res_any, raw_ref, ld_sem.at[9]))
        else:
            res_ref = res_any
        if raw:
            wo_load = load(wo_any.at[layer], wo, ld_sem.at[0])
        else:
            wo = wo_any.at[layer]
        wg_load = load(wg_hbm.at[layer], wg, ld_sem.at[1])
        wu_load = load(wu_hbm.at[layer], wu, ld_sem.at[2])
        wd_load = load(wd_hbm.at[layer], wd, ld_sem.at[3])
    if qkv:
        in_loads = [load(src.at[layer + 1], dst, ld_sem.at[4 + k]) for k, (src, dst) in enumerate(((wq_hbm, wq), (wk_hbm, wk), (wv_hbm, wv)))]

    def relay_weights(c):
        col = c * QKV_CHUNK
        for k in ((0,), (1, 2))[c]:
            in_loads[k].wait()
            weight = (wq, wk, wv)[k]
            n_heads, head_dim = weight.shape[1:]
            for h in range(n_heads):
                wi[:, col:col + head_dim] = weight[:, h, :]
                col += head_dim

    barrier = pltpu.get_barrier_semaphore()
    for dev in (sib, part, diag):
        pl.semaphore_signal(barrier, inc=1, device_id={"data": dev}, device_id_type=MESH)
    pl.semaphore_signal(barrier, inc=1, device_id={"model": 1 - model}, device_id_type=MESH)
    tcol[...] = jnp.zeros_like(tcol)
    for copy in early:
        copy.wait()
    pl.semaphore_wait(barrier, 4)

    def square_sums(h, block, value):
        total = None
        for k in range(share // LANES):
            piece = value[:, k * LANES:(k + 1) * LANES]
            total = piece * piece if total is None else total + piece * piece
        tcol[h, block, :] = total

    lane_block = lax.broadcasted_iota(jnp.int32, (8, LANES), 1) // rows

    def start_scales(h, which):
        idx = which * GROUPS + h
        st_src[idx] = jnp.sum(jnp.transpose(tcol[h]).reshape(LANES // 8, 8, LANES), axis=0)
        return [send(st_src.at[idx], st_rcv.at[idx, k], st_ss.at[idx, k], st_rs.at[idx, k], dev) for k, dev in enumerate((sib, part, diag))]

    def end_scales(h, which, copies):
        idx = which * GROUPS + h
        for copy in copies:
            copy.wait_recv()

        def exchange(value, n):
            even = lax.rem(lane_block // n, 2) == 0
            return jnp.where(even, pltpu.roll(value, LANES - n * rows, 1), pltpu.roll(value, n * rows, 1))

        total = st_src[idx] + exchange(st_rcv[idx, 0], 2) + exchange(st_rcv[idx, 1], 1) + exchange(exchange(st_rcv[idx, 2], 1), 2)
        total = jnp.sum(total, axis=0, keepdims=True)
        inverse = lax.rsqrt(total / width + NORM_EPS)
        tcol[h] = jnp.transpose(jnp.broadcast_to(inverse, (LANES, LANES)))

    def gain_row(k):
        at, which = (layer + 1, 0) if k == 3 else (layer, k + 1)
        return 1.0 + g_ref[at, which:which + 1, pl.ds(pl.multiple_of(me * share, LANES), share)].astype(jnp.float32)

    def scaled(h, block, value, gain):
        return value * jnp.concatenate([tcol[h, block, :]] * (share // LANES), axis=1) * gain_row(gain)

    def q_partner(s):
        return remote(q_mine.at[s, pl.ds(0, rows)], q_x.at[s], q_ss.at[1, s], q_rs.at[1, s], part)

    def start_qkv(h):
        before = None
        for c in range(n_q):
            s = h * n_q + c
            sums = jnp.dot(hp[h], wi[:, c * QKV_CHUNK:(c + 1) * QKV_CHUNK], preferred_element_type=jnp.float32)
            q_out[s] = sums[:2 * rows]
            q_mine[s] = sums[2 * rows:]
            copy = send(q_out.at[s], q_in.at[s], q_ss.at[0, s], q_rs.at[0, s], sib)
            if c >= 1:
                before.wait_recv()
                q_mine[s - 1] = q_mine[s - 1] + q_in[s - 1]
                q_partner(s - 1).start()
            before = copy
        before.wait_recv()
        s = h * n_q + n_q - 1
        q_mine[s] = q_mine[s] + q_in[s]
        q_partner(s).start()

    def end_qkv():
        for h in range(GROUPS):
            for c in range(n_q):
                s = h * n_q + c
                q_partner(s).wait_recv()
                qkv_ref[mine_rows[h], c * QKV_CHUNK:(c + 1) * QKV_CHUNK] = q_mine[s, pl.ds(rows, rows), :] + q_x[s]
        for s in range(GROUPS * n_q):
            q_partner(s).wait_send()

    def spread(src, dst, base):
        copies = []
        for h in range(GROUPS):
            for k, (dev, there) in enumerate(((sib, SIB), (part, PART), (diag, DIAG))):
                cols = pl.ds(pl.multiple_of(dev * share, LANES), share)
                i = base + h * 3 + k
                copies.append(send(src.at[mine_rows[h], cols], dst.at[h, there, :], misc_ss.at[i], misc_rs.at[i], dev))
        return copies

    my_cols = pl.ds(pl.multiple_of(me * share, LANES), share)
    if not post:
        xn = out_rows
        for h in range(GROUPS):
            value = x_ref[mine_rows[h], :].astype(jnp.float32)
            inverse = lax.rsqrt(jnp.mean(value * value, axis=1, keepdims=True) + NORM_EPS)
            xn[mine_rows[h], :] = (value * inverse * (1.0 + g_ref[0, 0:1, :].astype(jnp.float32))).astype(jnp.bfloat16)
        copies = spread(xn, hp, 0)
        relay_weights(0)
        relay_weights(1)
        for h in range(GROUPS):
            hp[h, OWN, :] = xn[mine_rows[h], my_cols]
            for copy in copies[h * 3:h * 3 + 3]:
                copy.wait_recv()
            start_qkv(h)
        end_qkv()
    else:
        head_cuts = (pl.ds(0, rows), pl.ds(rows, (GROUPS - 1) * rows))
        to_part = [send(x_ref.at[cut], hall.at[2, cut], misc_ss.at[n], misc_rs.at[n], part) for n, cut in enumerate(head_cuts)]
        to_sib = send(x_ref, hall.at[1], misc_ss.at[2], misc_rs.at[2], sib)
        if raw:
            raw_copies = spread(raw_ref, res_ref, 5)
            for h in range(GROUPS):
                res_ref[h, OWN, :] = raw_ref[mine_rows[h], my_cols]
        if raw:
            wo_load.wait()
        y_copies = [[None] * 4 for _ in range(GROUPS)]

        def project(heads, places):
            sums = jnp.dot(heads, wo[...], preferred_element_type=jnp.float32)
            for n, (h, k) in enumerate(places):
                apart[h, blocks[k], :] = sums[n * rows:(n + 1) * rows]

        def to_model(*pairs):
            for h, k in pairs:
                y_copies[h][k] = send(apart.at[h, blocks[k], :], arecv.at[h, blocks[k], :], y_ss.at[h * 4 + k], y_rs.at[h * 4 + k])

        def forward(n):
            to_part[n].wait_recv()
            return send(hall.at[2, head_cuts[n]], hall.at[0, head_cuts[n]], misc_ss.at[3 + n], misc_rs.at[3 + n], sib)

        project(x_ref[...], [(h, 0) for h in range(GROUPS)])
        to_model((0, 0), (1, 0))
        to_sib.wait_recv()
        project(hall[1], [(h, 1) for h in range(GROUPS)])
        to_model((0, 1), (1, 1))
        forward(0).wait_recv()
        project(jnp.concatenate([hall[2, head_cuts[0], :], hall[0, head_cuts[0], :]], axis=0), [(0, 2), (0, 3)])
        to_model((0, 2), (0, 3), (2, 0), (2, 1))
        rest = forward(1)
        project(hall[2, head_cuts[1], :], [(h, 2) for h in range(1, GROUPS)])
        to_model((1, 2))
        rest.wait_recv()
        project(hall[0, head_cuts[1], :], [(h, 3) for h in range(1, GROUPS)])
        to_model((1, 3), (2, 2), (2, 3), (3, 0), (3, 1), (3, 2), (3, 3))
        stats = {}

        def attn_sums(h):
            for k, block in enumerate(blocks):
                y_copies[h][k].wait_recv()
                total = apart[h, block, :] + arecv[h, block, :]
                arecv[h, block, :] = total
                square_sums(h, block, total)
            stats[h] = start_scales(h, 0)

        def attn_residual(h):
            end_scales(h, 0, stats[h])
            if raw:
                for copy in raw_copies[h * 3:h * 3 + 3]:
                    copy.wait_recv()
            for block in blocks:
                residual = res_ref[h, block, :].astype(jnp.float32)
                mid = (residual + scaled(h, block, arecv[h, block, :], 0)).astype(jnp.bfloat16).astype(jnp.float32)
                arecv[h, block, :] = mid
            for block in blocks:
                square_sums(h, block, arecv[h, block, :])
            stats[h] = start_scales(h, 1)

        def attn_normed(h):
            mpart[h] = jnp.zeros((n_group, share), jnp.float32)
            end_scales(h, 1, stats[h])
            for block in blocks:
                hp[h, block, :] = scaled(h, block, arecv[h, block, :], 1).astype(jnp.bfloat16)

        def to_sibling(s):
            return remote(sib_out.at[s], sib_in.at[s], ff_ss.at[0, s], ff_rs.at[0, s], sib)

        def to_partner(s):
            return remote(mine.at[s, pl.ds(0, rows)], x_in.at[s], ff_ss.at[1, s], ff_rs.at[1, s], part)

        def act_partner(s):
            return remote(u_all.at[s, OWN], u_all.at[s, PART], ff_ss.at[2, s], ff_rs.at[2, s], part)

        def act_sibling(s):
            return remote(u_all.at[s, OWN], u_all.at[s, SIB], ff_ss.at[3, s], ff_rs.at[3, s], sib)

        def act_forward(s):
            return remote(u_all.at[s, PART], u_all.at[s, DIAG], ff_ss.at[4, s], ff_rs.at[4, s], sib)

        def add_sibling(s):
            to_sibling(s).wait_recv()
            mine[s] = mine[s] + sib_in[s]

            @pl.when(s >= IN_FLIGHT)
            def _():
                to_partner(s - IN_FLIGHT).wait_send()
            to_partner(s).start()

        def gate_up(h, start, end):
            @pl.loop(start, end)
            def _(c):
                s = h * n_ff + c
                cols = pl.ds(pl.multiple_of(c * FF_CHUNK, FF_CHUNK), FF_CHUNK)
                for k, weight in enumerate((wg, wu)):
                    sums = jnp.dot(hp[h], weight[:, cols], preferred_element_type=jnp.float32)
                    sib_out[s, :, pl.ds(k * FF_CHUNK, FF_CHUNK)] = sums[:2 * rows]
                    mine[s, :, pl.ds(k * FF_CHUNK, FF_CHUNK)] = sums[2 * rows:]
                to_sibling(s).start()

                @pl.when(s >= 1)
                def _():
                    add_sibling(s - 1)

        attn_sums(0)
        if qkv:
            relay_weights(0)
        attn_residual(0)
        if qkv:
            relay_weights(1)
        attn_sums(1)
        attn_normed(0)
        wg_load.wait()
        wu_load.wait()
        cuts = (n_ff * 3 // 10, n_ff * 7 // 10)
        for h in range(GROUPS):
            if h + 1 < GROUPS:
                gate_up(h, 0, cuts[0])
                attn_residual(h + 1)
                gate_up(h, cuts[0], cuts[1])
                attn_normed(h + 1)
                if h + 2 < GROUPS:
                    attn_sums(h + 2)
                gate_up(h, cuts[1], n_ff)
            else:
                gate_up(h, 0, n_ff)
        add_sibling(GROUPS * n_ff - 1)
        @pl.loop(0, GROUPS * n_ff)
        def _(s):
            to_partner(s).wait_recv()
            both = mine[s, pl.ds(rows, rows), :] + x_in[s]
            u_all[s, OWN, :] = (jax.nn.gelu(both[:, :FF_CHUNK], approximate=True) * both[:, FF_CHUNK:]).astype(jnp.bfloat16)
            act_partner(s).start()
            act_sibling(s).start()

        wd_load.wait()

        def down(h, c):
            s = h * n_ff + c
            act_sibling(s).wait_recv()
            act_forward(s).wait_recv()
            deep = pl.ds(pl.multiple_of(c * FF_CHUNK, FF_CHUNK), FF_CHUNK)
            mpart[h] += jnp.dot(u_all[s], wd[deep, :], preferred_element_type=jnp.float32)

        m_copies = []
        for h in range(GROUPS):
            @pl.loop(0, n_ff)
            def _(c):
                act_partner(h * n_ff + c).wait_recv()
                act_forward(h * n_ff + c).start()

                @pl.when(c >= 1)
                def _():
                    down(h, c - 1)

            down(h, n_ff - 1)
            m_copies.append(send(mpart.at[h], mrecv.at[h], y_ss.at[4 * GROUPS + h], y_rs.at[4 * GROUPS + h]))

        out_copies = []

        def ff_sums(h):
            m_copies[h].wait_recv()
            for block in blocks:
                total = mpart[h, block, :] + mrecv[h, block, :]
                mrecv[h, block, :] = total
                square_sums(h, block, total)
            stats[h] = start_scales(h, 2)

        def ff_residual(h):
            end_scales(h, 2, stats[h])
            for block in blocks:
                value = (arecv[h, block, :] + scaled(h, block, mrecv[h, block, :], 2)).astype(jnp.bfloat16)
                if qkv:
                    hid_ref[h, block, :] = value
                else:
                    hp[h, block, :] = value
            if qkv:
                for block in blocks:
                    square_sums(h, block, hid_ref[h, block, :].astype(jnp.float32))
                stats[h] = start_scales(h, 3)
            else:
                for k, (dev, block) in enumerate(((sib, SIB), (part, PART), (diag, DIAG))):
                    i = 5 + h * 3 + k
                    out_copies.append(send(hp.at[h, block, :], out_ref.at[mine_rows[h], my_cols], misc_ss.at[i], misc_rs.at[i], dev))
                out_ref[mine_rows[h], my_cols] = hp[h, OWN, :]

        def ff_normed(h):
            end_scales(h, 3, stats[h])
            for block in blocks:
                hp[h, block, :] = scaled(h, block, hid_ref[h, block, :].astype(jnp.float32), 3).astype(jnp.bfloat16)
            start_qkv(h)

        ff_sums(0)
        ff_sums(1)
        ff_residual(0)
        ff_sums(2)
        ff_residual(1)
        if qkv:
            ff_normed(0)
        ff_sums(3)
        ff_residual(2)
        if qkv:
            ff_normed(1)
        ff_residual(3)
        if qkv:
            ff_normed(2)
            ff_normed(3)
        if qkv:
            end_qkv()
        for copy in out_copies:
            copy.wait_recv()

        @pl.loop(0, GROUPS * n_ff)
        def _(s):
            for copy in (to_sibling(s), act_partner(s), act_sibling(s), act_forward(s)):
                copy.wait_send()
        for s in range(GROUPS * n_ff - IN_FLIGHT, GROUPS * n_ff):
            to_partner(s).wait_send()
    for copy in sends:
        copy.wait_send()


def comm(x, gains, in_weights=None, post=None, layer=0, collective_id=0):
    rows = x.shape[0] // GROUPS
    share = gains.shape[2] // 4
    n_group = rows * 4
    f32, bf16, vmem, hbm = jnp.float32, jnp.bfloat16, pl.BlockSpec(memory_space=pltpu.VMEM), pl.BlockSpec(memory_space=pltpu.HBM)
    dma = pltpu.SemaphoreType.DMA
    args, specs = [x, gains], [hbm, hbm]
    raw = post is not None and post[0].ndim == 2
    if post is not None and not raw:
        specs[0] = vmem
    n_stat = 4 * GROUPS
    n_misc = 5 + 3 * GROUPS
    scratch = [pltpu.VMEM(x.shape, bf16)] if raw or post is None else []
    scratch += [pltpu.VMEM(gains.shape, bf16), pltpu.VMEM((GROUPS, LANES, LANES), f32), pltpu.VMEM((n_stat, 8, LANES), f32), pltpu.VMEM((n_stat, 3, 8, LANES), f32), pltpu.VMEM((GROUPS, n_group, share), bf16),
               dma((n_stat, 3)), dma((n_stat, 3)), dma((n_misc,)), dma((n_misc,)), dma((10,))]
    if post is None:
        scratch.append(pltpu.VMEM(x.shape, bf16))
    n_ff = n_q = 0
    if post is not None:
        residual, w_o, w_gate, w_up, w_down = post
        args += list(post)
        specs += [hbm if raw else vmem] * 2 + [hbm] * 3
        ff = w_gate.shape[2]
        n_ff = ff // FF_CHUNK
        steps = GROUPS * n_ff
        scratch += [pltpu.VMEM(residual.shape, bf16), pltpu.VMEM((GROUPS, n_group, share), bf16), pltpu.VMEM(w_o.shape[1:], bf16)] if raw else []
        scratch += [pltpu.VMEM((3, GROUPS * rows, w_o.shape[1]), bf16)] + [pltpu.VMEM((GROUPS, n_group, share), f32)] * 4
        scratch += [pltpu.VMEM((share, ff), bf16), pltpu.VMEM((share, ff), bf16), pltpu.VMEM((ff, share), bf16)]
        scratch += [pltpu.VMEM((steps, 2 * rows, 2 * FF_CHUNK), f32)] * 3 + [pltpu.VMEM((steps, rows, 2 * FF_CHUNK), f32), pltpu.VMEM((steps, n_group, FF_CHUNK), bf16)]
        scratch += [dma((5 * GROUPS,)), dma((5 * GROUPS,)), dma((5, steps)), dma((5, steps))]
    if in_weights is not None:
        args += list(in_weights)
        specs += [hbm] * 3
        n_in = sum(w.shape[2] * w.shape[3] for w in in_weights)
        n_q = n_in // QKV_CHUNK
        scratch += [pltpu.VMEM((share, n_in), bf16)] + [pltpu.VMEM(w.shape[1:], bf16) for w in in_weights]
        scratch += [pltpu.VMEM((GROUPS * n_q, 2 * rows, QKV_CHUNK), f32)] * 3 + [pltpu.VMEM((GROUPS * n_q, rows, QKV_CHUNK), f32), dma((2, GROUPS * n_q)), dma((2, GROUPS * n_q))]
        out_shape = [jax.ShapeDtypeStruct((GROUPS, n_group, share), bf16), jax.ShapeDtypeStruct((GROUPS * rows, n_in), f32)][post is None:]
        out_specs = [vmem, vmem][post is None:]
    else:
        out_shape = jax.ShapeDtypeStruct((GROUPS * rows, 4 * share), bf16)
        out_specs = vmem
    cfg = {"raw": raw, "post": post is not None, "qkv": in_weights is not None, "layer": layer, "rows": rows, "share": share, "width": 4 * share, "n_ff": n_ff, "n_q": n_q}
    return pl.pallas_call(
        functools.partial(comm_kernel, cfg),
        out_shape=out_shape, in_specs=specs, out_specs=out_specs, scratch_shapes=scratch,
        compiler_params=pltpu.CompilerParams(collective_id=collective_id, has_side_effects=True, vmem_limit_bytes=int((62, 62, 49)[collective_id] * 2**20)),
        name=f"comm_{collective_id}",
    )(*args)


def solution(mesh):
    def device_step(hidden, positions, k_local, v_local, k_global, v_global, w_q, w_k, w_v, w_o, w_gate, w_up, w_down, norm_gains):
        share = w_q.shape[1]
        tables = rope_tables(positions, w_q.shape[3])
        in_weights = (w_q, w_k, w_v)
        post_weights = (w_o.reshape(2, -1, share), w_gate, w_up, w_down)
        hidden_rows = hidden[:, 0, :]
        qkv, = comm(hidden_rows, norm_gains, in_weights, layer=-1, collective_id=0)
        heads, k_local, v_local = attend(qkv, tables, positions, k_local, v_local)
        residual, qkv = comm(heads, norm_gains, in_weights, (hidden_rows,) + post_weights, layer=0, collective_id=1)
        heads, k_global, v_global = attend(qkv, tables, positions, k_global, v_global)
        final = comm(heads, norm_gains, None, (residual,) + post_weights, layer=1, collective_id=2)[:, None, :]
        return final, k_local, v_local, k_global, v_global

    in_specs = (ROW_SPEC, POS_SPEC, CACHE_SPEC, CACHE_SPEC, CACHE_SPEC, CACHE_SPEC, PROJ_IN_SPEC, PROJ_IN_SPEC, PROJ_IN_SPEC, PROJ_OUT_SPEC, FF_IN_SPEC, FF_IN_SPEC, FF_OUT_SPEC, GAIN_SPEC)
    out_specs = (ROW_SPEC, CACHE_SPEC, CACHE_SPEC, CACHE_SPEC, CACHE_SPEC)
    return jax.shard_map(device_step, mesh=mesh, in_specs=in_specs, out_specs=out_specs, check_vma=False)
```

```python
import functools

import jax
import jax.numpy as jnp
from jax import lax
from jax.experimental import pallas as pl
from jax.experimental.pallas import tpu as pltpu
from jax.sharding import PartitionSpec as P

SOFT_CAP = 50.0
NORM_EPS = 1e-6
ROPE_BASE = 10000.0

ROW_SPEC = P(("part", "data"), None, None)
POS_SPEC = P(("part", "data"))
CACHE_SPEC = P(("part", "data"), None, "model", None)
PROJ_IN_SPEC = P(None, "data", "model", None)
PROJ_OUT_SPEC = P(None, "model", None, "data")
FF_IN_SPEC = P(None, "data", "model")
FF_OUT_SPEC = P(None, "model", "data")
GAIN_SPEC = P(None, None, None)


def rope_tables(positions, head_dim):
    inv_freq = ROPE_BASE ** (-jnp.arange(0, head_dim, 2).astype(jnp.float32) / head_dim)
    angles = positions.astype(jnp.float32)[:, None] * inv_freq[None, :]
    return jnp.cos(angles), jnp.sin(angles)


LANES = 128


def attend_kernel(cache_len, n_rows, group, depth, pos_ref, qkv_ref, cos_ref, sin_ref, k_hbm, v_hbm, head_ref, ko_hbm, vo_hbm, kbuf, vbuf, q8, kn, vn, outs, sbuf, pbuf, rd_sem, wr_sem):
    n_steps = n_rows // group
    n_cols = cache_len * 4

    def reads(step):
        slot = lax.rem(step, depth)
        rows = pl.ds(step * group, group)
        return (pltpu.make_async_copy(k_hbm.at[rows], kbuf.at[slot], rd_sem.at[0, slot]),
                pltpu.make_async_copy(v_hbm.at[rows], vbuf.at[slot], rd_sem.at[1, slot]))

    def writes(step):
        slot = lax.rem(step, depth)
        rows = pl.ds(step * group, group)
        return (pltpu.make_async_copy(kbuf.at[slot], ko_hbm.at[rows], wr_sem.at[0, slot]),
                pltpu.make_async_copy(vbuf.at[slot], vo_hbm.at[rows], wr_sem.at[1, slot]))

    ahead = depth // 2 if depth < n_steps else n_steps
    for step in range(ahead):
        for copy in reads(step):
            copy.start()

    cos_t, sin_t = cos_ref[...], sin_ref[...]
    scale = (2 * LANES) ** -0.5
    for h in range(4):
        first, second = qkv_ref[:, h * 256:h * 256 + LANES], qkv_ref[:, h * 256 + LANES:h * 256 + 256]
        q8[:, h, :] = (first * cos_t - second * sin_t) * scale
        q8[:, 4 + h, :] = (second * cos_t + first * sin_t) * scale
    for h in range(2):
        base = 1024 + h * 256
        first, second = qkv_ref[:, base:base + LANES], qkv_ref[:, base + LANES:base + 256]
        halves = (first * cos_t - second * sin_t, second * cos_t + first * sin_t)
        for half in range(2):
            value = qkv_ref[:, base + 512 + half * LANES:base + 512 + (half + 1) * LANES]
            for i in range(4):
                kn[:, i * 4 + half * 2 + h, :] = halves[half]
                vn[:, i * 4 + half * 2 + h, :] = value

    row_id = lax.broadcasted_iota(jnp.int32, (8, n_cols), 0)
    col_id = lax.broadcasted_iota(jnp.int32, (8, n_cols), 1)
    half_col = (col_id // 2) % 2
    same_half = row_id // 4 == half_col
    same_kv = (row_id // 2) % 2 == col_id % 2
    slot_col = col_id // 4
    sub_id = lax.broadcasted_iota(jnp.int32, (16, LANES), 0) // 4

    @pl.loop(0, n_steps)
    def _(step):
        slot = lax.rem(step, depth)
        if ahead < n_steps:
            @pl.when(step + ahead < n_steps)
            def _():
                @pl.when(step >= depth - ahead)
                def _():
                    for copy in writes(step - (depth - ahead)):
                        copy.wait()
                for copy in reads(step + ahead):
                    copy.start()

        for copy in reads(step):
            copy.wait()
        for i in range(group):
            row = step * group + i
            now = lax.rem(pos_ref[row], cache_len)
            window = pl.ds(pl.multiple_of(now // 4 * 16, 16), 16)
            hit = sub_id == lax.rem(now, 4)
            kbuf[slot, i, window, :] = jnp.where(hit, kn[row].astype(jnp.bfloat16), kbuf[slot, i, window, :])
            vbuf[slot, i, window, :] = jnp.where(hit, vn[row].astype(jnp.bfloat16), vbuf[slot, i, window, :])
        for i in range(group):
            part = lax.dot_general(q8[step * group + i].astype(jnp.bfloat16), kbuf[slot, i], (((1,), (1,)), ((), ())), preferred_element_type=jnp.float32)
            sbuf[i] = jnp.where(same_half & same_kv, part, 0.0)
        for i in range(group):
            part = sbuf[i]
            part = part + pltpu.roll(part, 4, 0)
            other = jnp.where(half_col == 0, pltpu.roll(part, n_cols - 2, 1), pltpu.roll(part, 2, 1))
            scores = SOFT_CAP * jnp.tanh((part + other) / SOFT_CAP)
            scores = jnp.where(same_kv & (slot_col <= pos_ref[step * group + i]), scores, -1e30)
            weights = jnp.exp(scores - jnp.max(scores, axis=1, keepdims=True))
            total = jnp.sum(jnp.where(same_half, weights, 0.0), axis=1, keepdims=True)
            pbuf[i] = jnp.where(same_half, weights / total, 0.0).astype(jnp.bfloat16)
        for i in range(group):
            outs[step * group + i] = jnp.dot(pbuf[i], vbuf[slot, i], preferred_element_type=jnp.float32)
        for copy in writes(step):
            copy.start()

    for h in range(4):
        for half in range(2):
            head_ref[:, h * 256 + half * LANES:h * 256 + (half + 1) * LANES] = outs[:, half * 4 + h, :].astype(jnp.bfloat16)
    for step in range(max(n_steps - depth, 0) if ahead < n_steps else 0, n_steps):
        for copy in writes(step):
            copy.wait()


def attend(qkv, tables, positions, k_cache, v_cache):
    n_rows, cache_len, kv_loc, head_dim = k_cache.shape
    halves = head_dim // LANES
    group = 32 if cache_len <= 64 else 4
    depth = 2 if cache_len <= 64 else 6
    f32, bf16 = jnp.float32, jnp.bfloat16

    def flat(cache):
        return cache.reshape(n_rows, cache_len, kv_loc, halves, LANES).transpose(0, 1, 3, 2, 4).reshape(n_rows, cache_len * halves * kv_loc, LANES)

    def unflat(cache):
        return cache.reshape(n_rows, cache_len, halves, kv_loc, LANES).transpose(0, 1, 3, 2, 4).reshape(n_rows, cache_len, kv_loc, head_dim)

    vmem, hbm = pl.BlockSpec(memory_space=pltpu.VMEM), pl.BlockSpec(memory_space=pltpu.HBM)
    k_flat, v_flat = flat(k_cache), flat(v_cache)
    n_cols = k_flat.shape[1]
    block = (depth, group, n_cols, LANES)
    dma = pltpu.SemaphoreType.DMA
    heads, k_out, v_out = pl.pallas_call(
        functools.partial(attend_kernel, cache_len, n_rows, group, depth),
        out_shape=(jax.ShapeDtypeStruct((n_rows, 4 * head_dim), bf16), jax.ShapeDtypeStruct(k_flat.shape, bf16), jax.ShapeDtypeStruct(v_flat.shape, bf16)),
        in_specs=[pl.BlockSpec(memory_space=pltpu.SMEM), vmem, vmem, vmem, hbm, hbm],
        out_specs=(vmem, hbm, hbm),
        scratch_shapes=[pltpu.VMEM(block, bf16), pltpu.VMEM(block, bf16), pltpu.VMEM((n_rows, 8, LANES), f32), pltpu.VMEM((n_rows, 16, LANES), f32),
                        pltpu.VMEM((n_rows, 16, LANES), f32), pltpu.VMEM((n_rows, 8, LANES), f32), pltpu.VMEM((group, 8, n_cols), f32), pltpu.VMEM((group, 8, n_cols), bf16),
                        dma((2, depth)), dma((2, depth))],
        compiler_params=pltpu.CompilerParams(vmem_limit_bytes=int((62 if cache_len <= 64 else 34) * 2**20)),
        cost_estimate=pl.CostEstimate(flops=n_rows * 8 * n_cols * LANES * 4, bytes_accessed=4 * k_flat.size * 2, transcendentals=0),
        name=f"attend_{cache_len}",
    )(positions, qkv, *tables, k_flat, v_flat)
    return heads, unflat(k_out), unflat(v_out)


FF_CHUNK = 512
IN_FLIGHT = 4
QKV_CHUNK = 1024
MESH = pl.DeviceIdType.MESH


GROUPS = 4


def comm_kernel(cfg, *refs):
    it = iter(refs)
    post, layer, rows, share, width = cfg["post"], cfg["layer"], cfg["rows"], cfg["share"], cfg["width"]
    qkv, n_ff, n_q = cfg["qkv"], cfg["n_ff"], cfg["n_q"]
    raw = cfg["raw"]
    x_any, g_hbm = next(it), next(it)
    if post:
        res_any, wo_any, wg_hbm, wu_hbm, wd_hbm = (next(it) for _ in range(5))
    if qkv:
        wq_hbm, wk_hbm, wv_hbm = (next(it) for _ in range(3))
        if post:
            hid_ref = next(it)
        qkv_ref = next(it)
    else:
        out_ref = next(it)
    if raw or not post:
        x_ref = next(it)
    g_ref, tcol, st_src, st_rcv, hp, st_ss, st_rs, misc_ss, misc_rs, ld_sem = (next(it) for _ in range(10))
    if not post:
        out_rows = next(it)
    if post:
        if raw:
            raw_ref, res_ref, wo = (next(it) for _ in range(3))
        hall, apart, arecv, mpart, mrecv, wg, wu, wd, sib_out, sib_in, mine, x_in, u_all = (next(it) for _ in range(13))
        y_ss, y_rs, ff_ss, ff_rs = (next(it) for _ in range(4))
    if qkv:
        wi, wq, wk, wv, q_out, q_in, q_mine, q_x, q_ss, q_rs = (next(it) for _ in range(10))

    model, me = lax.axis_index("model"), lax.axis_index("data")
    x_pos, core = me // 2, lax.rem(me, 2)
    sib, part, diag = x_pos * 2 + 1 - core, (1 - x_pos) * 2 + core, (1 - x_pos) * 2 + 1 - core
    n_group = 4 * rows
    DIAG, SIB, PART, OWN = (pl.ds(i * rows, rows) for i in range(4))
    blocks = (OWN, SIB, PART, DIAG)
    mine_rows = [pl.ds(h * rows, rows) for h in range(GROUPS)]
    sends = []

    def remote(src, dst, send_sem, recv_sem, data=None):
        where = {"data": data} if data is not None else {"model": 1 - model}
        return pltpu.make_async_remote_copy(src_ref=src, dst_ref=dst, send_sem=send_sem, recv_sem=recv_sem, device_id=where, device_id_type=MESH)

    def send(*args):
        copy = remote(*args)
        copy.start()
        sends.append(copy)
        return copy

    def load(src, dst, sem):
        copy = pltpu.make_async_copy(src, dst, sem)
        copy.start()
        return copy

    early = [load(g_hbm, g_ref, ld_sem.at[8])]
    if post and not raw:
        x_ref = x_any
    else:
        early.append(load(x_any, x_ref, ld_sem.at[7]))
    if post:
        if raw:
            early.append(load(res_any, raw_ref, ld_sem.at[9]))
        else:
            res_ref = res_any
        if raw:
            wo_load = load(wo_any.at[layer], wo, ld_sem.at[0])
        else:
            wo = wo_any.at[layer]
        wg_load = load(wg_hbm.at[layer], wg, ld_sem.at[1])
        wu_load = load(wu_hbm.at[layer], wu, ld_sem.at[2])
        wd_load = load(wd_hbm.at[layer], wd, ld_sem.at[3])
    if qkv:
        in_loads = [load(src.at[layer + 1], dst, ld_sem.at[4 + k]) for k, (src, dst) in enumerate(((wq_hbm, wq), (wk_hbm, wk), (wv_hbm, wv)))]

    def relay_weights(c):
        col = c * QKV_CHUNK
        for k in ((0,), (1, 2))[c]:
            in_loads[k].wait()
            weight = (wq, wk, wv)[k]
            n_heads, head_dim = weight.shape[1:]
            for h in range(n_heads):
                wi[:, col:col + head_dim] = weight[:, h, :]
                col += head_dim

    barrier = pltpu.get_barrier_semaphore()
    for dev in (sib, part, diag):
        pl.semaphore_signal(barrier, inc=1, device_id={"data": dev}, device_id_type=MESH)
    pl.semaphore_signal(barrier, inc=1, device_id={"model": 1 - model}, device_id_type=MESH)
    tcol[...] = jnp.zeros_like(tcol)
    for copy in early:
        copy.wait()
    pl.semaphore_wait(barrier, 4)

    def square_sums(h, block, value):
        total = None
        for k in range(share // LANES):
            piece = value[:, k * LANES:(k + 1) * LANES]
            total = piece * piece if total is None else total + piece * piece
        tcol[h, block, :] = total

    lane_block = lax.broadcasted_iota(jnp.int32, (8, LANES), 1) // rows

    def start_scales(h, which):
        idx = which * GROUPS + h
        st_src[idx] = jnp.sum(jnp.transpose(tcol[h]).reshape(LANES // 8, 8, LANES), axis=0)
        return [send(st_src.at[idx], st_rcv.at[idx, k], st_ss.at[idx, k], st_rs.at[idx, k], dev) for k, dev in enumerate((sib, part, diag))]

    def end_scales(h, which, copies):
        idx = which * GROUPS + h
        for copy in copies:
            copy.wait_recv()

        def exchange(value, n):
            even = lax.rem(lane_block // n, 2) == 0
            return jnp.where(even, pltpu.roll(value, LANES - n * rows, 1), pltpu.roll(value, n * rows, 1))

        total = st_src[idx] + exchange(st_rcv[idx, 0], 2) + exchange(st_rcv[idx, 1], 1) + exchange(exchange(st_rcv[idx, 2], 1), 2)
        total = jnp.sum(total, axis=0, keepdims=True)
        inverse = lax.rsqrt(total / width + NORM_EPS)
        tcol[h] = jnp.transpose(jnp.broadcast_to(inverse, (LANES, LANES)))

    def gain_row(k):
        at, which = (layer + 1, 0) if k == 3 else (layer, k + 1)
        return 1.0 + g_ref[at, which:which + 1, pl.ds(pl.multiple_of(me * share, LANES), share)].astype(jnp.float32)

    def scaled(h, block, value, gain):
        return value * jnp.concatenate([tcol[h, block, :]] * (share // LANES), axis=1) * gain_row(gain)

    def q_partner(s):
        return remote(q_mine.at[s, pl.ds(0, rows)], q_x.at[s], q_ss.at[1, s], q_rs.at[1, s], part)

    def finish_qkv(pending):
        if pending is not None:
            s, copy = pending
            copy.wait_recv()
            q_mine[s] = q_mine[s] + q_in[s]
            q_partner(s).start()

    def start_qkv(h, pending=None):
        for c in range(n_q):
            s = h * n_q + c
            sums = jnp.dot(hp[h], wi[:, c * QKV_CHUNK:(c + 1) * QKV_CHUNK], preferred_element_type=jnp.float32)
            q_out[s] = sums[:2 * rows]
            q_mine[s] = sums[2 * rows:]
            copy = send(q_out.at[s], q_in.at[s], q_ss.at[0, s], q_rs.at[0, s], sib)
            finish_qkv(pending)
            pending = s, copy
        return pending

    def end_qkv():
        for h in range(GROUPS):
            for c in range(n_q):
                s = h * n_q + c
                q_partner(s).wait_recv()
                qkv_ref[mine_rows[h], c * QKV_CHUNK:(c + 1) * QKV_CHUNK] = q_mine[s, pl.ds(rows, rows), :] + q_x[s]
        for s in range(GROUPS * n_q):
            q_partner(s).wait_send()

    def spread(src, dst, base):
        copies = []
        for h in range(GROUPS):
            for k, (dev, there) in enumerate(((sib, SIB), (part, PART), (diag, DIAG))):
                cols = pl.ds(pl.multiple_of(dev * share, LANES), share)
                i = base + h * 3 + k
                copies.append(send(src.at[mine_rows[h], cols], dst.at[h, there, :], misc_ss.at[i], misc_rs.at[i], dev))
        return copies

    my_cols = pl.ds(pl.multiple_of(me * share, LANES), share)
    if not post:
        xn = out_rows
        for h in range(GROUPS):
            value = x_ref[mine_rows[h], :].astype(jnp.float32)
            inverse = lax.rsqrt(jnp.mean(value * value, axis=1, keepdims=True) + NORM_EPS)
            xn[mine_rows[h], :] = (value * inverse * (1.0 + g_ref[0, 0:1, :].astype(jnp.float32))).astype(jnp.bfloat16)
        copies = spread(xn, hp, 0)
        pending = None
        relay_weights(0)
        relay_weights(1)
        for h in range(GROUPS):
            hp[h, OWN, :] = xn[mine_rows[h], my_cols]
            for copy in copies[h * 3:h * 3 + 3]:
                copy.wait_recv()
            pending = start_qkv(h, pending)
        finish_qkv(pending)
        end_qkv()
    else:
        head_cuts = (pl.ds(0, rows), pl.ds(rows, (GROUPS - 1) * rows))
        to_part = [send(x_ref.at[cut], hall.at[2, cut], misc_ss.at[n], misc_rs.at[n], part) for n, cut in enumerate(head_cuts)]
        to_sib = send(x_ref, hall.at[1], misc_ss.at[2], misc_rs.at[2], sib)
        if raw:
            raw_copies = spread(raw_ref, res_ref, 5)
            for h in range(GROUPS):
                res_ref[h, OWN, :] = raw_ref[mine_rows[h], my_cols]
        if raw:
            wo_load.wait()
        y_copies = [[None] * 4 for _ in range(GROUPS)]

        def project(heads, places):
            sums = jnp.dot(heads, wo[...], preferred_element_type=jnp.float32)
            for n, (h, k) in enumerate(places):
                apart[h, blocks[k], :] = sums[n * rows:(n + 1) * rows]

        def to_model(*pairs):
            for h, k in pairs:
                y_copies[h][k] = send(apart.at[h, blocks[k], :], arecv.at[h, blocks[k], :], y_ss.at[h * 4 + k], y_rs.at[h * 4 + k])

        def forward(n):
            to_part[n].wait_recv()
            return send(hall.at[2, head_cuts[n]], hall.at[0, head_cuts[n]], misc_ss.at[3 + n], misc_rs.at[3 + n], sib)

        project(x_ref[...], [(h, 0) for h in range(GROUPS)])
        to_model((0, 0), (1, 0))
        to_sib.wait_recv()
        project(hall[1], [(h, 1) for h in range(GROUPS)])
        to_model((0, 1), (1, 1))
        forward(0).wait_recv()
        project(jnp.concatenate([hall[2, head_cuts[0], :], hall[0, head_cuts[0], :]], axis=0), [(0, 2), (0, 3)])
        to_model((0, 2), (0, 3), (2, 0), (2, 1))
        rest = forward(1)
        project(hall[2, head_cuts[1], :], [(h, 2) for h in range(1, GROUPS)])
        to_model((1, 2))
        rest.wait_recv()
        project(hall[0, head_cuts[1], :], [(h, 3) for h in range(1, GROUPS)])
        to_model((1, 3), (2, 2), (2, 3), (3, 0), (3, 1), (3, 2), (3, 3))
        stats = {}

        def attn_sums(h):
            for k, block in enumerate(blocks):
                y_copies[h][k].wait_recv()
                total = apart[h, block, :] + arecv[h, block, :]
                arecv[h, block, :] = total
                square_sums(h, block, total)
            stats[h] = start_scales(h, 0)

        def attn_residual(h):
            end_scales(h, 0, stats[h])
            if raw:
                for copy in raw_copies[h * 3:h * 3 + 3]:
                    copy.wait_recv()
            for block in blocks:
                residual = res_ref[h, block, :].astype(jnp.float32)
                mid = (residual + scaled(h, block, arecv[h, block, :], 0)).astype(jnp.bfloat16).astype(jnp.float32)
                arecv[h, block, :] = mid
            for block in blocks:
                square_sums(h, block, arecv[h, block, :])
            stats[h] = start_scales(h, 1)

        def attn_normed(h):
            mpart[h] = jnp.zeros((n_group, share), jnp.float32)
            end_scales(h, 1, stats[h])
            for block in blocks:
                hp[h, block, :] = scaled(h, block, arecv[h, block, :], 1).astype(jnp.bfloat16)

        def to_sibling(s):
            return remote(sib_out.at[s], sib_in.at[s], ff_ss.at[0, s], ff_rs.at[0, s], sib)

        def to_partner(s):
            return remote(mine.at[s, pl.ds(0, rows)], x_in.at[s], ff_ss.at[1, s], ff_rs.at[1, s], part)

        def act_partner(s):
            return remote(u_all.at[s, OWN], u_all.at[s, PART], ff_ss.at[2, s], ff_rs.at[2, s], part)

        def act_sibling(s):
            return remote(u_all.at[s, OWN], u_all.at[s, SIB], ff_ss.at[3, s], ff_rs.at[3, s], sib)

        def act_forward(s):
            return remote(u_all.at[s, PART], u_all.at[s, DIAG], ff_ss.at[4, s], ff_rs.at[4, s], sib)

        def add_sibling(s):
            to_sibling(s).wait_recv()
            mine[s] = mine[s] + sib_in[s]

            @pl.when(s >= IN_FLIGHT)
            def _():
                to_partner(s - IN_FLIGHT).wait_send()
            to_partner(s).start()

        def gate_up(h, start, end):
            @pl.loop(start, end)
            def _(c):
                s = h * n_ff + c
                cols = pl.ds(pl.multiple_of(c * FF_CHUNK, FF_CHUNK), FF_CHUNK)
                for k, weight in enumerate((wg, wu)):
                    sums = jnp.dot(hp[h], weight[:, cols], preferred_element_type=jnp.float32)
                    sib_out[s, :, pl.ds(k * FF_CHUNK, FF_CHUNK)] = sums[:2 * rows]
                    mine[s, :, pl.ds(k * FF_CHUNK, FF_CHUNK)] = sums[2 * rows:]
                to_sibling(s).start()

                @pl.when(s >= 1)
                def _():
                    add_sibling(s - 1)

        attn_sums(0)
        if qkv:
            relay_weights(0)
        attn_residual(0)
        if qkv:
            relay_weights(1)
        attn_sums(1)
        attn_normed(0)
        wg_load.wait()
        wu_load.wait()
        cuts = (n_ff * 3 // 10, n_ff * 7 // 10)
        for h in range(GROUPS):
            if h + 1 < GROUPS:
                gate_up(h, 0, cuts[0])
                attn_residual(h + 1)
                gate_up(h, cuts[0], cuts[1])
                attn_normed(h + 1)
                if h + 2 < GROUPS:
                    attn_sums(h + 2)
                gate_up(h, cuts[1], n_ff)
            else:
                gate_up(h, 0, n_ff)
        add_sibling(GROUPS * n_ff - 1)
        @pl.loop(0, GROUPS * n_ff)
        def _(s):
            to_partner(s).wait_recv()
            both = mine[s, pl.ds(rows, rows), :] + x_in[s]
            u_all[s, OWN, :] = (jax.nn.gelu(both[:, :FF_CHUNK], approximate=True) * both[:, FF_CHUNK:]).astype(jnp.bfloat16)
            act_partner(s).start()
            act_sibling(s).start()

        wd_load.wait()

        def down(h, c):
            s = h * n_ff + c
            act_sibling(s).wait_recv()
            act_forward(s).wait_recv()
            deep = pl.ds(pl.multiple_of(c * FF_CHUNK, FF_CHUNK), FF_CHUNK)
            mpart[h] += jnp.dot(u_all[s], wd[deep, :], preferred_element_type=jnp.float32)

        m_copies = []
        for h in range(GROUPS):
            @pl.loop(0, n_ff)
            def _(c):
                act_partner(h * n_ff + c).wait_recv()
                act_forward(h * n_ff + c).start()

                @pl.when(c >= 1)
                def _():
                    down(h, c - 1)

            down(h, n_ff - 1)
            m_copies.append(send(mpart.at[h], mrecv.at[h], y_ss.at[4 * GROUPS + h], y_rs.at[4 * GROUPS + h]))

        out_copies = []

        def ff_sums(h):
            m_copies[h].wait_recv()
            for block in blocks:
                total = mpart[h, block, :] + mrecv[h, block, :]
                mrecv[h, block, :] = total
                square_sums(h, block, total)
            stats[h] = start_scales(h, 2)

        def ff_residual(h):
            end_scales(h, 2, stats[h])
            for block in blocks:
                value = (arecv[h, block, :] + scaled(h, block, mrecv[h, block, :], 2)).astype(jnp.bfloat16)
                if qkv:
                    hid_ref[h, block, :] = value
                else:
                    hp[h, block, :] = value
            if qkv:
                for block in blocks:
                    square_sums(h, block, hid_ref[h, block, :].astype(jnp.float32))
                stats[h] = start_scales(h, 3)
            else:
                for k, (dev, block) in enumerate(((sib, SIB), (part, PART), (diag, DIAG))):
                    i = 5 + h * 3 + k
                    out_copies.append(send(hp.at[h, block, :], out_ref.at[mine_rows[h], my_cols], misc_ss.at[i], misc_rs.at[i], dev))
                out_ref[mine_rows[h], my_cols] = hp[h, OWN, :]

        def ff_normed(h):
            end_scales(h, 3, stats[h])
            for block in blocks:
                hp[h, block, :] = scaled(h, block, hid_ref[h, block, :].astype(jnp.float32), 3).astype(jnp.bfloat16)
            finish_qkv(start_qkv(h))

        ff_sums(0)
        ff_sums(1)
        ff_residual(0)
        ff_sums(2)
        ff_residual(1)
        if qkv:
            ff_normed(0)
        ff_sums(3)
        ff_residual(2)
        if qkv:
            ff_normed(1)
        ff_residual(3)
        if qkv:
            ff_normed(2)
            ff_normed(3)
        if qkv:
            end_qkv()
        for copy in out_copies:
            copy.wait_recv()

        @pl.loop(0, GROUPS * n_ff)
        def _(s):
            for copy in (to_sibling(s), act_partner(s), act_sibling(s), act_forward(s)):
                copy.wait_send()
        for s in range(GROUPS * n_ff - IN_FLIGHT, GROUPS * n_ff):
            to_partner(s).wait_send()
    for copy in sends:
        copy.wait_send()


def comm(x, gains, in_weights=None, post=None, layer=0, collective_id=0):
    rows = x.shape[0] // GROUPS
    share = gains.shape[2] // 4
    n_group = rows * 4
    f32, bf16, vmem, hbm = jnp.float32, jnp.bfloat16, pl.BlockSpec(memory_space=pltpu.VMEM), pl.BlockSpec(memory_space=pltpu.HBM)
    dma = pltpu.SemaphoreType.DMA
    args, specs = [x, gains], [hbm, hbm]
    raw = post is not None and post[0].ndim == 2
    if post is not None and not raw:
        specs[0] = vmem
    n_stat = 4 * GROUPS
    n_misc = 5 + 3 * GROUPS
    scratch = [pltpu.VMEM(x.shape, bf16)] if raw or post is None else []
    scratch += [pltpu.VMEM(gains.shape, bf16), pltpu.VMEM((GROUPS, LANES, LANES), f32), pltpu.VMEM((n_stat, 8, LANES), f32), pltpu.VMEM((n_stat, 3, 8, LANES), f32), pltpu.VMEM((GROUPS, n_group, share), bf16),
               dma((n_stat, 3)), dma((n_stat, 3)), dma((n_misc,)), dma((n_misc,)), dma((10,))]
    if post is None:
        scratch.append(pltpu.VMEM(x.shape, bf16))
    n_ff = n_q = 0
    if post is not None:
        residual, w_o, w_gate, w_up, w_down = post
        args += list(post)
        specs += [hbm if raw else vmem] * 2 + [hbm] * 3
        ff = w_gate.shape[2]
        n_ff = ff // FF_CHUNK
        steps = GROUPS * n_ff
        scratch += [pltpu.VMEM(residual.shape, bf16), pltpu.VMEM((GROUPS, n_group, share), bf16), pltpu.VMEM(w_o.shape[1:], bf16)] if raw else []
        scratch += [pltpu.VMEM((3, GROUPS * rows, w_o.shape[1]), bf16)] + [pltpu.VMEM((GROUPS, n_group, share), f32)] * 4
        scratch += [pltpu.VMEM((share, ff), bf16), pltpu.VMEM((share, ff), bf16), pltpu.VMEM((ff, share), bf16)]
        scratch += [pltpu.VMEM((steps, 2 * rows, 2 * FF_CHUNK), f32)] * 3 + [pltpu.VMEM((steps, rows, 2 * FF_CHUNK), f32), pltpu.VMEM((steps, n_group, FF_CHUNK), bf16)]
        scratch += [dma((5 * GROUPS,)), dma((5 * GROUPS,)), dma((5, steps)), dma((5, steps))]
    if in_weights is not None:
        args += list(in_weights)
        specs += [hbm] * 3
        n_in = sum(w.shape[2] * w.shape[3] for w in in_weights)
        n_q = n_in // QKV_CHUNK
        scratch += [pltpu.VMEM((share, n_in), bf16)] + [pltpu.VMEM(w.shape[1:], bf16) for w in in_weights]
        scratch += [pltpu.VMEM((GROUPS * n_q, 2 * rows, QKV_CHUNK), f32)] * 3 + [pltpu.VMEM((GROUPS * n_q, rows, QKV_CHUNK), f32), dma((2, GROUPS * n_q)), dma((2, GROUPS * n_q))]
        out_shape = [jax.ShapeDtypeStruct((GROUPS, n_group, share), bf16), jax.ShapeDtypeStruct((GROUPS * rows, n_in), f32)][post is None:]
        out_specs = [vmem, vmem][post is None:]
    else:
        out_shape = jax.ShapeDtypeStruct((GROUPS * rows, 4 * share), bf16)
        out_specs = vmem
    cfg = {"raw": raw, "post": post is not None, "qkv": in_weights is not None, "layer": layer, "rows": rows, "share": share, "width": 4 * share, "n_ff": n_ff, "n_q": n_q}
    return pl.pallas_call(
        functools.partial(comm_kernel, cfg),
        out_shape=out_shape, in_specs=specs, out_specs=out_specs, scratch_shapes=scratch,
        compiler_params=pltpu.CompilerParams(collective_id=collective_id, has_side_effects=True, vmem_limit_bytes=int((62, 62, 49)[collective_id] * 2**20)),
        name=f"comm_{collective_id}",
    )(*args)


def solution(mesh):
    def device_step(hidden, positions, k_local, v_local, k_global, v_global, w_q, w_k, w_v, w_o, w_gate, w_up, w_down, norm_gains):
        share = w_q.shape[1]
        tables = rope_tables(positions, w_q.shape[3])
        in_weights = (w_q, w_k, w_v)
        post_weights = (w_o.reshape(2, -1, share), w_gate, w_up, w_down)
        hidden_rows = hidden[:, 0, :]
        qkv, = comm(hidden_rows, norm_gains, in_weights, layer=-1, collective_id=0)
        heads, k_local, v_local = attend(qkv, tables, positions, k_local, v_local)
        residual, qkv = comm(heads, norm_gains, in_weights, (hidden_rows,) + post_weights, layer=0, collective_id=1)
        heads, k_global, v_global = attend(qkv, tables, positions, k_global, v_global)
        final = comm(heads, norm_gains, None, (residual,) + post_weights, layer=1, collective_id=2)[:, None, :]
        return final, k_local, v_local, k_global, v_global

    in_specs = (ROW_SPEC, POS_SPEC, CACHE_SPEC, CACHE_SPEC, CACHE_SPEC, CACHE_SPEC, PROJ_IN_SPEC, PROJ_IN_SPEC, PROJ_IN_SPEC, PROJ_OUT_SPEC, FF_IN_SPEC, FF_IN_SPEC, FF_OUT_SPEC, GAIN_SPEC)
    out_specs = (ROW_SPEC, CACHE_SPEC, CACHE_SPEC, CACHE_SPEC, CACHE_SPEC)
    return jax.shard_map(device_step, mesh=mesh, in_specs=in_specs, out_specs=out_specs, check_vma=False)
```

```python
import functools

import jax
import jax.numpy as jnp
from jax import lax
from jax.experimental import pallas as pl
from jax.experimental.pallas import tpu as pltpu
from jax.sharding import PartitionSpec as P

SOFT_CAP = 50.0
NORM_EPS = 1e-6
ROPE_BASE = 10000.0

ROW_SPEC = P(("part", "data"), None, None)
POS_SPEC = P(("part", "data"))
CACHE_SPEC = P(("part", "data"), None, "model", None)
PROJ_IN_SPEC = P(None, "data", "model", None)
PROJ_OUT_SPEC = P(None, "model", None, "data")
FF_IN_SPEC = P(None, "data", "model")
FF_OUT_SPEC = P(None, "model", "data")
GAIN_SPEC = P(None, None, None)


def rope_tables(positions, head_dim):
    inv_freq = ROPE_BASE ** (-jnp.arange(0, head_dim, 2).astype(jnp.float32) / head_dim)
    angles = positions.astype(jnp.float32)[:, None] * inv_freq[None, :]
    return jnp.cos(angles), jnp.sin(angles)


LANES = 128


def attend_kernel(cache_len, n_rows, group, depth, pos_ref, qkv_ref, cos_ref, sin_ref, k_hbm, v_hbm, head_ref, ko_hbm, vo_hbm, kbuf, vbuf, q8, kn, vn, outs, sbuf, pbuf, rd_sem, wr_sem):
    n_steps = n_rows // group
    n_cols = cache_len * 4

    def reads(step):
        slot = lax.rem(step, depth)
        rows = pl.ds(step * group, group)
        return (pltpu.make_async_copy(k_hbm.at[rows], kbuf.at[slot], rd_sem.at[0, slot]),
                pltpu.make_async_copy(v_hbm.at[rows], vbuf.at[slot], rd_sem.at[1, slot]))

    def writes(step):
        slot = lax.rem(step, depth)
        rows = pl.ds(step * group, group)
        return (pltpu.make_async_copy(kbuf.at[slot], ko_hbm.at[rows], wr_sem.at[0, slot]),
                pltpu.make_async_copy(vbuf.at[slot], vo_hbm.at[rows], wr_sem.at[1, slot]))

    ahead = depth // 2 if depth < n_steps else n_steps
    for step in range(ahead):
        for copy in reads(step):
            copy.start()

    cos_t, sin_t = cos_ref[...], sin_ref[...]
    scale = (2 * LANES) ** -0.5
    for h in range(4):
        first, second = qkv_ref[:, h * 256:h * 256 + LANES], qkv_ref[:, h * 256 + LANES:h * 256 + 256]
        q8[:, h, :] = (first * cos_t - second * sin_t) * scale
        q8[:, 4 + h, :] = (second * cos_t + first * sin_t) * scale
    for h in range(2):
        base = 1024 + h * 256
        first, second = qkv_ref[:, base:base + LANES], qkv_ref[:, base + LANES:base + 256]
        halves = (first * cos_t - second * sin_t, second * cos_t + first * sin_t)
        for half in range(2):
            value = qkv_ref[:, base + 512 + half * LANES:base + 512 + (half + 1) * LANES]
            for i in range(4):
                kn[:, i * 4 + half * 2 + h, :] = halves[half]
                vn[:, i * 4 + half * 2 + h, :] = value

    row_id = lax.broadcasted_iota(jnp.int32, (8, n_cols), 0)
    col_id = lax.broadcasted_iota(jnp.int32, (8, n_cols), 1)
    half_col = (col_id // 2) % 2
    same_half = row_id // 4 == half_col
    same_kv = (row_id // 2) % 2 == col_id % 2
    slot_col = col_id // 4
    sub_id = lax.broadcasted_iota(jnp.int32, (16, LANES), 0) // 4

    @pl.loop(0, n_steps)
    def _(step):
        slot = lax.rem(step, depth)
        if ahead < n_steps:
            @pl.when(step + ahead < n_steps)
            def _():
                @pl.when(step >= depth - ahead)
                def _():
                    for copy in writes(step - (depth - ahead)):
                        copy.wait()
                for copy in reads(step + ahead):
                    copy.start()

        for copy in reads(step):
            copy.wait()
        for i in range(group):
            row = step * group + i
            now = lax.rem(pos_ref[row], cache_len)
            window = pl.ds(pl.multiple_of(now // 4 * 16, 16), 16)
            hit = sub_id == lax.rem(now, 4)
            kbuf[slot, i, window, :] = jnp.where(hit, kn[row].astype(jnp.bfloat16), kbuf[slot, i, window, :])
            vbuf[slot, i, window, :] = jnp.where(hit, vn[row].astype(jnp.bfloat16), vbuf[slot, i, window, :])
        for i in range(group):
            part = lax.dot_general(q8[step * group + i].astype(jnp.bfloat16), kbuf[slot, i], (((1,), (1,)), ((), ())), preferred_element_type=jnp.float32)
            sbuf[i] = jnp.where(same_half & same_kv, part, 0.0)
        for i in range(group):
            part = sbuf[i]
            part = part + pltpu.roll(part, 4, 0)
            other = jnp.where(half_col == 0, pltpu.roll(part, n_cols - 2, 1), pltpu.roll(part, 2, 1))
            scores = SOFT_CAP * jnp.tanh((part + other) / SOFT_CAP)
            scores = jnp.where(same_kv & (slot_col <= pos_ref[step * group + i]), scores, -1e30)
            weights = jnp.exp(scores - jnp.max(scores, axis=1, keepdims=True))
            total = jnp.sum(jnp.where(same_half, weights, 0.0), axis=1, keepdims=True)
            pbuf[i] = jnp.where(same_half, weights / total, 0.0).astype(jnp.bfloat16)
        for i in range(group):
            outs[step * group + i] = jnp.dot(pbuf[i], vbuf[slot, i], preferred_element_type=jnp.float32)
        for copy in writes(step):
            copy.start()

    for h in range(4):
        for half in range(2):
            head_ref[:, h * 256 + half * LANES:h * 256 + (half + 1) * LANES] = outs[:, half * 4 + h, :].astype(jnp.bfloat16)
    for step in range(max(n_steps - depth, 0) if ahead < n_steps else 0, n_steps):
        for copy in writes(step):
            copy.wait()


def attend(qkv, tables, positions, k_cache, v_cache):
    n_rows, cache_len, kv_loc, head_dim = k_cache.shape
    halves = head_dim // LANES
    group = 16 if cache_len <= 64 else 4
    depth = 4 if cache_len <= 64 else 8
    f32, bf16 = jnp.float32, jnp.bfloat16

    def flat(cache):
        return cache.reshape(n_rows, cache_len, kv_loc, halves, LANES).transpose(0, 1, 3, 2, 4).reshape(n_rows, cache_len * halves * kv_loc, LANES)

    def unflat(cache):
        return cache.reshape(n_rows, cache_len, halves, kv_loc, LANES).transpose(0, 1, 3, 2, 4).reshape(n_rows, cache_len, kv_loc, head_dim)

    vmem, hbm = pl.BlockSpec(memory_space=pltpu.VMEM), pl.BlockSpec(memory_space=pltpu.HBM)
    k_flat, v_flat = flat(k_cache), flat(v_cache)
    n_cols = k_flat.shape[1]
    block = (depth, group, n_cols, LANES)
    dma = pltpu.SemaphoreType.DMA
    heads, k_out, v_out = pl.pallas_call(
        functools.partial(attend_kernel, cache_len, n_rows, group, depth),
        out_shape=(jax.ShapeDtypeStruct((n_rows, 4 * head_dim), bf16), jax.ShapeDtypeStruct(k_flat.shape, bf16), jax.ShapeDtypeStruct(v_flat.shape, bf16)),
        in_specs=[pl.BlockSpec(memory_space=pltpu.SMEM), vmem, vmem, vmem, hbm, hbm],
        out_specs=(vmem, hbm, hbm),
        scratch_shapes=[pltpu.VMEM(block, bf16), pltpu.VMEM(block, bf16), pltpu.VMEM((n_rows, 8, LANES), f32), pltpu.VMEM((n_rows, 16, LANES), f32),
                        pltpu.VMEM((n_rows, 16, LANES), f32), pltpu.VMEM((n_rows, 8, LANES), f32), pltpu.VMEM((group, 8, n_cols), f32), pltpu.VMEM((group, 8, n_cols), bf16),
                        dma((2, depth)), dma((2, depth))],
        compiler_params=pltpu.CompilerParams(vmem_limit_bytes=int((62 if cache_len <= 64 else 42) * 2**20)),
        cost_estimate=pl.CostEstimate(flops=n_rows * 8 * n_cols * LANES * 4, bytes_accessed=4 * k_flat.size * 2, transcendentals=0),
        name=f"attend_{cache_len}",
    )(positions, qkv, *tables, k_flat, v_flat)
    return heads, unflat(k_out), unflat(v_out)


FF_CHUNK = 512
IN_FLIGHT = 4
QKV_CHUNK = 1024
MESH = pl.DeviceIdType.MESH


GROUPS = 4


def comm_kernel(cfg, *refs):
    it = iter(refs)
    post, layer, rows, share, width = cfg["post"], cfg["layer"], cfg["rows"], cfg["share"], cfg["width"]
    qkv, n_ff, n_q = cfg["qkv"], cfg["n_ff"], cfg["n_q"]
    raw = cfg["raw"]
    x_any, g_hbm = next(it), next(it)
    if post:
        res_any, wo_any, wg_hbm, wu_hbm, wd_hbm = (next(it) for _ in range(5))
    if qkv:
        wq_hbm, wk_hbm, wv_hbm = (next(it) for _ in range(3))
        if post:
            hid_ref = next(it)
        qkv_ref = next(it)
    else:
        out_ref = next(it)
    if raw or not post:
        x_ref = next(it)
    g_ref, tcol, st_src, st_rcv, hp, st_ss, st_rs, misc_ss, misc_rs, ld_sem = (next(it) for _ in range(10))
    if not post:
        out_rows = next(it)
    if post:
        if raw:
            raw_ref, res_ref, wo = (next(it) for _ in range(3))
        hall, apart, arecv, mpart, mrecv, wg, wu, wd, sib_out, sib_in, mine, x_in, u_all = (next(it) for _ in range(13))
        y_ss, y_rs, ff_ss, ff_rs = (next(it) for _ in range(4))
    if qkv:
        wi, wq, wk, wv, q_out, q_in, q_mine, q_x, q_ss, q_rs = (next(it) for _ in range(10))

    model, me = lax.axis_index("model"), lax.axis_index("data")
    x_pos, core = me // 2, lax.rem(me, 2)
    sib, part, diag = x_pos * 2 + 1 - core, (1 - x_pos) * 2 + core, (1 - x_pos) * 2 + 1 - core
    n_group = 4 * rows
    DIAG, SIB, PART, OWN = (pl.ds(i * rows, rows) for i in range(4))
    blocks = (OWN, SIB, PART, DIAG)
    mine_rows = [pl.ds(h * rows, rows) for h in range(GROUPS)]
    sends = []

    def remote(src, dst, send_sem, recv_sem, data=None):
        where = {"data": data} if data is not None else {"model": 1 - model}
        return pltpu.make_async_remote_copy(src_ref=src, dst_ref=dst, send_sem=send_sem, recv_sem=recv_sem, device_id=where, device_id_type=MESH)

    def send(*args):
        copy = remote(*args)
        copy.start()
        sends.append(copy)
        return copy

    def load(src, dst, sem):
        copy = pltpu.make_async_copy(src, dst, sem)
        copy.start()
        return copy

    early = [load(g_hbm, g_ref, ld_sem.at[8])]
    if post and not raw:
        x_ref = x_any
    else:
        early.append(load(x_any, x_ref, ld_sem.at[7]))
    if post:
        if raw:
            early.append(load(res_any, raw_ref, ld_sem.at[9]))
        else:
            res_ref = res_any
        if raw:
            wo_load = load(wo_any.at[layer], wo, ld_sem.at[0])
        else:
            wo = wo_any.at[layer]
        wg_load = load(wg_hbm.at[layer], wg, ld_sem.at[1])
        wu_load = load(wu_hbm.at[layer], wu, ld_sem.at[2])
        wd_load = load(wd_hbm.at[layer], wd, ld_sem.at[3])
    if qkv:
        in_loads = [load(src.at[layer + 1], dst, ld_sem.at[4 + k]) for k, (src, dst) in enumerate(((wq_hbm, wq), (wk_hbm, wk), (wv_hbm, wv)))]

    def relay_weights(c):
        col = c * QKV_CHUNK
        for k in ((0,), (1, 2))[c]:
            in_loads[k].wait()
            weight = (wq, wk, wv)[k]
            n_heads, head_dim = weight.shape[1:]
            for h in range(n_heads):
                wi[:, col:col + head_dim] = weight[:, h, :]
                col += head_dim

    barrier = pltpu.get_barrier_semaphore()
    for dev in (sib, part, diag):
        pl.semaphore_signal(barrier, inc=1, device_id={"data": dev}, device_id_type=MESH)
    pl.semaphore_signal(barrier, inc=1, device_id={"model": 1 - model}, device_id_type=MESH)
    tcol[...] = jnp.zeros_like(tcol)
    for copy in early:
        copy.wait()
    pl.semaphore_wait(barrier, 4)

    def square_sums(h, block, value):
        total = None
        for k in range(share // LANES):
            piece = value[:, k * LANES:(k + 1) * LANES]
            total = piece * piece if total is None else total + piece * piece
        tcol[h, block, :] = total

    lane_block = lax.broadcasted_iota(jnp.int32, (8, LANES), 1) // rows

    def start_scales(h, which):
        idx = which * GROUPS + h
        st_src[idx] = jnp.sum(jnp.transpose(tcol[h]).reshape(LANES // 8, 8, LANES), axis=0)
        return [send(st_src.at[idx], st_rcv.at[idx, k], st_ss.at[idx, k], st_rs.at[idx, k], dev) for k, dev in enumerate((sib, part, diag))]

    def end_scales(h, which, copies):
        idx = which * GROUPS + h
        for copy in copies:
            copy.wait_recv()

        def exchange(value, n):
            even = lax.rem(lane_block // n, 2) == 0
            return jnp.where(even, pltpu.roll(value, LANES - n * rows, 1), pltpu.roll(value, n * rows, 1))

        total = st_src[idx] + exchange(st_rcv[idx, 0], 2) + exchange(st_rcv[idx, 1], 1) + exchange(exchange(st_rcv[idx, 2], 1), 2)
        total = jnp.sum(total, axis=0, keepdims=True)
        inverse = lax.rsqrt(total / width + NORM_EPS)
        tcol[h] = jnp.transpose(jnp.broadcast_to(inverse, (LANES, LANES)))

    def gain_row(k):
        at, which = (layer + 1, 0) if k == 3 else (layer, k + 1)
        return 1.0 + g_ref[at, which:which + 1, pl.ds(pl.multiple_of(me * share, LANES), share)].astype(jnp.float32)

    def scaled(h, block, value, gain):
        return value * jnp.concatenate([tcol[h, block, :]] * (share // LANES), axis=1) * gain_row(gain)

    def q_partner(s):
        return remote(q_mine.at[s, pl.ds(0, rows)], q_x.at[s], q_ss.at[1, s], q_rs.at[1, s], part)

    def finish_qkv(pending):
        if pending is not None:
            s, copy = pending
            copy.wait_recv()
            q_mine[s] = q_mine[s] + q_in[s]
            q_partner(s).start()

    def start_qkv(h, pending=None):
        for c in range(n_q):
            s = h * n_q + c
            sums = jnp.dot(hp[h], wi[:, c * QKV_CHUNK:(c + 1) * QKV_CHUNK], preferred_element_type=jnp.float32)
            q_out[s] = sums[:2 * rows]
            q_mine[s] = sums[2 * rows:]
            copy = send(q_out.at[s], q_in.at[s], q_ss.at[0, s], q_rs.at[0, s], sib)
            finish_qkv(pending)
            pending = s, copy
        return pending

    def end_qkv():
        for h in range(GROUPS):
            for c in range(n_q):
                s = h * n_q + c
                q_partner(s).wait_recv()
                qkv_ref[mine_rows[h], c * QKV_CHUNK:(c + 1) * QKV_CHUNK] = q_mine[s, pl.ds(rows, rows), :] + q_x[s]
        for s in range(GROUPS * n_q):
            q_partner(s).wait_send()

    def spread(src, dst, base):
        copies = []
        for h in range(GROUPS):
            for k, (dev, there) in enumerate(((sib, SIB), (part, PART), (diag, DIAG))):
                cols = pl.ds(pl.multiple_of(dev * share, LANES), share)
                i = base + h * 3 + k
                copies.append(send(src.at[mine_rows[h], cols], dst.at[h, there, :], misc_ss.at[i], misc_rs.at[i], dev))
        return copies

    my_cols = pl.ds(pl.multiple_of(me * share, LANES), share)
    if not post:
        xn = out_rows
        for h in range(GROUPS):
            value = x_ref[mine_rows[h], :].astype(jnp.float32)
            inverse = lax.rsqrt(jnp.mean(value * value, axis=1, keepdims=True) + NORM_EPS)
            xn[mine_rows[h], :] = (value * inverse * (1.0 + g_ref[0, 0:1, :].astype(jnp.float32))).astype(jnp.bfloat16)
        copies = spread(xn, hp, 0)
        pending = None
        relay_weights(0)
        relay_weights(1)
        for h in range(GROUPS):
            hp[h, OWN, :] = xn[mine_rows[h], my_cols]
            for copy in copies[h * 3:h * 3 + 3]:
                copy.wait_recv()
            pending = start_qkv(h, pending)
        finish_qkv(pending)
        end_qkv()
    else:
        head_cuts = (pl.ds(0, rows), pl.ds(rows, (GROUPS - 1) * rows))
        to_part = [send(x_ref.at[cut], hall.at[2, cut], misc_ss.at[n], misc_rs.at[n], part) for n, cut in enumerate(head_cuts)]
        to_sib = send(x_ref, hall.at[1], misc_ss.at[2], misc_rs.at[2], sib)
        if raw:
            raw_copies = spread(raw_ref, res_ref, 5)
            for h in range(GROUPS):
                res_ref[h, OWN, :] = raw_ref[mine_rows[h], my_cols]
        if raw:
            wo_load.wait()
        y_copies = [[None] * 4 for _ in range(GROUPS)]

        def project(heads, places):
            sums = jnp.dot(heads, wo[...], preferred_element_type=jnp.float32)
            for n, (h, k) in enumerate(places):
                apart[h, blocks[k], :] = sums[n * rows:(n + 1) * rows]

        def to_model(*pairs):
            for h, k in pairs:
                y_copies[h][k] = send(apart.at[h, blocks[k], :], arecv.at[h, blocks[k], :], y_ss.at[h * 4 + k], y_rs.at[h * 4 + k])

        def forward(n):
            to_part[n].wait_recv()
            return send(hall.at[2, head_cuts[n]], hall.at[0, head_cuts[n]], misc_ss.at[3 + n], misc_rs.at[3 + n], sib)

        project(x_ref[...], [(h, 0) for h in range(GROUPS)])
        to_model((0, 0), (1, 0))
        to_sib.wait_recv()
        project(hall[1], [(h, 1) for h in range(GROUPS)])
        to_model((0, 1), (1, 1))
        forward(0).wait_recv()
        project(jnp.concatenate([hall[2, head_cuts[0], :], hall[0, head_cuts[0], :]], axis=0), [(0, 2), (0, 3)])
        to_model((0, 2), (0, 3), (2, 0), (2, 1))
        rest = forward(1)
        project(hall[2, head_cuts[1], :], [(h, 2) for h in range(1, GROUPS)])
        to_model((1, 2))
        rest.wait_recv()
        project(hall[0, head_cuts[1], :], [(h, 3) for h in range(1, GROUPS)])
        to_model((1, 3), (2, 2), (2, 3), (3, 0), (3, 1), (3, 2), (3, 3))
        stats = {}

        def attn_sums(h):
            for k, block in enumerate(blocks):
                y_copies[h][k].wait_recv()
                total = apart[h, block, :] + arecv[h, block, :]
                arecv[h, block, :] = total
                square_sums(h, block, total)
            stats[h] = start_scales(h, 0)

        def attn_residual(h):
            end_scales(h, 0, stats[h])
            if raw:
                for copy in raw_copies[h * 3:h * 3 + 3]:
                    copy.wait_recv()
            for block in blocks:
                residual = res_ref[h, block, :].astype(jnp.float32)
                mid = (residual + scaled(h, block, arecv[h, block, :], 0)).astype(jnp.bfloat16).astype(jnp.float32)
                arecv[h, block, :] = mid
            for block in blocks:
                square_sums(h, block, arecv[h, block, :])
            stats[h] = start_scales(h, 1)

        def attn_normed(h):
            mpart[h] = jnp.zeros((n_group, share), jnp.float32)
            end_scales(h, 1, stats[h])
            for block in blocks:
                hp[h, block, :] = scaled(h, block, arecv[h, block, :], 1).astype(jnp.bfloat16)

        def to_sibling(s):
            return remote(sib_out.at[s], sib_in.at[s], ff_ss.at[0, s], ff_rs.at[0, s], sib)

        def to_partner(s):
            return remote(mine.at[s, pl.ds(0, rows)], x_in.at[s], ff_ss.at[1, s], ff_rs.at[1, s], part)

        def act_partner(s):
            return remote(u_all.at[s, OWN], u_all.at[s, PART], ff_ss.at[2, s], ff_rs.at[2, s], part)

        def act_sibling(s):
            return remote(u_all.at[s, OWN], u_all.at[s, SIB], ff_ss.at[3, s], ff_rs.at[3, s], sib)

        def act_forward(s):
            return remote(u_all.at[s, PART], u_all.at[s, DIAG], ff_ss.at[4, s], ff_rs.at[4, s], sib)

        def add_sibling(s):
            to_sibling(s).wait_recv()
            mine[s] = mine[s] + sib_in[s]

            @pl.when(s >= IN_FLIGHT)
            def _():
                to_partner(s - IN_FLIGHT).wait_send()
            to_partner(s).start()

        def gate_up(h, start, end):
            @pl.loop(start, end)
            def _(c):
                s = h * n_ff + c
                cols = pl.ds(pl.multiple_of(c * FF_CHUNK, FF_CHUNK), FF_CHUNK)
                for k, weight in enumerate((wg, wu)):
                    sums = jnp.dot(hp[h], weight[:, cols], preferred_element_type=jnp.float32)
                    sib_out[s, :, pl.ds(k * FF_CHUNK, FF_CHUNK)] = sums[:2 * rows]
                    mine[s, :, pl.ds(k * FF_CHUNK, FF_CHUNK)] = sums[2 * rows:]
                to_sibling(s).start()

                @pl.when(s >= 1)
                def _():
                    add_sibling(s - 1)

        attn_sums(0)
        if qkv:
            relay_weights(0)
        attn_residual(0)
        if qkv:
            relay_weights(1)
        attn_sums(1)
        attn_normed(0)
        wg_load.wait()
        wu_load.wait()
        cuts = (n_ff * 3 // 10, n_ff * 7 // 10)
        for h in range(GROUPS):
            if h + 1 < GROUPS:
                gate_up(h, 0, cuts[0])
                attn_residual(h + 1)
                gate_up(h, cuts[0], cuts[1])
                attn_normed(h + 1)
                if h + 2 < GROUPS:
                    attn_sums(h + 2)
                gate_up(h, cuts[1], n_ff)
            else:
                gate_up(h, 0, n_ff)
        add_sibling(GROUPS * n_ff - 1)
        @pl.loop(0, GROUPS * n_ff)
        def _(s):
            to_partner(s).wait_recv()
            both = mine[s, pl.ds(rows, rows), :] + x_in[s]
            u_all[s, OWN, :] = (jax.nn.gelu(both[:, :FF_CHUNK], approximate=True) * both[:, FF_CHUNK:]).astype(jnp.bfloat16)
            act_partner(s).start()
            act_sibling(s).start()

        wd_load.wait()

        def down(h, c):
            s = h * n_ff + c
            act_sibling(s).wait_recv()
            act_forward(s).wait_recv()
            deep = pl.ds(pl.multiple_of(c * FF_CHUNK, FF_CHUNK), FF_CHUNK)
            mpart[h] += jnp.dot(u_all[s], wd[deep, :], preferred_element_type=jnp.float32)

        m_copies = []
        for h in range(GROUPS):
            @pl.loop(0, n_ff)
            def _(c):
                act_partner(h * n_ff + c).wait_recv()
                act_forward(h * n_ff + c).start()

                @pl.when(c >= 1)
                def _():
                    down(h, c - 1)

            down(h, n_ff - 1)
            m_copies.append(send(mpart.at[h], mrecv.at[h], y_ss.at[4 * GROUPS + h], y_rs.at[4 * GROUPS + h]))

        out_copies = []

        def ff_sums(h):
            m_copies[h].wait_recv()
            for block in blocks:
                total = mpart[h, block, :] + mrecv[h, block, :]
                mrecv[h, block, :] = total
                square_sums(h, block, total)
            stats[h] = start_scales(h, 2)

        def ff_residual(h):
            end_scales(h, 2, stats[h])
            for block in blocks:
                value = (arecv[h, block, :] + scaled(h, block, mrecv[h, block, :], 2)).astype(jnp.bfloat16)
                if qkv:
                    hid_ref[h, block, :] = value
                else:
                    hp[h, block, :] = value
            if qkv:
                for block in blocks:
                    square_sums(h, block, hid_ref[h, block, :].astype(jnp.float32))
                stats[h] = start_scales(h, 3)
            else:
                for k, (dev, block) in enumerate(((sib, SIB), (part, PART), (diag, DIAG))):
                    i = 5 + h * 3 + k
                    out_copies.append(send(hp.at[h, block, :], out_ref.at[mine_rows[h], my_cols], misc_ss.at[i], misc_rs.at[i], dev))
                out_ref[mine_rows[h], my_cols] = hp[h, OWN, :]

        def ff_normed(h):
            end_scales(h, 3, stats[h])
            for block in blocks:
                hp[h, block, :] = scaled(h, block, hid_ref[h, block, :].astype(jnp.float32), 3).astype(jnp.bfloat16)
            finish_qkv(start_qkv(h))

        ff_sums(0)
        ff_sums(1)
        ff_residual(0)
        ff_sums(2)
        ff_residual(1)
        if qkv:
            ff_normed(0)
        ff_sums(3)
        ff_residual(2)
        if qkv:
            ff_normed(1)
        ff_residual(3)
        if qkv:
            ff_normed(2)
            ff_normed(3)
        if qkv:
            end_qkv()
        for copy in out_copies:
            copy.wait_recv()

        @pl.loop(0, GROUPS * n_ff)
        def _(s):
            for copy in (to_sibling(s), act_partner(s), act_sibling(s), act_forward(s)):
                copy.wait_send()
        for s in range(GROUPS * n_ff - IN_FLIGHT, GROUPS * n_ff):
            to_partner(s).wait_send()
    for copy in sends:
        copy.wait_send()


def comm(x, gains, in_weights=None, post=None, layer=0, collective_id=0):
    rows = x.shape[0] // GROUPS
    share = gains.shape[2] // 4
    n_group = rows * 4
    f32, bf16, vmem, hbm = jnp.float32, jnp.bfloat16, pl.BlockSpec(memory_space=pltpu.VMEM), pl.BlockSpec(memory_space=pltpu.HBM)
    dma = pltpu.SemaphoreType.DMA
    args, specs = [x, gains], [hbm, hbm]
    raw = post is not None and post[0].ndim == 2
    if post is not None and not raw:
        specs[0] = vmem
    n_stat = 4 * GROUPS
    n_misc = 5 + 3 * GROUPS
    scratch = [pltpu.VMEM(x.shape, bf16)] if raw or post is None else []
    scratch += [pltpu.VMEM(gains.shape, bf16), pltpu.VMEM((GROUPS, LANES, LANES), f32), pltpu.VMEM((n_stat, 8, LANES), f32), pltpu.VMEM((n_stat, 3, 8, LANES), f32), pltpu.VMEM((GROUPS, n_group, share), bf16),
               dma((n_stat, 3)), dma((n_stat, 3)), dma((n_misc,)), dma((n_misc,)), dma((10,))]
    if post is None:
        scratch.append(pltpu.VMEM(x.shape, bf16))
    n_ff = n_q = 0
    if post is not None:
        residual, w_o, w_gate, w_up, w_down = post
        args += list(post)
        specs += [hbm if raw else vmem] * 2 + [hbm] * 3
        ff = w_gate.shape[2]
        n_ff = ff // FF_CHUNK
        steps = GROUPS * n_ff
        scratch += [pltpu.VMEM(residual.shape, bf16), pltpu.VMEM((GROUPS, n_group, share), bf16), pltpu.VMEM(w_o.shape[1:], bf16)] if raw else []
        scratch += [pltpu.VMEM((3, GROUPS * rows, w_o.shape[1]), bf16)] + [pltpu.VMEM((GROUPS, n_group, share), f32)] * 4
        scratch += [pltpu.VMEM((share, ff), bf16), pltpu.VMEM((share, ff), bf16), pltpu.VMEM((ff, share), bf16)]
        scratch += [pltpu.VMEM((steps, 2 * rows, 2 * FF_CHUNK), f32)] * 3 + [pltpu.VMEM((steps, rows, 2 * FF_CHUNK), f32), pltpu.VMEM((steps, n_group, FF_CHUNK), bf16)]
        scratch += [dma((5 * GROUPS,)), dma((5 * GROUPS,)), dma((5, steps)), dma((5, steps))]
    if in_weights is not None:
        args += list(in_weights)
        specs += [hbm] * 3
        n_in = sum(w.shape[2] * w.shape[3] for w in in_weights)
        n_q = n_in // QKV_CHUNK
        scratch += [pltpu.VMEM((share, n_in), bf16)] + [pltpu.VMEM(w.shape[1:], bf16) for w in in_weights]
        scratch += [pltpu.VMEM((GROUPS * n_q, 2 * rows, QKV_CHUNK), f32)] * 3 + [pltpu.VMEM((GROUPS * n_q, rows, QKV_CHUNK), f32), dma((2, GROUPS * n_q)), dma((2, GROUPS * n_q))]
        out_shape = [jax.ShapeDtypeStruct((GROUPS, n_group, share), bf16), jax.ShapeDtypeStruct((GROUPS * rows, n_in), f32)][post is None:]
        out_specs = [vmem, vmem][post is None:]
    else:
        out_shape = jax.ShapeDtypeStruct((GROUPS * rows, 4 * share), bf16)
        out_specs = vmem
    cfg = {"raw": raw, "post": post is not None, "qkv": in_weights is not None, "layer": layer, "rows": rows, "share": share, "width": 4 * share, "n_ff": n_ff, "n_q": n_q}
    return pl.pallas_call(
        functools.partial(comm_kernel, cfg),
        out_shape=out_shape, in_specs=specs, out_specs=out_specs, scratch_shapes=scratch,
        compiler_params=pltpu.CompilerParams(collective_id=collective_id, has_side_effects=True, vmem_limit_bytes=int((62, 62, 49)[collective_id] * 2**20)),
        name=f"comm_{collective_id}",
    )(*args)


def solution(mesh):
    def device_step(hidden, positions, k_local, v_local, k_global, v_global, w_q, w_k, w_v, w_o, w_gate, w_up, w_down, norm_gains):
        share = w_q.shape[1]
        tables = rope_tables(positions, w_q.shape[3])
        in_weights = (w_q, w_k, w_v)
        post_weights = (w_o.reshape(2, -1, share), w_gate, w_up, w_down)
        hidden_rows = hidden[:, 0, :]
        qkv, = comm(hidden_rows, norm_gains, in_weights, layer=-1, collective_id=0)
        heads, k_local, v_local = attend(qkv, tables, positions, k_local, v_local)
        residual, qkv = comm(heads, norm_gains, in_weights, (hidden_rows,) + post_weights, layer=0, collective_id=1)
        heads, k_global, v_global = attend(qkv, tables, positions, k_global, v_global)
        final = comm(heads, norm_gains, None, (residual,) + post_weights, layer=1, collective_id=2)[:, None, :]
        return final, k_local, v_local, k_global, v_global

    in_specs = (ROW_SPEC, POS_SPEC, CACHE_SPEC, CACHE_SPEC, CACHE_SPEC, CACHE_SPEC, PROJ_IN_SPEC, PROJ_IN_SPEC, PROJ_IN_SPEC, PROJ_OUT_SPEC, FF_IN_SPEC, FF_IN_SPEC, FF_OUT_SPEC, GAIN_SPEC)
    out_specs = (ROW_SPEC, CACHE_SPEC, CACHE_SPEC, CACHE_SPEC, CACHE_SPEC)
    return jax.shard_map(device_step, mesh=mesh, in_specs=in_specs, out_specs=out_specs, check_vma=False)
```
